512 devices in a mesh: gx: 8 (over y), gy: 8 (over z), gz: 8 (over x, core).
Axes of the slice: x: 4, y: 8, z: 8, core: 2. Of those that a mesh axis runs over, the one named last changes fastest.
Arguments:
- source: float32 [2, 32, 64, 1024], P(None, 'gx', 'gy', 'gz'), may hold values from -6 to 6
- sigma_intra: float32 [3, 32, 64, 1024], P(None, 'gx', 'gy', 'gz'), may hold values from 0.3 to 3
- sigma_extra: float32 [3, 32, 64, 1024], P(None, 'gx', 'gy', 'gz'), may hold values from 0.5 to 3
- membrane: float32 [32, 64, 1024], P('gx', 'gy', 'gz'), may hold values from 0.5 to 5
Outputs:
- solution: float32 [2, 32, 64, 1024], P(None, 'gx', 'gy', 'gz')
- residual: float32 [2, 32, 64, 1024], P(None, 'gx', 'gy', 'gz')
The draws below stay inside these ranges and needn't reach their ends.
All inputs are finite; a program needn't handle non-finite values.
Results may differ from the reference program's by a relative error of at most 0.0009.
Values sent between devices are 32-bit elements; how exact they have to be, the bound alone decides.
No kernel may reach another device: no remote copies, remote signals or barrier semaphores. Data moves between devices by JAX's collectives and lax.ppermute only.
A program may use at most 64 MiB of HBM per device.

```python
import math
import jax
import jax.numpy as jnp
from jax import lax

KRYLOV = 10
NX = 32
NY = 64
NZ = 1024


def steps_of(stream_key, shape, shards, low, largest):
    gain, own = 1.0, jax.random.fold_in(stream_key, 6)
    for dim, parts in shards:
        draws = jnp.exp(jax.random.uniform(jax.random.fold_in(own, dim), (parts,), jnp.float32, low / len(shards), largest / len(shards)))
        gain = gain * jnp.repeat(draws, shape[dim] // parts).reshape([-1 if axis == dim else 1 for axis in range(len(shape))])
    return gain


def normal_values(stream_key, shape, width, most, shards=(), dtype=jnp.bfloat16):
    array = jax.random.normal(stream_key, shape, jnp.float32) * width
    if len(shards) > 0:
        array = steps_of(stream_key, shape, shards, -0.22, 0.18) * array
    return jnp.clip(array, min=-most, max=most).astype(dtype)


def setup_inputs(seed: int = 0) -> dict:
    keys = jax.random.split(jax.random.key(seed), 5)
    return {
        "source": normal_values(keys[0], (2, NX, NY, NZ), 1.0, 6.0, ((1, 8), (2, 8), (3, 8)), jnp.float32),
        "sigma_intra": jnp.clip(jnp.exp(math.log(3.0) - 2.3025851 * jax.random.uniform(keys[1], (3, NX, NY, NZ), jnp.float32) ** steps_of(keys[1], (3, NX, NY, NZ), ((1, 8), (2, 8), (3, 8)), -0.2, 0.2)), 0.3, 3.0),
        "sigma_extra": jnp.clip(jnp.exp(math.log(3.0) - 1.7917595 * jax.random.uniform(keys[2], (3, NX, NY, NZ), jnp.float32) ** steps_of(keys[2], (3, NX, NY, NZ), ((1, 8), (2, 8), (3, 8)), -0.2, 0.2)), 0.5, 3.0),
        "membrane": jnp.clip(jnp.exp(math.log(5.0) - 2.3025851 * jax.random.uniform(keys[3], (NX, NY, NZ), jnp.float32) ** steps_of(keys[3], (NX, NY, NZ), ((0, 8), (1, 8), (2, 8)), -0.2, 0.2)), 0.5, 5.0),
    }


highest = lax.Precision.HIGHEST

def shifted(padded_grid, spatial, offset):
    pieces = [slice(1, -1), slice(1, -1), slice(1, -1)]
    if offset > 0:
        pieces[spatial] = slice(2, None)
    else:
        pieces[spatial] = slice(None, -2)
    return padded_grid[tuple(pieces)]

def face_terms(padded_sigma):
    upper_faces = []
    lower_faces = []
    for spatial in range(3):
        component = padded_sigma[spatial]
        middle = component[1:-1, 1:-1, 1:-1]
        upper_faces.append(0.5 * (middle + shifted(component, spatial, 1)))
        lower_faces.append(0.5 * (middle + shifted(component, spatial, -1)))
    diagonal = upper_faces[0] + lower_faces[0]
    for spatial in range(1, 3):
        diagonal = diagonal + upper_faces[spatial] + lower_faces[spatial]
    return (upper_faces, lower_faces, diagonal)

def apply_laplace(faces, padded_field):
    upper_faces, lower_faces, diagonal = faces
    result = diagonal * padded_field[1:-1, 1:-1, 1:-1]
    for spatial in range(3):
        result = result - upper_faces[spatial] * shifted(padded_field, spatial, 1)
        result = result - lower_faces[spatial] * shifted(padded_field, spatial, -1)
    return result

def operate(intra_faces, extra_faces, membrane, padded_pair):
    joined = padded_pair[0] + padded_pair[1]
    shared = apply_laplace(intra_faces, joined)
    leading = membrane * padded_pair[0, 1:-1, 1:-1, 1:-1] + shared
    second = shared + apply_laplace(extra_faces, padded_pair[1])
    return jnp.stack([leading, second])

def inverse_blocks(intra_faces, extra_faces, membrane):
    intra_sum = intra_faces[2]
    extra_sum = extra_faces[2]
    determinant = membrane * intra_sum + membrane * extra_sum + intra_sum * extra_sum
    return jnp.stack([(intra_sum + extra_sum) / determinant, -intra_sum / determinant, (membrane + intra_sum) / determinant])

def precondition(inverse, pair):
    leading = inverse[0] * pair[0] + inverse[1] * pair[1]
    second = inverse[1] * pair[0] + inverse[2] * pair[1]
    return jnp.stack([leading, second])

def least_squares(hessenberg, start_norm):
    krylov = hessenberg.shape[1]
    rotated = hessenberg
    target = jnp.zeros((krylov + 1,), jnp.float32).at[0].set(start_norm)
    for column in range(krylov):
        pivot = rotated[column, column]
        lower_entry = rotated[column + 1, column]
        radius = jnp.sqrt(pivot * pivot + lower_entry * lower_entry)
        cosine = pivot / radius
        sine_value = lower_entry / radius
        row_top = cosine * rotated[column] + sine_value * rotated[column + 1]
        row_below = -sine_value * rotated[column] + cosine * rotated[column + 1]
        rotated = rotated.at[column].set(row_top).at[column + 1].set(row_below)
        leading = cosine * target[column] + sine_value * target[column + 1]
        second = -sine_value * target[column] + cosine * target[column + 1]
        target = target.at[column].set(leading).at[column + 1].set(second)
    coeffs = jnp.zeros((krylov,), jnp.float32)
    for column in range(krylov - 1, -1, -1):
        partial_sum = jnp.sum(rotated[column, column + 1:] * coeffs[column + 1:])
        coeffs = coeffs.at[column].set((target[column] - partial_sum) / rotated[column, column])
    return coeffs

def reference(source, sigma_intra, sigma_extra, membrane):
    margins = ((0, 0), (1, 1), (1, 1), (1, 1))
    intra_faces = face_terms(jnp.pad(sigma_intra, margins))
    extra_faces = face_terms(jnp.pad(sigma_extra, margins))
    inverse = inverse_blocks(intra_faces, extra_faces, membrane)
    start_norm = jnp.sqrt(jnp.sum(source * source))
    basis = jnp.zeros((KRYLOV + 1,) + source.shape, jnp.float32).at[0].set(source / start_norm)
    hessenberg = jnp.zeros((KRYLOV + 1, KRYLOV), jnp.float32)
    for column in range(KRYLOV):
        solved = precondition(inverse, basis[column])
        applied = operate(intra_faces, extra_faces, membrane, jnp.pad(solved, margins))
        flat_basis = basis[:column + 1].reshape(column + 1, -1)
        project = jnp.dot(flat_basis, applied.reshape(-1), precision=highest)
        applied = applied - jnp.dot(project, flat_basis, precision=highest).reshape(applied.shape)
        new_norm = jnp.sqrt(jnp.sum(applied * applied))
        basis = basis.at[column + 1].set(applied / new_norm)
        hessenberg = hessenberg.at[:column + 1, column].set(project).at[column + 1, column].set(new_norm)
    coeffs = least_squares(hessenberg, start_norm)
    combined = jnp.dot(coeffs, basis[:KRYLOV].reshape(KRYLOV, -1), precision=highest).reshape(source.shape)
    solution = precondition(inverse, combined)
    remainder = jnp.zeros((KRYLOV + 1,), jnp.float32).at[0].set(start_norm) - jnp.dot(hessenberg, coeffs, precision=highest)
    residual = jnp.dot(remainder, basis.reshape(KRYLOV + 1, -1), precision=highest).reshape(source.shape)
    return (solution, residual)
```

```python
import jax
import jax.numpy as jnp
from jax import lax
from jax.experimental import pallas as pl
from jax.experimental.pallas import tpu as pltpu
from jax.sharding import PartitionSpec as P

KRYLOV = 10
DEPTH = KRYLOV + 1
FINE = 16
EXT = FINE + 2 * DEPTH
FIELDS = 9
SLOT = KRYLOV + 2
ROWS = 40
f32 = jnp.float32


def lanes():
    return lax.broadcasted_iota(jnp.int32, (8, 128), 1)


def sublanes(rows=8):
    return lax.broadcasted_iota(jnp.int32, (rows, 128), 0)


def turn(v, by):
    return pltpu.roll(v, by % 128, 1)


def sink(v, by):
    return pltpu.roll(v, by % 8, 0)


def two_sum(a, b):
    s = a + b
    z = s - a
    return s, (a - (s - z)) + (b - z)


def quick_sum(a, b):
    s = a + b
    return s, b - (s - a)


def split(a):
    c = a * 4097.0
    high = c - (c - a)
    return high, a - high


def two_prod(a, b):
    p = a * b
    ah, al = split(a)
    bh, bl = split(b)
    return p, ((ah * bh - p) + ah * bl + al * bh) + al * bl


def dd_add(a, b):
    s, e = two_sum(a[0], b[0])
    t, g = two_sum(a[1], b[1])
    s, e = quick_sum(s, e + t)
    return quick_sum(s, e + g)


def dd_mul(a, b):
    p, e = two_prod(a[0], b[0])
    return quick_sum(p, e + (a[0] * b[1] + a[1] * b[0]))


def dd_neg(a):
    return (-a[0], -a[1])


def dd_inverse(a):
    x = 1.0 / a[0]
    for _ in range(2):
        p = dd_mul(a, (x, jnp.zeros_like(x))) if not isinstance(x, tuple) else dd_mul(a, x)
        r = dd_add((jnp.ones_like(p[0]), jnp.zeros_like(p[0])), dd_neg(p))
        full = x if isinstance(x, tuple) else (x, jnp.zeros_like(x))
        x = dd_add(full, dd_mul(full, r))
    return x


def dd_fold(a):
    for by in (4, 2, 1):
        a = dd_add(a, (sink(a[0], by), sink(a[1], by)))
    return a


def dd_total(pairs):
    pairs = list(pairs)
    while len(pairs) > 1:
        pairs = [
            dd_add(pairs[i], pairs[i + 1]) if i + 1 < len(pairs) else pairs[i]
            for i in range(0, len(pairs), 2)
        ]
    return pairs[0]


def swap_blocks(v, width):
    v = list(v)
    block = lanes() // width
    d = len(v) // 2
    while d >= 1:
        low = (block & d) == 0
        for k in range(len(v)):
            if k & d == 0:
                a, b = v[k], v[k + d]
                v[k] = jnp.where(low, a, turn(b, width * d))
                v[k + d] = jnp.where(low, turn(a, -width * d), b)
        d //= 2
    return v


def pack_kernel(source, intra, extra, membrane, out, rows):
    pieces = [(intra, i) for i in range(3)] + [(extra, i) for i in range(3)]
    pieces += [(source, i) for i in range(2)]
    for f, (ref, i) in enumerate(pieces):
        for x in range(4):
            rows[pl.ds(f * 32 + x, 8, stride=4), :] = ref[i, x]
    for x in range(4):
        rows[pl.ds(256 + x, 8, stride=4), :] = membrane[x]
    rows[pl.ds(288, 96), :] = jnp.zeros((96, 128), f32)
    halves = []
    for half in (0, 16):
        halves.append(
            jnp.concatenate([rows[pl.ds(f * 32 + half, 16), :] for f in range(8)], 0).T
        )
    last = rows[pl.ds(256, 128), :].T
    near = lanes() < 32
    for j in range(8):
        at = j * ROWS
        out[pl.ds(at, 16), :] = halves[0][16 * j : 16 * j + 16]
        out[pl.ds(at + 16, 8), :] = jnp.where(
            near, last[16 * j : 16 * j + 8], turn(last[16 * j + 8 : 16 * j + 16], 32)
        )
        out[pl.ds(at + 24, 16), :] = halves[1][16 * j : 16 * j + 16]


def plane_kernel(main, above, below, above2, below2, out, first, final):
    lane = lanes()
    quarter = lane // 32
    early = (lane % 32) < 16

    def take(ref, row, height):
        return ref[pl.ds(row, 8, stride=height), :]

    for z in range(FINE):
        v = [
            take(main, z, ROWS),
            take(main, 24 + z, ROWS),
            take(above, z, ROWS),
            take(above, 24 + z, ROWS),
            take(above2, z, 24),
            take(below2, 8 + z, 24),
            take(below, z, ROWS),
            take(below, 24 + z, ROWS),
        ]
        v = swap_blocks(v, 16)
        r, shift = z % 8, 32 * (z // 8)
        outer = jnp.where(early, take(above2, 16 + r, 24), take(below2, r, 24))
        m = turn(take(below, 16 + r, ROWS), 96 - shift)
        m = jnp.where(quarter == 2, turn(outer, 64 - shift), m)
        m = jnp.where(quarter == 1, turn(take(above, 16 + r, ROWS), 32 - shift), m)
        m = jnp.where(quarter == 0, turn(take(main, 16 + r, ROWS), -shift), m)
        for f, value in enumerate(v + [m]):
            out[f, z] = value
            if z < DEPTH:
                first[f, z] = value
            if z >= FINE - DEPTH:
                final[f, z - (FINE - DEPTH)] = value


def x_up(v):
    return jnp.where(lanes() % 4 < 3, turn(v, -1), turn(sink(v, -1), 3))


def x_down(v):
    return jnp.where(lanes() % 4 > 0, turn(v, 1), turn(sink(v, 1), -3))


def y_up(v):
    return turn(v, -4)


def y_down(v):
    return turn(v, 4)


def cycle_kernel(
    main, low, high, sums, fields, images, ext, face, inv, ta, tb, tc, qp, cbuf, gram, parts, acc
):
    for f in range(FIELDS):
        ext[f, pl.ds(0, DEPTH)] = low[f]
        ext[f, pl.ds(DEPTH, FINE)] = main[f]
        ext[f, pl.ds(DEPTH + FINE, DEPTH)] = high[f]

    lane = lanes()
    ix = sublanes() * 4 + lane % 4
    last_x, first_x = ix == 31, ix == 0

    def faces_z(i, _):
        for s in range(2):
            face[s * 3 + 2, i] = 0.5 * (ext[s * 3 + 2, i] + ext[s * 3 + 2, i + 1])
        return _

    lax.fori_loop(0, EXT - 1, faces_z, 0)

    def coefficients(i, _):
        diagonals = []
        for s in range(2):
            sx, sy = ext[s * 3, i], ext[s * 3 + 1, i]
            up_x = 0.5 * (sx + jnp.where(last_x, 0.0, x_up(sx)))
            low_x = 0.5 * (sx + jnp.where(first_x, 0.0, x_down(sx)))
            up_y = 0.5 * (sy + y_up(sy))
            low_y = 0.5 * (sy + y_down(sy))
            up_z, low_z = face[s * 3 + 2, i], face[s * 3 + 2, i - 1]
            face[s * 3, i] = jnp.where(last_x, 0.0, up_x)
            face[s * 3 + 1, i] = up_y
            diagonals.append(up_x + low_x + up_y + low_y + up_z + low_z)
        di, de = diagonals
        m = ext[8, i]
        det = m * di + m * de + di * de
        inside = m > 0.0
        scale = jnp.where(inside, 1.0 / jnp.where(inside, det, 1.0), 0.0)
        inv[0, i] = de * scale
        inv[1, i] = m * scale
        inv[2, i] = -di * scale
        inv[3, i] = (m + di) * scale
        ta[0, i] = ext[6, i]
        ta[1, i] = ext[7, i]
        return _

    lax.fori_loop(1, EXT - 1, coefficients, 0, unroll=2)

    block = lane // 32

    def compact(read):
        got = []
        for g in range(FINE // 4):
            value = turn(read(4 * g + 3), 96)
            for j in (2, 1):
                value = jnp.where(block == j, turn(read(4 * g + j), 32 * j), value)
            got.append(jnp.where(block == 0, read(4 * g), value))
        return got

    def remember(r, part, values):
        for g, value in enumerate(values):
            at = part * 4 + g
            images[r, at] = value
            high_part, low_part = split(value)
            gram[0, r, at] = high_part
            gram[1, r, at] = low_part

    for part in range(2):
        remember(0, part, compact(lambda z: main[6 + part, z]))

    buffers = (ta, tb, tc)
    for k in range(KRYLOV):
        now, then, new = buffers[k % 3], buffers[(k - 1) % 3], buffers[(k + 1) % 3]

        def blocks(i, _):
            v, p = now[0, i], now[1, i]
            qp[0, i] = inv[0, i] * v + inv[1, i] * p
            qp[1, i] = inv[2, i] * v + inv[3, i] * p
            return _

        lax.fori_loop(1 + k, EXT - 1 - k, blocks, 0, unroll=2)

        def spread(s, i):
            u = qp[s, i]
            fx, fy = face[s * 3, i], face[s * 3 + 1, i]
            total = fx * x_up(u) + x_down(fx * u)
            total = total + (fy * y_up(u) + y_down(fy * u))
            return total + (
                face[s * 3 + 2, i] * qp[s, i + 1] + face[s * 3 + 2, i - 1] * qp[s, i - 1]
            )

        def apply(i, main_planes):
            shared = spread(0, i)
            bv, bp = -shared, -(shared + spread(1, i))
            if main_planes:
                cbuf[0, i - DEPTH] = now[0, i] + bv
                cbuf[1, i - DEPTH] = now[1, i] + bp
            if k + 1 < KRYLOV:
                if k == 0:
                    new[0, i] = bv
                    new[1, i] = bp
                else:
                    new[0, i] = 2.0 * bv - then[0, i]
                    new[1, i] = 2.0 * bp - then[1, i]

        def outer(i, _):
            apply(i, False)
            return _

        def inner(i, _):
            apply(i, True)
            return _

        if k + 1 < KRYLOV:
            lax.fori_loop(2 + k, DEPTH, outer, 0)
            lax.fori_loop(DEPTH + FINE, EXT - 2 - k, outer, 0)
        lax.fori_loop(DEPTH, DEPTH + FINE, inner, 0, unroll=2)
        for part in range(2):
            values = compact(lambda z: qp[part, DEPTH + z])
            for g, value in enumerate(values):
                fields[k, part * 4 + g] = value
            remember(k + 1, part, compact(lambda z: cbuf[part, z]))

    parts[...] = jnp.zeros((2048, 128), f32)
    for r in range(1, KRYLOV + 1):

        def product(s, _):
            total, error = None, None
            for at in range(8):
                a, b = images[r, at], images[s, at]
                ah, al, bh, bl = gram[0, r, at], gram[1, r, at], gram[0, s, at], gram[1, s, at]
                p = a * b
                e = ((ah * bh - p) + ah * bl + al * bh) + al * bl
                if total is None:
                    total, error = p, e
                else:
                    total, e2 = two_sum(total, p)
                    error = error + (e + e2)
            column = jnp.where(s == 0, KRYLOV, s - 1)
            slot = ((r - 1) * SLOT + column) * 8
            mirror = jnp.where(s == 0, slot, ((s - 1) * SLOT + r - 1) * 8)
            for at in (slot, mirror):
                at = pl.multiple_of(at, 8)
                parts[pl.ds(at, 8), :] = total
                parts[pl.ds(1024 + at, 8), :] = error
            return _

        lax.fori_loop(0, r + 1, product, 0)

    for group in range(16):
        total = dd_total(
            (
                parts[pl.ds(group * 64 + i, 8, stride=8), :],
                parts[pl.ds(1024 + group * 64 + i, 8, stride=8), :],
            )
            for i in range(8)
        )
        acc[0, pl.ds(group * 8, 8), :] = total[0]
        acc[1, pl.ds(group * 8, 8), :] = total[1]
    turned = acc[0].T, acc[1].T
    total = dd_total(
        (turned[0][8 * i : 8 * i + 8], turned[1][8 * i : 8 * i + 8]) for i in range(16)
    )
    share(dd_fold(total), sums)


def share(total, out):
    rows = jnp.where(sublanes() % 2 == 0, total[0], total[1])
    for i in range(out.shape[0] // 8):
        out[pl.ds(8 * i, 8), :] = rows


def gathered(ref):
    count = ref.shape[0] // 2
    total = dd_total(
        (ref[pl.ds(16 * i, 8, stride=2), :], ref[pl.ds(16 * i + 1, 8, stride=2), :])
        for i in range(count // 8)
    )
    return dd_fold(total)


def sum_kernel(received, out):
    share(gathered(received), out)


def solve_kernel(received, fields, images, out):
    total = gathered(received)
    row = sublanes(16)
    matrix = []
    for part in total:
        part = jnp.concatenate([part, part], 0)
        value = jnp.zeros((16, 128), f32)
        for r in range(KRYLOV):
            value = jnp.where(row == r, turn(part, -r * SLOT), value)
        matrix.append(value)
    for j in range(KRYLOV):
        pivot_row = tuple(
            jnp.broadcast_to(part[j : j + 1, :], (8, 128)) for part in matrix
        )
        pivot = tuple(jnp.broadcast_to(part[:, j : j + 1], (8, 128)) for part in pivot_row)
        scaled = dd_mul(pivot_row, dd_inverse(pivot))
        scaled = tuple(jnp.concatenate([part, part], 0) for part in scaled)
        column = tuple(jnp.broadcast_to(part[:, j : j + 1], (16, 128)) for part in matrix)
        rest = dd_add(tuple(matrix), dd_neg(dd_mul(column, scaled)))
        matrix = [jnp.where(row == j, a, b) for a, b in zip(scaled, rest)]
    coeffs = [
        jnp.broadcast_to(matrix[0][k : k + 1, KRYLOV : KRYLOV + 1], (8, 128))
        for k in range(KRYLOV)
    ]
    for g in range(FINE // 4):
        v = []
        for part in range(2):
            value = coeffs[0] * fields[0, part * 4 + g]
            for k in range(1, KRYLOV):
                value = value + coeffs[k] * fields[k, part * 4 + g]
            v.append(value)
        v[0] = v[0] - v[1]
        for part in range(2):
            value = coeffs[0] * images[1, part * 4 + g]
            for k in range(1, KRYLOV):
                value = value + coeffs[k] * images[k + 1, part * 4 + g]
            v.append(images[0, part * 4 + g] - value)
        for j, value in enumerate(swap_blocks(v, 32)):
            out[pl.ds(4 * g + j, 8, stride=FINE), :] = value


def unpack_kernel(received, solution, residual, rows):
    rows[...] = received[...].T
    for f in range(4):
        ref = solution if f < 2 else residual
        for x in range(4):
            ref[f % 2, x] = rows[pl.ds(f * 32 + x, 8, stride=4), :]


def shape(*dims):
    return jax.ShapeDtypeStruct(dims, f32)


def scratch(*dims):
    return pltpu.VMEM(dims, f32)


def body(source, sigma_intra, sigma_extra, membrane):
    nx, ny, nz = (lax.axis_size(a) for a in ("gx", "gy", "gz"))
    packed = pl.pallas_call(
        pack_kernel, out_shape=shape(8 * ROWS, 128), scratch_shapes=[scratch(384, 128)]
    )(source, sigma_intra, sigma_extra, membrane)
    own = lax.all_to_all(packed.reshape(8, ROWS, 128), "gx", 0, 0, tiled=True)

    def from_y(value, by):
        pairs = [(i, i - by) for i in range(ny) if 0 <= i - by < ny]
        got = lax.ppermute(value, "gy", pairs)
        return got.reshape(-1, 128)

    halo = (from_y(own, 1), from_y(own, -1), from_y(own[:, :24], 2), from_y(own[:, 16:], -2))
    planes, first, final = pl.pallas_call(
        plane_kernel,
        out_shape=(
            shape(FIELDS, FINE, 8, 128),
            shape(FIELDS, DEPTH, 8, 128),
            shape(FIELDS, DEPTH, 8, 128),
        ),
    )(own.reshape(-1, 128), *halo)

    def place(c):
        return (c % nx) * nz + c // nx

    up = [(place(c), place(c + 1)) for c in range(nx * nz - 1)]
    low = lax.ppermute(final, ("gx", "gz"), up)
    high = lax.ppermute(first, ("gx", "gz"), [(b, a) for a, b in up])

    sums, fields, images = pl.pallas_call(
        cycle_kernel,
        out_shape=(
            shape(2 * nx * ny, 128),
            shape(KRYLOV, 8, 8, 128),
            shape(KRYLOV + 1, 8, 8, 128),
        ),
        scratch_shapes=[
            scratch(FIELDS, EXT, 8, 128),
            scratch(6, EXT, 8, 128),
            scratch(4, EXT, 8, 128),
            scratch(2, EXT, 8, 128),
            scratch(2, EXT, 8, 128),
            scratch(2, EXT, 8, 128),
            scratch(2, EXT, 8, 128),
            scratch(2, FINE, 8, 128),
            scratch(2, KRYLOV + 1, 8, 8, 128),
            scratch(2048, 128),
            scratch(2, 128, 128),
        ],
    )(planes, low, high)

    got = lax.all_to_all(sums.reshape(nx * ny, 2, 128), ("gx", "gy"), 0, 0, tiled=True)
    sums = pl.pallas_call(sum_kernel, out_shape=shape(2 * nz, 128))(got.reshape(-1, 128))
    got = lax.all_to_all(sums.reshape(nz, 2, 128), "gz", 0, 0, tiled=True)
    result = pl.pallas_call(solve_kernel, out_shape=shape(8 * FINE, 128))(
        got.reshape(-1, 128), fields, images
    )
    result = lax.all_to_all(result.reshape(8, FINE, 128), "gx", 0, 0, tiled=True)
    return pl.pallas_call(
        unpack_kernel,
        out_shape=(shape(2, 4, 8, 128), shape(2, 4, 8, 128)),
        scratch_shapes=[scratch(128, 128)],
    )(result.reshape(-1, 128))


def solution(mesh):
    spread = P(None, "gx", "gy", "gz")
    return jax.shard_map(
        body,
        mesh=mesh,
        in_specs=(spread, spread, spread, P("gx", "gy", "gz")),
        out_specs=(spread, spread),
        check_vma=False,
    )
```

```python
import jax
import jax.numpy as jnp
from jax import lax
from jax.experimental import pallas as pl
from jax.experimental.pallas import tpu as pltpu
from jax.sharding import PartitionSpec as P

KRYLOV = 10
DEPTH = KRYLOV + 1
FINE = 16
EXT = FINE + 2 * DEPTH
SENT = 7
FIELDS = 9
ROWS = 40
UNIQUE = KRYLOV * (KRYLOV + 1) // 2
f32 = jnp.float32


def lanes(rows=8):
    return lax.broadcasted_iota(jnp.int32, (rows, 128), 1)


def sublanes(rows=8):
    return lax.broadcasted_iota(jnp.int32, (rows, 128), 0)


def turn(v, by):
    return v if by % 128 == 0 else pltpu.roll(v, by % 128, 1)


def sink(v, by):
    return pltpu.roll(v, by % 8, 0)


def two_sum(a, b):
    s = a + b
    z = s - a
    return s, (a - (s - z)) + (b - z)


def quick_sum(a, b):
    s = a + b
    return s, b - (s - a)


def split(a):
    c = a * 4097.0
    high = c - (c - a)
    return high, a - high


def two_prod(a, b):
    p = a * b
    ah, al = split(a)
    bh, bl = split(b)
    return p, ((ah * bh - p) + ah * bl + al * bh) + al * bl


def dd_add(a, b):
    s, e = two_sum(a[0], b[0])
    return quick_sum(s, e + (a[1] + b[1]))


def dd_mul(a, b):
    p, e = two_prod(a[0], b[0])
    return quick_sum(p, e + (a[0] * b[1] + a[1] * b[0]))


def dd_inverse(a):
    x = 1.0 / a[0]
    p, e = two_prod(a[0], x)
    return quick_sum(x, x * (((1.0 - p) - e) - a[1] * x))


def add_pairs(a, b):
    s, e = two_sum(a[0], b[0])
    return s, e + (a[1] + b[1])


def total_of(pairs):
    pairs = list(pairs)
    while len(pairs) > 1:
        pairs = [
            add_pairs(pairs[i], pairs[i + 1]) if i + 1 < len(pairs) else pairs[i]
            for i in range(0, len(pairs), 2)
        ]
    return pairs[0]


def fold_sublanes(a):
    for by in (4, 2, 1):
        a = add_pairs(a, (sink(a[0], by), sink(a[1], by)))
    return quick_sum(*a)


def swap_blocks(v, width):
    v = list(v)
    block = lanes() // width
    d = len(v) // 2
    while d >= 1:
        low = (block & d) == 0
        for k in range(len(v)):
            if k & d == 0:
                a, b = v[k], v[k + d]
                v[k] = jnp.where(low, a, turn(b, width * d))
                v[k + d] = jnp.where(low, turn(a, -width * d), b)
        d //= 2
    return v


def pack_kernel(source, intra, extra, membrane, out):
    refs = [(intra, 0), (intra, 1), (intra, 2), (extra, 0), (extra, 1), (extra, 2), (source, 0), (source, 1)]
    top = sublanes() < 4
    lower, upper = [], []
    for x in range(4):
        for f in range(0, 8, 2):
            a, b = refs[f][0][refs[f][1], x], refs[f + 1][0][refs[f + 1][1], x]
            lower.append(jnp.where(top, a, sink(b, 4)))
            upper.append(jnp.where(top, sink(a, 4), b))
    empty = jnp.zeros((24, 128), f32)
    last = []
    for x in range(4):
        last += [membrane[x], empty]
    lower, upper, last = (jnp.concatenate(part, 0).T for part in (lower, upper, last))
    near = (lanes() % 32) < 8
    for j in range(8):
        at = j * ROWS
        out[pl.ds(at, 16), :] = lower[16 * j : 16 * j + 16]
        out[pl.ds(at + 16, 8), :] = jnp.where(
            near, last[16 * j : 16 * j + 8], turn(last[16 * j + 8 : 16 * j + 16], 8)
        )
        out[pl.ds(at + 24, 16), :] = upper[16 * j : 16 * j + 16]


def plane_kernel(main, above, below, above2, below2, out, first, final):
    y = lanes() % 32

    def take(ref, row, height):
        return ref[pl.ds(row, 8, stride=height), :]

    def plane(z):
        v = [
            take(below2, 8 + z, 24),
            take(below, z, ROWS),
            take(below, 24 + z, ROWS),
            take(main, z, ROWS),
            take(main, 24 + z, ROWS),
            take(above, z, ROWS),
            take(above, 24 + z, ROWS),
            take(above2, z, 24),
        ]
        v = swap_blocks(v, 4)
        r, shift = z % 8, 8 * (z // 8)
        m = turn(take(above2, 16 + r, 24), 28 - shift)
        m = jnp.where(y < 28, turn(take(above, 16 + r, ROWS), 20 - shift), m)
        m = jnp.where(y < 20, turn(take(main, 16 + r, ROWS), 12 - shift), m)
        m = jnp.where(y < 12, turn(take(below, 16 + r, ROWS), 4 - shift), m)
        m = jnp.where(y < 4, turn(take(below2, r, 24), -4 - shift), m)
        return v + [m]

    for z in range(FINE):
        for f, value in enumerate(plane(z)):
            out[f, z] = value
    for ref, at in ((first, lambda d: d - 1), (final, lambda d: FINE - d)):
        for d in range(1, SENT + 1):
            near = (y > d) & (y < 31 - d)
            for f in range(FIELDS):
                value = out[f, at(d)]
                if 2 < d < SENT:
                    value = jnp.where(near, value, turn(out[f, at(14 - d)], 16))
                ref[f, d - 1] = value


def x_up(v):
    v = turn(v, -32)
    return jnp.where(lanes() < 96, v, sink(v, -1))


def x_down(v):
    v = turn(v, 32)
    return jnp.where(lanes() >= 32, v, sink(v, 1))


def y_up(v):
    return turn(v, -1)


def y_down(v):
    return turn(v, 1)


def slot_of(r, s):
    if s < 0:
        return UNIQUE + r if r < KRYLOV - 1 else 64 + UNIQUE
    return r * (r + 1) // 2 + s


def cycle_kernel(main, low, high, sums, fields, images, face, inv, ta, tb, halves, parts, acc):
    lane = lanes()
    ix = sublanes() * 4 + lane // 32
    last_x, first_x = ix == 31, ix == 0

    def far(ref, f, d):
        return ref[f, d - 1] if d <= SENT else turn(ref[f, 13 - d], -16)

    def field(f, i):
        if i < DEPTH:
            return far(low, f, DEPTH - i)
        if i < DEPTH + FINE:
            return main[f, i - DEPTH]
        return far(high, f, i - DEPTH - FINE + 1)

    sz = [field(2, 0), field(5, 0)]
    low_z = [None, None]
    for i in range(EXT - 1):
        diagonals = []
        for s in range(2):
            above = field(s * 3 + 2, i + 1)
            up_z = 0.5 * (sz[s] + above)
            face[s * 3 + 2, i] = up_z
            if i > 0:
                sx, sy = field(s * 3, i), field(s * 3 + 1, i)
                up_x = 0.5 * (sx + jnp.where(last_x, 0.0, x_up(sx)))
                low_x = 0.5 * (sx + jnp.where(first_x, 0.0, x_down(sx)))
                up_y = 0.5 * (sy + y_up(sy))
                low_y = 0.5 * (sy + y_down(sy))
                face[s * 3, i] = jnp.where(last_x, 0.0, up_x)
                face[s * 3 + 1, i] = up_y
                diagonals.append(up_x + low_x + up_y + low_y + up_z + low_z[s])
            sz[s], low_z[s] = above, up_z
        if i > 0:
            di, de = diagonals
            m = field(8, i)
            det = m * di + m * de + di * de
            inside = m > 0.0
            scale = jnp.where(inside, 1.0 / jnp.where(inside, det, 1.0), 0.0)
            inv[0, i] = de * scale
            inv[1, i] = m * scale
            inv[2, i] = -di * scale
            inv[3, i] = (m + di) * scale

    block = (lane % 32) // 8

    def compact(planes):
        value = turn(planes[3], 12)
        for j in (2, 1, 0):
            value = jnp.where(block == j, turn(planes[j], 8 * j - 12), value)
        return value

    def remember(r, at, value):
        images[r, at] = value
        halves[0, r, at], halves[1, r, at] = split(value)

    for part in range(2):
        for g in range(FINE // 4):
            remember(0, part * 4 + g, compact([main[6 + part, 4 * g + j] for j in range(4)]))

    buffers = (ta, tb)

    def vector(k, part, i):
        return field(6 + part, i) if k == 0 else buffers[k % 2][part, i]

    for k in range(KRYLOV):

        def blocks(i):
            v, p = vector(k, 0, i), vector(k, 1, i)
            return (inv[0, i] * v + inv[1, i] * p, inv[2, i] * v + inv[3, i] * p), (v, p)

        def spread(s, i, u):
            fx, fy = face[s * 3, i], face[s * 3 + 1, i]
            across = fx * x_up(u[1][s]) + x_down(fx * u[1][s])
            along = fy * y_up(u[1][s]) + y_down(fy * u[1][s])
            deep = face[s * 3 + 2, i] * u[2][s] + face[s * 3 + 2, i - 1] * u[0][s]
            return across + along + deep

        start, end = 2 + k, EXT - 2 - k
        (before, _), (here, t_here) = blocks(start - 1), blocks(start)
        kept = ([], [], [], [])
        for i in range(start, end):
            after, t_after = blocks(i + 1)
            shared = spread(0, i, (before, here, after))
            b = (-shared, -(shared + spread(1, i, (before, here, after))))
            if DEPTH <= i < DEPTH + FINE:
                for part in range(2):
                    kept[part].append(here[part])
                    kept[2 + part].append(t_here[part] + b[part])
                if len(kept[0]) == 4:
                    g = (i - DEPTH) // 4
                    for part in range(2):
                        fields[k, part * 4 + g] = compact(kept[part])
                        remember(k + 1, part * 4 + g, compact(kept[2 + part]))
                    kept = ([], [], [], [])
            if k + 1 < KRYLOV:
                for part in range(2):
                    value = b[part]
                    if k > 0:
                        value = 2.0 * value - vector(k - 1, part, i)
                    buffers[(k + 1) % 2][part, i] = value
            before, here, t_here = here, after, t_after

    parts[...] = jnp.zeros((2048, 128), f32)
    for r in range(1, KRYLOV + 1):
        for s in range(r + 1):
            terms = []
            for at in range(8):
                a, b = images[r, at], images[s, at]
                ah, al, bh, bl = halves[0, r, at], halves[1, r, at], halves[0, s, at], halves[1, s, at]
                p = a * b
                terms.append((p, ((ah * bh - p) + ah * bl + al * bh) + al * bl))
            value = total_of(terms)
            slot = slot_of(r - 1, s - 1) * 8
            parts[pl.ds(slot, 8), :] = value[0]
            parts[pl.ds(1024 + slot, 8), :] = value[1]

    for group in range(16):
        value = total_of(
            (
                parts[pl.ds(group * 64 + i, 8, stride=8), :],
                parts[pl.ds(1024 + group * 64 + i, 8, stride=8), :],
            )
            for i in range(8)
        )
        acc[0, pl.ds(group * 8, 8), :] = value[0]
        acc[1, pl.ds(group * 8, 8), :] = value[1]
    turned = acc[0].T, acc[1].T
    value = fold_sublanes(
        total_of((turned[0][8 * i : 8 * i + 8], turned[1][8 * i : 8 * i + 8]) for i in range(16))
    )
    whole = (lane < 64) | (lane == 64 + UNIQUE)
    row = jnp.where(whole, value[0], turn(value[1], 64))
    for i in range(sums.shape[0] // 8):
        sums[pl.ds(8 * i, 8), :] = row


def solve_kernel(received, fields, images, out):
    chunk = 8
    groups = received.shape[0] // 8
    value = total_of(
        total_of(
            (received[pl.ds(8 * i, 8), :], jnp.zeros((8, 128), f32))
            for i in range(at, min(at + chunk, groups))
        )
        for at in range(0, groups, chunk)
    )
    high, error = fold_sublanes(value)
    error = error + jnp.where(lanes() < UNIQUE, turn(high, 64), 0.0)
    row, lane = sublanes(16), lanes(16)
    matrix = []
    for n, part in enumerate((high, error)):
        part = jnp.concatenate([part, part], 0)
        value = jnp.zeros((16, 128), f32)
        for r in range(KRYLOV):
            value = jnp.where(row == r, turn(part, -slot_of(r, 0)), value)
        value = jnp.where(lane <= row, value, 0.0)
        flipped = jnp.concatenate([value, jnp.zeros((112, 128), f32)], 0).T[:16]
        value = jnp.where(lane <= row, value, flipped)
        right = jnp.zeros((16, 128), f32)
        for r in range(KRYLOV):
            right = jnp.where(row == r, turn(part, KRYLOV - slot_of(r, -1)), right)
        matrix.append(jnp.where(lane == KRYLOV, right, value))
    matrix = quick_sum(*matrix)
    for j in range(KRYLOV):
        pivot_row = tuple(jnp.broadcast_to(part[j : j + 1, :], (8, 128)) for part in matrix)
        pivot = tuple(jnp.broadcast_to(part[j : j + 1, j : j + 1], (8, 128)) for part in matrix)
        scaled = dd_mul(pivot_row, dd_inverse(pivot))
        scaled = tuple(jnp.concatenate([part, part], 0) for part in scaled)
        column = tuple(-jnp.broadcast_to(part[:, j : j + 1], (16, 128)) for part in matrix)
        rest = dd_add(matrix, dd_mul(column, scaled))
        matrix = tuple(jnp.where(row == j, a, b) for a, b in zip(scaled, rest))
    coeffs = [
        jnp.broadcast_to(matrix[0][k : k + 1, KRYLOV : KRYLOV + 1], (8, 128))
        for k in range(KRYLOV)
    ]
    for g in range(FINE // 4):
        v = []
        for part in range(2):
            v.append(sum(coeffs[k] * fields[k, part * 4 + g] for k in range(KRYLOV)))
        v[0] = v[0] - v[1]
        for part in range(2):
            value = sum(coeffs[k] * images[k + 1, part * 4 + g] for k in range(KRYLOV))
            v.append(images[0, part * 4 + g] - value)
        for j, value in enumerate(swap_blocks(v, 8)):
            out[pl.ds(4 * g + j, 8, stride=FINE), :] = value


def unpack_kernel(received, solution, residual):
    rows = received[...].T
    for f in range(4):
        ref = solution if f < 2 else residual
        for x in range(4):
            ref[f % 2, x] = rows[x * 32 + f * 8 : x * 32 + f * 8 + 8]


def shape(*dims):
    return jax.ShapeDtypeStruct(dims, f32)


def scratch(*dims):
    return pltpu.VMEM(dims, f32)


def body(source, sigma_intra, sigma_extra, membrane):
    nx, ny, nz = (lax.axis_size(a) for a in ("gx", "gy", "gz"))
    packed = pl.pallas_call(pack_kernel, out_shape=shape(8 * ROWS, 128))(
        source, sigma_intra, sigma_extra, membrane
    )
    own = lax.all_to_all(packed.reshape(8, ROWS, 128), "gx", 0, 0, tiled=True)

    def from_y(value, by):
        pairs = [(i, i - by) for i in range(ny) if 0 <= i - by < ny]
        got = lax.ppermute(value, "gy", pairs)
        return got.reshape(-1, 128)

    halo = (from_y(own, 1), from_y(own, -1), from_y(own[:, :24], 2), from_y(own[:, 16:], -2))
    planes, first, final = pl.pallas_call(
        plane_kernel,
        out_shape=(
            shape(FIELDS, FINE, 8, 128),
            shape(FIELDS, SENT, 8, 128),
            shape(FIELDS, SENT, 8, 128),
        ),
    )(own.reshape(-1, 128), *halo)

    def place(c):
        return (c % nx) * nz + c // nx

    up = [(place(c), place(c + 1)) for c in range(nx * nz - 1)]
    low = lax.ppermute(final, ("gx", "gz"), up)
    high = lax.ppermute(first, ("gx", "gz"), [(b, a) for a, b in up])

    sums, fields, images = pl.pallas_call(
        cycle_kernel,
        out_shape=(
            shape(nx * ny * nz, 128),
            shape(KRYLOV, 8, 8, 128),
            shape(KRYLOV + 1, 8, 8, 128),
        ),
        scratch_shapes=[
            scratch(6, EXT, 8, 128),
            scratch(4, EXT, 8, 128),
            scratch(2, EXT, 8, 128),
            scratch(2, EXT, 8, 128),
            scratch(2, KRYLOV + 1, 8, 8, 128),
            scratch(2048, 128),
            scratch(2, 128, 128),
        ],
    )(planes, low, high)

    everyone = ("gx", "gy", "gz")
    got = lax.all_to_all(sums.reshape(-1, 1, 128), everyone, 0, 0, tiled=True)
    result = pl.pallas_call(solve_kernel, out_shape=shape(8 * FINE, 128))(
        got.reshape(-1, 128), fields, images
    )
    result = lax.all_to_all(result.reshape(8, FINE, 128), "gx", 0, 0, tiled=True)
    return pl.pallas_call(
        unpack_kernel,
        out_shape=(shape(2, 4, 8, 128), shape(2, 4, 8, 128)),
    )(result.reshape(-1, 128))


def solution(mesh):
    spread = P(None, "gx", "gy", "gz")
    return jax.shard_map(
        body,
        mesh=mesh,
        in_specs=(spread, spread, spread, P("gx", "gy", "gz")),
        out_specs=(spread, spread),
        check_vma=False,
    )
```

```python
import jax
import jax.numpy as jnp
from jax import lax
from jax.experimental import pallas as pl
from jax.experimental.pallas import tpu as pltpu
from jax.sharding import PartitionSpec as P

KRYLOV = 10
DEPTH = KRYLOV + 1
FINE = 16
EXT = FINE + 2 * DEPTH
SENT = 7
FIELDS = 9
ROWS = 40
UNIQUE = KRYLOV * (KRYLOV + 1) // 2
f32 = jnp.float32


def lanes(rows=8):
    return lax.broadcasted_iota(jnp.int32, (rows, 128), 1)


def sublanes(rows=8):
    return lax.broadcasted_iota(jnp.int32, (rows, 128), 0)


def turn(v, by):
    return v if by % 128 == 0 else pltpu.roll(v, by % 128, 1)


def sink(v, by):
    return pltpu.roll(v, by % 8, 0)


def two_sum(a, b):
    s = a + b
    z = s - a
    return s, (a - (s - z)) + (b - z)


def quick_sum(a, b):
    s = a + b
    return s, b - (s - a)


def split(a):
    c = a * 4097.0
    high = c - (c - a)
    return high, a - high


def two_prod(a, b):
    p = a * b
    ah, al = split(a)
    bh, bl = split(b)
    return p, ((ah * bh - p) + ah * bl + al * bh) + al * bl


def dd_add(a, b):
    s, e = two_sum(a[0], b[0])
    return quick_sum(s, e + (a[1] + b[1]))


def dd_mul(a, b):
    p, e = two_prod(a[0], b[0])
    return quick_sum(p, e + (a[0] * b[1] + a[1] * b[0]))


def dd_inverse(a):
    x = 1.0 / a[0]
    p, e = two_prod(a[0], x)
    return quick_sum(x, x * (((1.0 - p) - e) - a[1] * x))


def add_pairs(a, b):
    s, e = two_sum(a[0], b[0])
    return s, e + (a[1] + b[1])


def total_of(pairs):
    pairs = list(pairs)
    while len(pairs) > 1:
        pairs = [
            add_pairs(pairs[i], pairs[i + 1]) if i + 1 < len(pairs) else pairs[i]
            for i in range(0, len(pairs), 2)
        ]
    return pairs[0]


def fold_sublanes(a):
    for by in (4, 2, 1):
        a = add_pairs(a, (sink(a[0], by), sink(a[1], by)))
    return quick_sum(*a)


def swap_blocks(v, width):
    v = list(v)
    block = lanes() // width
    d = len(v) // 2
    while d >= 1:
        low = (block & d) == 0
        for k in range(len(v)):
            if k & d == 0:
                a, b = v[k], v[k + d]
                v[k] = jnp.where(low, a, turn(b, width * d))
                v[k + d] = jnp.where(low, turn(a, -width * d), b)
        d //= 2
    return v


def pack_kernel(source, intra, extra, membrane, out):
    refs = [(intra, 0), (intra, 1), (intra, 2), (extra, 0), (extra, 1), (extra, 2), (source, 0), (source, 1)]
    top = sublanes() < 4
    lower, upper = [], []
    for x in range(4):
        for f in range(0, 8, 2):
            a, b = refs[f][0][refs[f][1], x], refs[f + 1][0][refs[f + 1][1], x]
            lower.append(jnp.where(top, a, sink(b, 4)))
            upper.append(jnp.where(top, sink(a, 4), b))
    empty = jnp.zeros((24, 128), f32)
    last = []
    for x in range(4):
        last += [membrane[x], empty]
    lower, upper, last = (jnp.concatenate(part, 0).T for part in (lower, upper, last))
    near = (lanes() % 32) < 8
    for j in range(8):
        at = j * ROWS
        out[pl.ds(at, 16), :] = lower[16 * j : 16 * j + 16]
        out[pl.ds(at + 16, 8), :] = jnp.where(
            near, last[16 * j : 16 * j + 8], turn(last[16 * j + 8 : 16 * j + 16], 8)
        )
        out[pl.ds(at + 24, 16), :] = upper[16 * j : 16 * j + 16]


def plane_kernel(main, above, below, above2, below2, out, first, final):
    y = lanes() % 32

    def take(ref, row, height):
        return ref[pl.ds(row, 8, stride=height), :]

    def plane(z):
        v = [
            take(below2, 8 + z, 24),
            take(below, z, ROWS),
            take(below, 24 + z, ROWS),
            take(main, z, ROWS),
            take(main, 24 + z, ROWS),
            take(above, z, ROWS),
            take(above, 24 + z, ROWS),
            take(above2, z, 24),
        ]
        v = swap_blocks(v, 4)
        r, shift = z % 8, 8 * (z // 8)
        m = turn(take(above2, 16 + r, 24), 28 - shift)
        m = jnp.where(y < 28, turn(take(above, 16 + r, ROWS), 20 - shift), m)
        m = jnp.where(y < 20, turn(take(main, 16 + r, ROWS), 12 - shift), m)
        m = jnp.where(y < 12, turn(take(below, 16 + r, ROWS), 4 - shift), m)
        m = jnp.where(y < 4, turn(take(below2, r, 24), -4 - shift), m)
        return v + [m]

    for z in range(FINE):
        for f, value in enumerate(plane(z)):
            out[f, z] = value
    for ref, at in ((first, lambda d: d - 1), (final, lambda d: FINE - d)):
        for d in range(1, SENT + 1):
            near = (y > d) & (y < 31 - d)
            for f in range(FIELDS):
                value = out[f, at(d)]
                if 2 < d < SENT:
                    value = jnp.where(near, value, turn(out[f, at(14 - d)], 16))
                ref[f, d - 1] = value


def x_up(v):
    v = turn(v, -32)
    return jnp.where(lanes() < 96, v, sink(v, -1))


def x_down(v):
    v = turn(v, 32)
    return jnp.where(lanes() >= 32, v, sink(v, 1))


def y_up(v):
    return turn(v, -1)


def y_down(v):
    return turn(v, 1)


def slot_of(r, s):
    if s < 0:
        return UNIQUE + r if r < KRYLOV - 1 else 64 + UNIQUE
    return r * (r + 1) // 2 + s


def cycle_kernel(main, low, high, sums, fields, images, face, inv, ta, tb, halves, parts, acc):
    lane = lanes()
    ix = sublanes() * 4 + lane // 32
    last_x, first_x = ix == 31, ix == 0

    def far(ref, f, d):
        return ref[f, d - 1] if d <= SENT else turn(ref[f, 13 - d], -16)

    def field(f, i):
        if i < DEPTH:
            return far(low, f, DEPTH - i)
        if i < DEPTH + FINE:
            return main[f, i - DEPTH]
        return far(high, f, i - DEPTH - FINE + 1)

    sz = [field(2, 0), field(5, 0)]
    low_z = [None, None]
    for i in range(EXT - 1):
        diagonals = []
        for s in range(2):
            above = field(s * 3 + 2, i + 1)
            up_z = 0.5 * (sz[s] + above)
            face[s * 3 + 2, i] = up_z
            if i > 0:
                sx, sy = field(s * 3, i), field(s * 3 + 1, i)
                up_x = 0.5 * (sx + jnp.where(last_x, 0.0, x_up(sx)))
                low_x = 0.5 * (sx + jnp.where(first_x, 0.0, x_down(sx)))
                up_y = 0.5 * (sy + y_up(sy))
                low_y = 0.5 * (sy + y_down(sy))
                face[s * 3, i] = jnp.where(last_x, 0.0, up_x)
                face[s * 3 + 1, i] = up_y
                diagonals.append(up_x + low_x + up_y + low_y + up_z + low_z[s])
            sz[s], low_z[s] = above, up_z
        if i > 0:
            di, de = diagonals
            m = field(8, i)
            det = m * di + m * de + di * de
            inside = m > 0.0
            scale = jnp.where(inside, 1.0 / jnp.where(inside, det, 1.0), 0.0)
            inv[0, i] = de * scale
            inv[1, i] = m * scale
            inv[2, i] = -di * scale
            inv[3, i] = (m + di) * scale

    block = (lane % 32) // 8

    def compact(planes):
        value = turn(planes[3], 12)
        for j in (2, 1, 0):
            value = jnp.where(block == j, turn(planes[j], 8 * j - 12), value)
        return value

    def remember(r, at, value):
        images[r, at] = value
        halves[0, r, at], halves[1, r, at] = split(value)

    for part in range(2):
        for g in range(FINE // 4):
            remember(0, part * 4 + g, compact([main[6 + part, 4 * g + j] for j in range(4)]))

    buffers = (ta, tb)

    def vector(k, part, i):
        return field(6 + part, i) if k == 0 else buffers[k % 2][part, i]

    for k in range(KRYLOV):

        def blocks(i):
            v, p = vector(k, 0, i), vector(k, 1, i)
            return (inv[0, i] * v + inv[1, i] * p, inv[2, i] * v + inv[3, i] * p), (v, p)

        def spread(s, i, u):
            fx, fy = face[s * 3, i], face[s * 3 + 1, i]
            across = fx * x_up(u[1][s]) + x_down(fx * u[1][s])
            along = fy * y_up(u[1][s]) + y_down(fy * u[1][s])
            deep = face[s * 3 + 2, i] * u[2][s] + face[s * 3 + 2, i - 1] * u[0][s]
            return across + along + deep

        start, end = 2 + k, EXT - 2 - k
        (before, _), (here, t_here) = blocks(start - 1), blocks(start)
        kept = ([], [], [], [])
        for i in range(start, end):
            after, t_after = blocks(i + 1)
            shared = spread(0, i, (before, here, after))
            b = (-shared, -(shared + spread(1, i, (before, here, after))))
            if DEPTH <= i < DEPTH + FINE:
                for part in range(2):
                    kept[part].append(here[part])
                    kept[2 + part].append(t_here[part] + b[part])
                if len(kept[0]) == 4:
                    g = (i - DEPTH) // 4
                    for part in range(2):
                        fields[k, part * 4 + g] = compact(kept[part])
                        remember(k + 1, part * 4 + g, compact(kept[2 + part]))
                    kept = ([], [], [], [])
            if k + 1 < KRYLOV:
                for part in range(2):
                    value = b[part]
                    if k > 0:
                        value = 2.0 * value - vector(k - 1, part, i)
                    buffers[(k + 1) % 2][part, i] = value
            before, here, t_here = here, after, t_after

    parts[...] = jnp.zeros((2048, 128), f32)
    for r in range(1, KRYLOV + 1):
        for s in range(r + 1):
            terms = []
            for at in range(8):
                a, b = images[r, at], images[s, at]
                ah, al, bh, bl = halves[0, r, at], halves[1, r, at], halves[0, s, at], halves[1, s, at]
                p = a * b
                terms.append((p, ((ah * bh - p) + ah * bl + al * bh) + al * bl))
            value = total_of(terms)
            slot = slot_of(r - 1, s - 1) * 8
            parts[pl.ds(slot, 8), :] = value[0]
            parts[pl.ds(1024 + slot, 8), :] = value[1]

    for group in range(16):
        value = total_of(
            (
                parts[pl.ds(group * 64 + i, 8, stride=8), :],
                parts[pl.ds(1024 + group * 64 + i, 8, stride=8), :],
            )
            for i in range(8)
        )
        acc[0, pl.ds(group * 8, 8), :] = value[0]
        acc[1, pl.ds(group * 8, 8), :] = value[1]
    turned = acc[0].T, acc[1].T
    value = fold_sublanes(
        total_of((turned[0][8 * i : 8 * i + 8], turned[1][8 * i : 8 * i + 8]) for i in range(16))
    )
    whole = (lane < 64) | (lane == 64 + UNIQUE)
    row = jnp.where(whole, value[0], turn(value[1], 64))
    for i in range(sums.shape[0] // 8):
        sums[pl.ds(8 * i, 8), :] = row


def solve_kernel(received, fields, images, out):
    chunk = 8
    groups = received.shape[0] // 8
    value = total_of(
        total_of(
            (received[pl.ds(8 * i, 8), :], jnp.zeros((8, 128), f32))
            for i in range(at, min(at + chunk, groups))
        )
        for at in range(0, groups, chunk)
    )
    high, error = fold_sublanes(value)
    error = error + jnp.where(lanes() < UNIQUE, turn(high, 64), 0.0)
    row, lane = sublanes(16), lanes(16)
    matrix = []
    for n, part in enumerate((high, error)):
        part = jnp.concatenate([part, part], 0)
        value = jnp.zeros((16, 128), f32)
        for r in range(KRYLOV):
            value = jnp.where(row == r, turn(part, -slot_of(r, 0)), value)
        value = jnp.where(lane <= row, value, 0.0)
        flipped = jnp.concatenate([value, jnp.zeros((112, 128), f32)], 0).T[:16]
        value = jnp.where(lane <= row, value, flipped)
        right = jnp.zeros((16, 128), f32)
        for r in range(KRYLOV):
            right = jnp.where(row == r, turn(part, KRYLOV - slot_of(r, -1)), right)
        matrix.append(jnp.where(lane == KRYLOV, right, value))
    matrix = quick_sum(*matrix)
    for j in range(KRYLOV):
        pivot_row = tuple(jnp.broadcast_to(part[j : j + 1, :], (8, 128)) for part in matrix)
        pivot = tuple(jnp.broadcast_to(part[j : j + 1, j : j + 1], (8, 128)) for part in matrix)
        scaled = dd_mul(pivot_row, dd_inverse(pivot))
        scaled = tuple(jnp.concatenate([part, part], 0) for part in scaled)
        column = tuple(-jnp.broadcast_to(part[:, j : j + 1], (16, 128)) for part in matrix)
        rest = dd_add(matrix, dd_mul(column, scaled))
        matrix = tuple(jnp.where(row == j, a, b) for a, b in zip(scaled, rest))
    coeffs = [
        jnp.broadcast_to(matrix[0][k : k + 1, KRYLOV : KRYLOV + 1], (8, 128))
        for k in range(KRYLOV)
    ]
    for g in range(FINE // 4):
        v = []
        for part in range(2):
            v.append(sum(coeffs[k] * fields[k, part * 4 + g] for k in range(KRYLOV)))
        v[0] = v[0] - v[1]
        for part in range(2):
            value = sum(coeffs[k] * images[k + 1, part * 4 + g] for k in range(KRYLOV))
            v.append(images[0, part * 4 + g] - value)
        for j, value in enumerate(swap_blocks(v, 8)):
            out[pl.ds(4 * g + j, 8, stride=FINE), :] = value


def unpack_kernel(received, solution, residual):
    rows = received[...].T
    for f in range(4):
        ref = solution if f < 2 else residual
        for x in range(4):
            ref[f % 2, x] = rows[x * 32 + f * 8 : x * 32 + f * 8 + 8]


def shape(*dims):
    return jax.ShapeDtypeStruct(dims, f32)


def held(*dims):
    return pltpu.VMEM(dims, f32)


def near(*values):
    return tuple(pltpu.with_memory_space_constraint(v, pltpu.VMEM) for v in values)


def scratch(*dims):
    return pltpu.VMEM(dims, f32)


def body(source, sigma_intra, sigma_extra, membrane):
    nx, ny, nz = (lax.axis_size(a) for a in ("gx", "gy", "gz"))
    packed = pl.pallas_call(pack_kernel, out_shape=held(8 * ROWS, 128))(
        source, sigma_intra, sigma_extra, membrane
    )
    own = lax.all_to_all(packed.reshape(8, ROWS, 128), "gx", 0, 0, tiled=True)

    def from_y(value, by):
        pairs = [(i, i - by) for i in range(ny) if 0 <= i - by < ny]
        got = lax.ppermute(value, "gy", pairs)
        return got.reshape(-1, 128)

    halo = (from_y(own, 1), from_y(own, -1), from_y(own[:, :24], 2), from_y(own[:, 16:], -2))
    planes, first, final = pl.pallas_call(
        plane_kernel,
        out_shape=(
            held(FIELDS, FINE, 8, 128),
            held(FIELDS, SENT, 8, 128),
            held(FIELDS, SENT, 8, 128),
        ),
    )(*near(own.reshape(-1, 128), *halo))

    def place(c):
        return (c % nx) * nz + c // nx

    up = [(place(c), place(c + 1)) for c in range(nx * nz - 1)]
    low = lax.ppermute(final, ("gx", "gz"), up)
    high = lax.ppermute(first, ("gx", "gz"), [(b, a) for a, b in up])

    sums, fields, images = pl.pallas_call(
        cycle_kernel,
        out_shape=(
            held(nx * ny * nz, 128),
            held(KRYLOV, 8, 8, 128),
            held(KRYLOV + 1, 8, 8, 128),
        ),
        scratch_shapes=[
            scratch(6, EXT, 8, 128),
            scratch(4, EXT, 8, 128),
            scratch(2, EXT, 8, 128),
            scratch(2, EXT, 8, 128),
            scratch(2, KRYLOV + 1, 8, 8, 128),
            scratch(2048, 128),
            scratch(2, 128, 128),
        ],
    )(*near(planes, low, high))

    everyone = ("gx", "gy", "gz")
    got = lax.all_to_all(sums.reshape(-1, 1, 128), everyone, 0, 0, tiled=True)
    result = pl.pallas_call(solve_kernel, out_shape=held(8 * FINE, 128))(
        *near(got.reshape(-1, 128), fields, images)
    )
    result = lax.all_to_all(result.reshape(8, FINE, 128), "gx", 0, 0, tiled=True)
    return pl.pallas_call(
        unpack_kernel,
        out_shape=(shape(2, 4, 8, 128), shape(2, 4, 8, 128)),
    )(*near(result.reshape(-1, 128)))


def solution(mesh):
    spread = P(None, "gx", "gy", "gz")
    return jax.shard_map(
        body,
        mesh=mesh,
        in_specs=(spread, spread, spread, P("gx", "gy", "gz")),
        out_specs=(spread, spread),
        check_vma=False,
    )
```

```python
import jax
import jax.numpy as jnp
from jax import lax
from jax.experimental import pallas as pl
from jax.experimental.pallas import tpu as pltpu
from jax.sharding import PartitionSpec as P

KRYLOV = 10
DEPTH = KRYLOV + 1
FINE = 16
EXT = FINE + 2 * DEPTH
SENT = 7
FIELDS = 9
ROWS = 40
BACK = 104
SUMS = 4 * (2 * KRYLOV + 5)
UNIQUE = KRYLOV * (KRYLOV + 1) // 2
f32 = jnp.float32


def lanes(rows=8):
    return lax.broadcasted_iota(jnp.int32, (rows, 128), 1)


def sublanes(rows=8):
    return lax.broadcasted_iota(jnp.int32, (rows, 128), 0)


def turn(v, by):
    return v if by % 128 == 0 else pltpu.roll(v, by % 128, 1)


def sink(v, by):
    return pltpu.roll(v, by % 8, 0)


def two_sum(a, b):
    s = a + b
    z = s - a
    return s, (a - (s - z)) + (b - z)


def quick_sum(a, b):
    s = a + b
    return s, b - (s - a)


def split(a):
    c = a * 4097.0
    high = c - (c - a)
    return high, a - high


def two_prod(a, b):
    p = a * b
    ah, al = split(a)
    bh, bl = split(b)
    return p, ((ah * bh - p) + ah * bl + al * bh) + al * bl


def dd_add(a, b):
    s, e = two_sum(a[0], b[0])
    return quick_sum(s, e + (a[1] + b[1]))


def dd_mul(a, b):
    p, e = two_prod(a[0], b[0])
    return quick_sum(p, e + (a[0] * b[1] + a[1] * b[0]))


def dd_inverse(a):
    x = 1.0 / a[0]
    p, e = two_prod(a[0], x)
    return quick_sum(x, x * (((1.0 - p) - e) - a[1] * x))


def add_pairs(a, b):
    s, e = two_sum(a[0], b[0])
    return s, e + (a[1] + b[1])


def total_of(pairs):
    pairs = list(pairs)
    while len(pairs) > 1:
        pairs = [
            add_pairs(pairs[i], pairs[i + 1]) if i + 1 < len(pairs) else pairs[i]
            for i in range(0, len(pairs), 2)
        ]
    return pairs[0]


def fold_sublanes(a):
    for by in (4, 2, 1):
        a = add_pairs(a, (sink(a[0], by), sink(a[1], by)))
    return quick_sum(*a)


def swap_blocks(v, width):
    v = list(v)
    block = lanes() // width
    d = len(v) // 2
    while d >= 1:
        low = (block & d) == 0
        for k in range(len(v)):
            if k & d == 0:
                a, b = v[k], v[k + d]
                v[k] = jnp.where(low, a, turn(b, width * d))
                v[k + d] = jnp.where(low, turn(a, -width * d), b)
        d //= 2
    return v


def pack_kernel(source, intra, extra, membrane, out):
    refs = [(intra, 0), (intra, 1), (intra, 2), (extra, 0), (extra, 1), (extra, 2), (source, 0), (source, 1)]
    top = sublanes() < 4
    lower, upper = [], []
    for x in range(4):
        for f in range(0, 8, 2):
            a, b = refs[f][0][refs[f][1], x], refs[f + 1][0][refs[f + 1][1], x]
            lower.append(jnp.where(top, a, sink(b, 4)))
            upper.append(jnp.where(top, sink(a, 4), b))
    empty = jnp.zeros((24, 128), f32)
    last = []
    for x in range(4):
        last += [membrane[x], empty]
    lower, upper, last = (jnp.concatenate(part, 0).T for part in (lower, upper, last))
    near = (lanes() % 32) < 8
    for j in range(8):
        at = j * ROWS
        out[pl.ds(at, 16), :] = lower[16 * j : 16 * j + 16]
        out[pl.ds(at + 16, 8), :] = jnp.where(
            near, last[16 * j : 16 * j + 8], turn(last[16 * j + 8 : 16 * j + 16], 8)
        )
        out[pl.ds(at + 24, 16), :] = upper[16 * j : 16 * j + 16]


def plane_kernel(main, above, below, above2, below2, out, first, final):
    y = lanes() % 32

    def take(ref, row, height):
        return ref[pl.ds(row, 8, stride=height), :]

    def plane(z):
        v = [
            take(below2, 8 + z, 24),
            take(below, z, ROWS),
            take(below, 24 + z, ROWS),
            take(main, z, ROWS),
            take(main, 24 + z, ROWS),
            take(above, z, ROWS),
            take(above, 24 + z, ROWS),
            take(above2, z, 24),
        ]
        v = swap_blocks(v, 4)
        r, shift = z % 8, 8 * (z // 8)
        m = turn(take(above2, 16 + r, 24), 28 - shift)
        m = jnp.where(y < 28, turn(take(above, 16 + r, ROWS), 20 - shift), m)
        m = jnp.where(y < 20, turn(take(main, 16 + r, ROWS), 12 - shift), m)
        m = jnp.where(y < 12, turn(take(below, 16 + r, ROWS), 4 - shift), m)
        m = jnp.where(y < 4, turn(take(below2, r, 24), -4 - shift), m)
        return v + [m]

    for z in range(FINE):
        for f, value in enumerate(plane(z)):
            out[f, z] = value
    for ref, at in ((first, lambda d: d - 1), (final, lambda d: FINE - d)):
        for d in range(1, SENT + 1):
            near = (y > d) & (y < 31 - d)
            for f in range(FIELDS):
                value = out[f, at(d)]
                if 2 < d < SENT:
                    value = jnp.where(near, value, turn(out[f, at(14 - d)], 16))
                ref[f, d - 1] = value


def x_up(v):
    v = turn(v, -32)
    return jnp.where(lanes() < 96, v, sink(v, -1))


def x_down(v):
    v = turn(v, 32)
    return jnp.where(lanes() >= 32, v, sink(v, 1))


def y_up(v):
    return turn(v, -1)


def y_down(v):
    return turn(v, 1)


def slot_of(r, s):
    if s < 0:
        return UNIQUE + r if r < KRYLOV - 1 else 64 + UNIQUE
    return r * (r + 1) // 2 + s


def cycle_kernel(main, low, high, sums, back, face, inv, ta, tb, images, halves, parts, acc):
    lane = lanes()
    ix = sublanes() * 4 + lane // 32
    last_x, first_x = ix == 31, ix == 0

    def far(ref, f, d):
        return ref[f, d - 1] if d <= SENT else turn(ref[f, 13 - d], -16)

    def field(f, i):
        if i < DEPTH:
            return far(low, f, DEPTH - i)
        if i < DEPTH + FINE:
            return main[f, i - DEPTH]
        return far(high, f, i - DEPTH - FINE + 1)

    block = (lane % 32) // 8

    def compact(planes):
        value = turn(planes[3], 12)
        for j in (2, 1, 0):
            value = jnp.where(block == j, turn(planes[j], 8 * j - 12), value)
        return value

    def send_back(array, g, planes):
        back[pl.ds(array * 4 + g, 8, stride=BACK), :] = compact(planes)

    blocks_kept = ([], [], [])
    sz = [field(2, 0), field(5, 0)]
    low_z = [None, None]
    for i in range(EXT - 1):
        diagonals = []
        for s in range(2):
            above = field(s * 3 + 2, i + 1)
            up_z = 0.5 * (sz[s] + above)
            face[s * 3 + 2, i] = up_z
            if i > 0:
                sx, sy = field(s * 3, i), field(s * 3 + 1, i)
                up_x = 0.5 * (sx + jnp.where(last_x, 0.0, x_up(sx)))
                low_x = 0.5 * (sx + jnp.where(first_x, 0.0, x_down(sx)))
                up_y = 0.5 * (sy + y_up(sy))
                low_y = 0.5 * (sy + y_down(sy))
                face[s * 3, i] = jnp.where(last_x, 0.0, up_x)
                face[s * 3 + 1, i] = up_y
                diagonals.append(up_x + low_x + up_y + low_y + up_z + low_z[s])
            sz[s], low_z[s] = above, up_z
        if i > 0:
            di, de = diagonals
            m = field(8, i)
            det = m * di + m * de + di * de
            inside = m > 0.0
            scale = jnp.where(inside, 1.0 / jnp.where(inside, det, 1.0), 0.0)
            inv[0, i] = de * scale
            inv[1, i] = m * scale
            inv[2, i] = -di * scale
            inv[3, i] = (m + di) * scale
            if DEPTH <= i < DEPTH + FINE:
                for n, value in enumerate(((di + de) * scale, -di * scale, (m + di) * scale)):
                    blocks_kept[n].append(value)
                if len(blocks_kept[0]) == 4:
                    for n in range(3):
                        send_back(2 * KRYLOV + 2 + n, (i - DEPTH) // 4, blocks_kept[n])
                    blocks_kept = ([], [], [])

    def remember(r, at, value):
        images[r, at] = value
        halves[0, r, at], halves[1, r, at] = split(value)

    for part in range(2):
        for g in range(FINE // 4):
            planes = [main[6 + part, 4 * g + j] for j in range(4)]
            remember(0, part * 4 + g, compact(planes))
            send_back(part, g, planes)

    buffers = (ta, tb)

    def vector(k, part, i):
        return field(6 + part, i) if k == 0 else buffers[k % 2][part, i]

    for k in range(KRYLOV):

        def blocks(i):
            v, p = vector(k, 0, i), vector(k, 1, i)
            return (inv[0, i] * v + inv[1, i] * p, inv[2, i] * v + inv[3, i] * p), (v, p)

        def spread(s, i, u):
            fx, fy = face[s * 3, i], face[s * 3 + 1, i]
            across = fx * x_up(u[1][s]) + x_down(fx * u[1][s])
            along = fy * y_up(u[1][s]) + y_down(fy * u[1][s])
            deep = face[s * 3 + 2, i] * u[2][s] + face[s * 3 + 2, i - 1] * u[0][s]
            return across + along + deep

        start, end = 2 + k, EXT - 2 - k
        (before, _), (here, t_here) = blocks(start - 1), blocks(start)
        kept = ([], [], [], [])
        for i in range(start, end):
            after, t_after = blocks(i + 1)
            shared = spread(0, i, (before, here, after))
            b = (-shared, -(shared + spread(1, i, (before, here, after))))
            if DEPTH <= i < DEPTH + FINE:
                for part in range(2):
                    kept[part].append(t_here[part] + b[part])
            for part in range(2):
                value = b[part]
                if k > 0:
                    value = 2.0 * value - vector(k - 1, part, i)
                if k + 1 < KRYLOV:
                    buffers[(k + 1) % 2][part, i] = value
                if DEPTH <= i < DEPTH + FINE:
                    kept[2 + part].append(value)
            if len(kept[0]) == 4:
                g = (i - DEPTH) // 4
                for part in range(2):
                    remember(k + 1, part * 4 + g, compact(kept[part]))
                    send_back(2 * k + 2 + part, g, kept[2 + part])
                kept = ([], [], [], [])
            before, here, t_here = here, after, t_after

    parts[...] = jnp.zeros((2048, 128), f32)
    for r in range(1, KRYLOV + 1):
        for s in range(r + 1):
            terms = []
            for at in range(8):
                a, b = images[r, at], images[s, at]
                ah, al, bh, bl = halves[0, r, at], halves[1, r, at], halves[0, s, at], halves[1, s, at]
                p = a * b
                terms.append((p, ((ah * bh - p) + ah * bl + al * bh) + al * bl))
            value = total_of(terms)
            slot = slot_of(r - 1, s - 1) * 8
            parts[pl.ds(slot, 8), :] = value[0]
            parts[pl.ds(1024 + slot, 8), :] = value[1]

    for group in range(16):
        value = total_of(
            (
                parts[pl.ds(group * 64 + i, 8, stride=8), :],
                parts[pl.ds(1024 + group * 64 + i, 8, stride=8), :],
            )
            for i in range(8)
        )
        acc[0, pl.ds(group * 8, 8), :] = value[0]
        acc[1, pl.ds(group * 8, 8), :] = value[1]
    turned = acc[0].T, acc[1].T
    value = fold_sublanes(
        total_of((turned[0][8 * i : 8 * i + 8], turned[1][8 * i : 8 * i + 8]) for i in range(16))
    )
    row = jnp.where(is_high(), value[0], turn(value[1], 64))
    for i in range(sums.shape[0] // 8):
        sums[pl.ds(8 * i, 8), :] = row


def is_high():
    return (lanes() < 64) | (lanes() == 64 + UNIQUE)


def low_words(error):
    return turn(jnp.where(lanes() < UNIQUE, error, 0.0), 64)


def sum_kernel(received, _, back):
    zero = jnp.zeros((8, 128), f32)
    groups = range(received.shape[0] // 8)
    high, error = fold_sublanes(total_of((received[pl.ds(8 * i, 8), :], zero) for i in groups))
    row = jnp.where(is_high(), high, high + low_words(error))
    back[pl.ds(SUMS, 8, stride=BACK), :] = row


def solve_kernel(received, solution, residual, rows):
    def take(array, g):
        return received[pl.ds(array * 4 + g, 8, stride=BACK), :]

    zero = jnp.zeros((8, 128), f32)
    high, error = fold_sublanes((received[pl.ds(SUMS, 8, stride=BACK), :], zero))
    error = jnp.where(lanes() < UNIQUE, error + turn(high, 64), error)
    row, lane = sublanes(16), lanes(16)
    matrix = []
    for n, part in enumerate((high, error)):
        part = jnp.concatenate([part, part], 0)
        value = jnp.zeros((16, 128), f32)
        for r in range(KRYLOV):
            value = jnp.where(row == r, turn(part, -slot_of(r, 0)), value)
        value = jnp.where(lane <= row, value, 0.0)
        flipped = jnp.concatenate([value, jnp.zeros((112, 128), f32)], 0).T[:16]
        value = jnp.where(lane <= row, value, flipped)
        right = jnp.zeros((16, 128), f32)
        for r in range(KRYLOV):
            right = jnp.where(row == r, turn(part, KRYLOV - slot_of(r, -1)), right)
        matrix.append(jnp.where(lane == KRYLOV, right, value))
    matrix = quick_sum(*matrix)
    for j in range(KRYLOV):
        pivot_row = tuple(jnp.broadcast_to(part[j : j + 1, :], (8, 128)) for part in matrix)
        pivot = tuple(jnp.broadcast_to(part[j : j + 1, j : j + 1], (8, 128)) for part in matrix)
        scaled = dd_mul(pivot_row, dd_inverse(pivot))
        scaled = tuple(jnp.concatenate([part, part], 0) for part in scaled)
        column = tuple(-jnp.broadcast_to(part[:, j : j + 1], (16, 128)) for part in matrix)
        rest = dd_add(matrix, dd_mul(column, scaled))
        matrix = tuple(jnp.where(row == j, a, b) for a, b in zip(scaled, rest))
    coeffs = [
        jnp.broadcast_to(matrix[0][k : k + 1, KRYLOV : KRYLOV + 1], (8, 128))
        for k in range(KRYLOV)
    ]
    image = [y for y in coeffs] + [jnp.zeros((8, 128), f32)]
    for k in range(KRYLOV):
        image[k + 1] = image[k + 1] + (coeffs[k] if k == 0 else 0.5 * coeffs[k])
        if k > 0:
            image[k - 1] = image[k - 1] + 0.5 * coeffs[k]
    image[0] = image[0] - 1.0
    for g in range(FINE // 4):
        combined, left = [], []
        for part in range(2):
            vectors = [take(2 * m + part, g) for m in range(KRYLOV + 1)]
            combined.append(sum(coeffs[k] * vectors[k] for k in range(KRYLOV)))
            left.append(-sum(image[m] * vectors[m] for m in range(KRYLOV + 1)))
        b = [take(2 * KRYLOV + 2 + n, g) for n in range(3)]
        v = [
            b[0] * combined[0] + b[1] * combined[1],
            b[1] * combined[0] + b[2] * combined[1],
        ]
        for j, value in enumerate(swap_blocks(v + left, 8)):
            rows[pl.ds(4 * g + j, 8, stride=FINE), :] = value
    turned = rows[...].T
    for f in range(4):
        ref = solution if f < 2 else residual
        for x in range(4):
            ref[f % 2, x] = turned[x * 32 + f * 8 : x * 32 + f * 8 + 8]


def shape(*dims):
    return jax.ShapeDtypeStruct(dims, f32)


def held(*dims):
    return pltpu.VMEM(dims, f32)


def near(*values):
    return tuple(pltpu.with_memory_space_constraint(v, pltpu.VMEM) for v in values)


def scratch(*dims):
    return pltpu.VMEM(dims, f32)


def body(source, sigma_intra, sigma_extra, membrane):
    nx, ny, nz = (lax.axis_size(a) for a in ("gx", "gy", "gz"))
    packed = pl.pallas_call(pack_kernel, out_shape=held(8 * ROWS, 128))(
        source, sigma_intra, sigma_extra, membrane
    )
    own = lax.all_to_all(packed.reshape(8, ROWS, 128), "gx", 0, 0, tiled=True)

    def from_y(value, by):
        pairs = [(i, i - by) for i in range(ny) if 0 <= i - by < ny]
        got = lax.ppermute(value, "gy", pairs)
        return got.reshape(-1, 128)

    halo = (from_y(own, 1), from_y(own, -1), from_y(own[:, :24], 2), from_y(own[:, 16:], -2))
    planes, first, final = pl.pallas_call(
        plane_kernel,
        out_shape=(
            held(FIELDS, FINE, 8, 128),
            held(FIELDS, SENT, 8, 128),
            held(FIELDS, SENT, 8, 128),
        ),
    )(*near(own.reshape(-1, 128), *halo))

    def place(c):
        return (c % nx) * nz + c // nx

    up = [(place(c), place(c + 1)) for c in range(nx * nz - 1)]
    low = lax.ppermute(final, ("gx", "gz"), up)
    high = lax.ppermute(first, ("gx", "gz"), [(b, a) for a, b in up])

    sums, back = pl.pallas_call(
        cycle_kernel,
        out_shape=(held(ny * nz, 128), held(8 * BACK, 128)),
        scratch_shapes=[
            scratch(6, EXT, 8, 128),
            scratch(4, EXT, 8, 128),
            scratch(2, EXT, 8, 128),
            scratch(2, EXT, 8, 128),
            scratch(KRYLOV + 1, 8, 8, 128),
            scratch(2, KRYLOV + 1, 8, 8, 128),
            scratch(2048, 128),
            scratch(2, 128, 128),
        ],
    )(*near(planes, low, high))

    got = lax.all_to_all(sums.reshape(-1, 1, 128), ("gy", "gz"), 0, 0, tiled=True)
    back = pl.pallas_call(
        sum_kernel, out_shape=held(8 * BACK, 128), input_output_aliases={1: 0}
    )(*near(got.reshape(-1, 128), back))
    got = lax.all_to_all(back.reshape(8, BACK, 128), "gx", 0, 0, tiled=True)
    return pl.pallas_call(
        solve_kernel,
        out_shape=(shape(2, 4, 8, 128), shape(2, 4, 8, 128)),
        scratch_shapes=[scratch(128, 128)],
    )(*near(got.reshape(-1, 128)))


def solution(mesh):
    spread = P(None, "gx", "gy", "gz")
    return jax.shard_map(
        body,
        mesh=mesh,
        in_specs=(spread, spread, spread, P("gx", "gy", "gz")),
        out_specs=(spread, spread),
        check_vma=False,
    )
```

```python
import jax
import jax.numpy as jnp
from jax import lax
from jax.experimental import pallas as pl
from jax.experimental.pallas import tpu as pltpu
from jax.sharding import PartitionSpec as P

KRYLOV = 10
DEPTH = KRYLOV + 1
FINE = 16
EXT = FINE + 2 * DEPTH
SENT = 7
FIELDS = 9
ROWS = 36
BACK = 101
SUMS = 4 * (2 * KRYLOV + 5)
UNIQUE = KRYLOV * (KRYLOV + 1) // 2
f32 = jnp.float32


def lanes(rows=8):
    return lax.broadcasted_iota(jnp.int32, (rows, 128), 1)


def sublanes(rows=8):
    return lax.broadcasted_iota(jnp.int32, (rows, 128), 0)


def turn(v, by):
    return v if by % 128 == 0 else pltpu.roll(v, by % 128, 1)


def sink(v, by):
    return pltpu.roll(v, by % 8, 0)


def two_sum(a, b):
    s = a + b
    z = s - a
    return s, (a - (s - z)) + (b - z)


def quick_sum(a, b):
    s = a + b
    return s, b - (s - a)


def split(a):
    c = a * 4097.0
    high = c - (c - a)
    return high, a - high


def two_prod(a, b):
    p = a * b
    ah, al = split(a)
    bh, bl = split(b)
    return p, ((ah * bh - p) + ah * bl + al * bh) + al * bl


def dd_add(a, b):
    s, e = two_sum(a[0], b[0])
    return quick_sum(s, e + (a[1] + b[1]))


def dd_mul(a, b):
    p, e = two_prod(a[0], b[0])
    return quick_sum(p, e + (a[0] * b[1] + a[1] * b[0]))


def dd_inverse(a):
    x = 1.0 / a[0]
    p, e = two_prod(a[0], x)
    return quick_sum(x, x * (((1.0 - p) - e) - a[1] * x))


def add_pairs(a, b):
    s, e = two_sum(a[0], b[0])
    return s, e + (a[1] + b[1])


def total_of(pairs):
    pairs = list(pairs)
    while len(pairs) > 1:
        pairs = [
            add_pairs(pairs[i], pairs[i + 1]) if i + 1 < len(pairs) else pairs[i]
            for i in range(0, len(pairs), 2)
        ]
    return pairs[0]


def fold_sublanes(a):
    for by in (4, 2, 1):
        a = add_pairs(a, (sink(a[0], by), sink(a[1], by)))
    return quick_sum(*a)


def merge(a, b, d):
    low = (sublanes() & d) == 0
    return add_pairs(
        tuple(jnp.where(low, x, y) for x, y in zip(a, b)),
        tuple(jnp.where(low, sink(x, -d), sink(y, d)) for x, y in zip(a, b)),
    )


def swap_blocks(v, width):
    v = list(v)
    block = lanes() // width
    d = len(v) // 2
    while d >= 1:
        low = (block & d) == 0
        for k in range(len(v)):
            if k & d == 0:
                a, b = v[k], v[k + d]
                v[k] = jnp.where(low, a, turn(b, width * d))
                v[k + d] = jnp.where(low, turn(a, -width * d), b)
        d //= 2
    return v


def pack_kernel(source, intra, extra, membrane, out):
    refs = [(intra, 0), (intra, 1), (intra, 2), (extra, 0), (extra, 1), (extra, 2), (source, 0), (source, 1)]
    top = sublanes() < 4
    lower, upper = [], []
    for x in range(4):
        for f in range(0, 8, 2):
            a, b = refs[f][0][refs[f][1], x], refs[f + 1][0][refs[f + 1][1], x]
            lower.append(jnp.where(top, a, sink(b, 4)))
            upper.append(jnp.where(top, sink(a, 4), b))
    empty = jnp.zeros((24, 128), f32)
    last = []
    for x in range(4):
        last += [membrane[x], empty]
    lower, upper, last = (jnp.concatenate(part, 0).T for part in (lower, upper, last))
    group = (lanes() % 32) // 8
    for j in range(8):
        at = j * ROWS
        a, b = last[16 * j : 16 * j + 8], last[16 * j + 8 : 16 * j + 16]
        m = jnp.where(group == 2, turn(b, 16), turn(sink(b, 4), 24))
        m = jnp.where(group == 1, turn(sink(a, 4), 8), m)
        m = jnp.where(group == 0, a, m)
        out[pl.ds(at, 16), :] = lower[16 * j : 16 * j + 16]
        out[pl.ds(at + 16, 4), :] = m[:4]
        out[pl.ds(at + 20, 16), :] = upper[16 * j : 16 * j + 16]


def plane_kernel(main, above, below, above2, below2, out, first, final):
    y = lanes() % 32

    def take(ref, row, height):
        return ref[pl.ds(row, 8, stride=height), :]

    def plane(z):
        v = [
            take(below2, 4 + z, 20),
            take(below, z, ROWS),
            take(below, 20 + z, ROWS),
            take(main, z, ROWS),
            take(main, 20 + z, ROWS),
            take(above, z, ROWS),
            take(above, 20 + z, ROWS),
            take(above2, z, 20),
        ]
        v = swap_blocks(v, 4)
        r, shift = z % 4, 8 * (z // 4)
        m = turn(take(above2, 16 + r, 20), 28 - shift)
        m = jnp.where(y < 28, turn(take(above, 16 + r, ROWS), 20 - shift), m)
        m = jnp.where(y < 20, turn(take(main, 16 + r, ROWS), 12 - shift), m)
        m = jnp.where(y < 12, turn(take(below, 16 + r, ROWS), 4 - shift), m)
        m = jnp.where(y < 4, turn(take(below2, r, 20), -4 - shift), m)
        return v + [m]

    for z in range(FINE):
        for f, value in enumerate(plane(z)):
            out[f, z] = value
    for ref, at in ((first, lambda d: d - 1), (final, lambda d: FINE - d)):
        for d in range(1, SENT + 1):
            near = (y > d) & (y < 31 - d)
            for f in range(FIELDS):
                value = out[f, at(d)]
                if 2 < d < SENT:
                    value = jnp.where(near, value, turn(out[f, at(14 - d)], 16))
                ref[f, d - 1] = value


def x_up(v):
    v = turn(v, -32)
    return jnp.where(lanes() < 96, v, sink(v, -1))


def x_down(v):
    v = turn(v, 32)
    return jnp.where(lanes() >= 32, v, sink(v, 1))


def y_up(v):
    return turn(v, -1)


def y_down(v):
    return turn(v, 1)


def slot_of(r, s):
    if s < 0:
        return UNIQUE + r if r < KRYLOV - 1 else 64 + UNIQUE
    return r * (r + 1) // 2 + s


def cycle_kernel(main, low, high, sums, back, face, inv, ta, tb, images, halves, acc):
    lane = lanes()
    ix = sublanes() * 4 + lane // 32
    last_x, first_x = ix == 31, ix == 0

    def far(ref, f, d):
        return ref[f, d - 1] if d <= SENT else turn(ref[f, 13 - d], -16)

    def field(f, i):
        if i < DEPTH:
            return far(low, f, DEPTH - i)
        if i < DEPTH + FINE:
            return main[f, i - DEPTH]
        return far(high, f, i - DEPTH - FINE + 1)

    block = (lane % 32) // 8

    def compact(planes):
        value = turn(planes[3], 12)
        for j in (2, 1, 0):
            value = jnp.where(block == j, turn(planes[j], 8 * j - 12), value)
        return value

    def send_back(array, g, planes):
        back[pl.ds(array * 4 + g, 8, stride=BACK), :] = compact(planes)

    blocks_kept = ([], [], [])
    sz = [field(2, 0), field(5, 0)]
    low_z = [None, None]
    for i in range(EXT - 1):
        diagonals = []
        for s in range(2):
            above = field(s * 3 + 2, i + 1)
            up_z = 0.5 * (sz[s] + above)
            face[s * 3 + 2, i] = up_z
            if i > 0:
                sx, sy = field(s * 3, i), field(s * 3 + 1, i)
                up_x = 0.5 * (sx + jnp.where(last_x, 0.0, x_up(sx)))
                low_x = 0.5 * (sx + jnp.where(first_x, 0.0, x_down(sx)))
                up_y = 0.5 * (sy + y_up(sy))
                low_y = 0.5 * (sy + y_down(sy))
                face[s * 3, i] = jnp.where(last_x, 0.0, up_x)
                face[s * 3 + 1, i] = up_y
                diagonals.append(up_x + low_x + up_y + low_y + up_z + low_z[s])
            sz[s], low_z[s] = above, up_z
        if i > 0:
            di, de = diagonals
            m = field(8, i)
            det = m * di + m * de + di * de
            inside = m > 0.0
            scale = jnp.where(inside, 1.0 / jnp.where(inside, det, 1.0), 0.0)
            inv[0, i] = de * scale
            inv[1, i] = m * scale
            inv[2, i] = -di * scale
            inv[3, i] = (m + di) * scale
            if DEPTH <= i < DEPTH + FINE:
                for n, value in enumerate(((di + de) * scale, -di * scale, (m + di) * scale)):
                    blocks_kept[n].append(value)
                if len(blocks_kept[0]) == 4:
                    for n in range(3):
                        send_back(2 * KRYLOV + 2 + n, (i - DEPTH) // 4, blocks_kept[n])
                    blocks_kept = ([], [], [])

    def remember(r, at, value):
        images[r, at] = value
        halves[0, r, at], halves[1, r, at] = split(value)

    for part in range(2):
        for g in range(FINE // 4):
            planes = [main[6 + part, 4 * g + j] for j in range(4)]
            remember(0, part * 4 + g, compact(planes))
            send_back(part, g, planes)

    buffers = (ta, tb)

    def vector(k, part, i):
        return field(6 + part, i) if k == 0 else buffers[k % 2][part, i]

    for k in range(KRYLOV):

        def blocks(i):
            v, p = vector(k, 0, i), vector(k, 1, i)
            return (inv[0, i] * v + inv[1, i] * p, inv[2, i] * v + inv[3, i] * p), (v, p)

        def spread(s, i, u):
            fx, fy = face[s * 3, i], face[s * 3 + 1, i]
            across = fx * x_up(u[1][s]) + x_down(fx * u[1][s])
            along = fy * y_up(u[1][s]) + y_down(fy * u[1][s])
            deep = face[s * 3 + 2, i] * u[2][s] + face[s * 3 + 2, i - 1] * u[0][s]
            return across + along + deep

        start, end = 2 + k, EXT - 2 - k
        (before, _), (here, t_here) = blocks(start - 1), blocks(start)
        kept = ([], [], [], [])
        for i in range(start, end):
            after, t_after = blocks(i + 1)
            shared = spread(0, i, (before, here, after))
            b = (-shared, -(shared + spread(1, i, (before, here, after))))
            if DEPTH <= i < DEPTH + FINE:
                for part in range(2):
                    kept[part].append(t_here[part] + b[part])
            for part in range(2):
                value = b[part]
                if k > 0:
                    value = 2.0 * value - vector(k - 1, part, i)
                if k + 1 < KRYLOV:
                    buffers[(k + 1) % 2][part, i] = value
                if DEPTH <= i < DEPTH + FINE:
                    kept[2 + part].append(value)
            if len(kept[0]) == 4:
                g = (i - DEPTH) // 4
                for part in range(2):
                    remember(k + 1, part * 4 + g, compact(kept[part]))
                    send_back(2 * k + 2 + part, g, kept[2 + part])
                kept = ([], [], [], [])
            before, here, t_here = here, after, t_after

    def product(r, s):
        terms = []
        for at in range(8):
            a, b = images[r, at], images[s, at]
            ah, al, bh, bl = halves[0, r, at], halves[1, r, at], halves[0, s, at], halves[1, s, at]
            p = a * b
            terms.append((p, ((ah * bh - p) + ah * bl + al * bh) + al * bl))
        return total_of(terms)

    pairs = {
        slot_of(r - 1, s - 1): (r, s) for r in range(1, KRYLOV + 1) for s in range(r + 1)
    }
    for group in range(16):
        found = [pairs.get(8 * group + i) for i in range(8)]
        if None not in found:
            values = [product(*pair) for pair in found]
            for d in (4, 2, 1):
                values = [merge(values[i], values[i + d], d) for i in range(d)]
            value = values[0]
        elif any(found):
            (pair,) = (pair for pair in found if pair)
            value = fold_sublanes(product(*pair))
        else:
            value = (jnp.zeros((8, 128), f32),) * 2
        acc[0, pl.ds(group * 8, 8), :] = value[0]
        acc[1, pl.ds(group * 8, 8), :] = value[1]
    turned = acc[0].T, acc[1].T
    value = fold_sublanes(
        total_of((turned[0][8 * i : 8 * i + 8], turned[1][8 * i : 8 * i + 8]) for i in range(16))
    )
    row = jnp.where(is_high(), value[0], turn(value[1], 64))
    for i in range(sums.shape[0] // 8):
        sums[pl.ds(8 * i, 8), :] = row


def is_high():
    return (lanes() < 64) | (lanes() == 64 + UNIQUE)


def low_words(error):
    return turn(jnp.where(lanes() < UNIQUE, error, 0.0), 64)


def sum_kernel(received, _, back):
    zero = jnp.zeros((8, 128), f32)
    groups = range(received.shape[0] // 8)
    high, error = fold_sublanes(total_of((received[pl.ds(8 * i, 8), :], zero) for i in groups))
    row = jnp.where(is_high(), high, high + low_words(error))
    back[pl.ds(SUMS, 8, stride=BACK), :] = row


def solve_kernel(received, solution, residual, rows):
    def take(array, g):
        return received[pl.ds(array * 4 + g, 8, stride=BACK), :]

    zero = jnp.zeros((8, 128), f32)
    high, error = fold_sublanes((received[pl.ds(SUMS, 8, stride=BACK), :], zero))
    error = jnp.where(lanes() < UNIQUE, error + turn(high, 64), error)
    row, lane = sublanes(16), lanes(16)
    matrix = []
    for n, part in enumerate((high, error)):
        part = jnp.concatenate([part, part], 0)
        value = jnp.zeros((16, 128), f32)
        for r in range(KRYLOV):
            value = jnp.where(row == r, turn(part, -slot_of(r, 0)), value)
        value = jnp.where(lane <= row, value, 0.0)
        flipped = jnp.concatenate([value, jnp.zeros((112, 128), f32)], 0).T[:16]
        value = jnp.where(lane <= row, value, flipped)
        right = jnp.zeros((16, 128), f32)
        for r in range(KRYLOV):
            right = jnp.where(row == r, turn(part, KRYLOV - slot_of(r, -1)), right)
        matrix.append(jnp.where(lane == KRYLOV, right, value))
    matrix = quick_sum(*matrix)
    for j in range(KRYLOV):
        pivot_row = tuple(jnp.broadcast_to(part[j : j + 1, :], (8, 128)) for part in matrix)
        pivot = tuple(jnp.broadcast_to(part[j : j + 1, j : j + 1], (8, 128)) for part in matrix)
        scaled = dd_mul(pivot_row, dd_inverse(pivot))
        scaled = tuple(jnp.concatenate([part, part], 0) for part in scaled)
        column = tuple(-jnp.broadcast_to(part[:, j : j + 1], (16, 128)) for part in matrix)
        rest = dd_add(matrix, dd_mul(column, scaled))
        matrix = tuple(jnp.where(row == j, a, b) for a, b in zip(scaled, rest))
    coeffs = [
        jnp.broadcast_to(matrix[0][k : k + 1, KRYLOV : KRYLOV + 1], (8, 128))
        for k in range(KRYLOV)
    ]
    image = [y for y in coeffs] + [jnp.zeros((8, 128), f32)]
    for k in range(KRYLOV):
        image[k + 1] = image[k + 1] + (coeffs[k] if k == 0 else 0.5 * coeffs[k])
        if k > 0:
            image[k - 1] = image[k - 1] + 0.5 * coeffs[k]
    image[0] = image[0] - 1.0
    for g in range(FINE // 4):
        combined, left = [], []
        for part in range(2):
            vectors = [take(2 * m + part, g) for m in range(KRYLOV + 1)]
            combined.append(sum(coeffs[k] * vectors[k] for k in range(KRYLOV)))
            left.append(-sum(image[m] * vectors[m] for m in range(KRYLOV + 1)))
        b = [take(2 * KRYLOV + 2 + n, g) for n in range(3)]
        v = [
            b[0] * combined[0] + b[1] * combined[1],
            b[1] * combined[0] + b[2] * combined[1],
        ]
        for j, value in enumerate(swap_blocks(v + left, 8)):
            rows[pl.ds(4 * g + j, 8, stride=FINE), :] = value
    turned = rows[...].T
    for f in range(4):
        ref = solution if f < 2 else residual
        for x in range(4):
            ref[f % 2, x] = turned[x * 32 + f * 8 : x * 32 + f * 8 + 8]


def shape(*dims):
    return jax.ShapeDtypeStruct(dims, f32)


def held(*dims):
    return pltpu.VMEM(dims, f32)


def near(*values):
    return tuple(pltpu.with_memory_space_constraint(v, pltpu.VMEM) for v in values)


def scratch(*dims):
    return pltpu.VMEM(dims, f32)


def body(source, sigma_intra, sigma_extra, membrane):
    nx, ny, nz = (lax.axis_size(a) for a in ("gx", "gy", "gz"))
    packed = pl.pallas_call(pack_kernel, out_shape=held(8 * ROWS, 128))(
        source, sigma_intra, sigma_extra, membrane
    )
    own = lax.all_to_all(packed.reshape(8, ROWS, 1, 128), "gx", 0, 0, tiled=True)

    def from_y(value, by):
        pairs = [(i, i - by) for i in range(ny) if 0 <= i - by < ny]
        got = lax.ppermute(value, "gy", pairs)
        return got.reshape(-1, 128)

    halo = (from_y(own, 1), from_y(own, -1), from_y(own[:, :20], 2), from_y(own[:, 16:], -2))
    planes, first, final = pl.pallas_call(
        plane_kernel,
        out_shape=(
            held(FIELDS, FINE, 8, 128),
            held(FIELDS, SENT, 8, 128),
            held(FIELDS, SENT, 8, 128),
        ),
    )(*near(own.reshape(-1, 128), *halo))

    def place(c):
        return (c % nx) * nz + c // nx

    up = [(place(c), place(c + 1)) for c in range(nx * nz - 1)]
    low = lax.ppermute(final, ("gx", "gz"), up)
    high = lax.ppermute(first, ("gx", "gz"), [(b, a) for a, b in up])

    sums, back = pl.pallas_call(
        cycle_kernel,
        out_shape=(held(ny * nz, 128), held(8 * BACK, 128)),
        scratch_shapes=[
            scratch(6, EXT, 8, 128),
            scratch(4, EXT, 8, 128),
            scratch(2, EXT, 8, 128),
            scratch(2, EXT, 8, 128),
            scratch(KRYLOV + 1, 8, 8, 128),
            scratch(2, KRYLOV + 1, 8, 8, 128),
            scratch(2, 128, 128),
        ],
    )(*near(planes, low, high))

    got = lax.all_to_all(sums.reshape(-1, 1, 128), ("gy", "gz"), 0, 0, tiled=True)
    back = pl.pallas_call(
        sum_kernel, out_shape=held(8 * BACK, 128), input_output_aliases={1: 0}
    )(*near(got.reshape(-1, 128), back))
    got = lax.all_to_all(back.reshape(8, BACK, 1, 128), "gx", 0, 0, tiled=True)
    return pl.pallas_call(
        solve_kernel,
        out_shape=(shape(2, 4, 8, 128), shape(2, 4, 8, 128)),
        scratch_shapes=[scratch(128, 128)],
    )(*near(got.reshape(-1, 128)))


def solution(mesh):
    spread = P(None, "gx", "gy", "gz")
    return jax.shard_map(
        body,
        mesh=mesh,
        in_specs=(spread, spread, spread, P("gx", "gy", "gz")),
        out_specs=(spread, spread),
        check_vma=False,
    )
```

```python
import jax
import jax.numpy as jnp
from jax import lax
from jax.experimental import pallas as pl
from jax.experimental.pallas import tpu as pltpu
from jax.sharding import Mesh
from jax.sharding import PartitionSpec as P

KRYLOV = 10
DEPTH = KRYLOV + 1
FINE = 16
EXT = FINE + 2 * DEPTH
SENT = 7
FIELDS = 9
ROWS = 36
WIDE, THIN = 56, 20
BACK = 101
SUMS = 4 * (2 * KRYLOV + 5)
UNIQUE = KRYLOV * (KRYLOV + 1) // 2
f32 = jnp.float32
GY = ("gy_0", "gy_1")


def lanes(rows=8):
    return lax.broadcasted_iota(jnp.int32, (rows, 128), 1)


def sublanes(rows=8):
    return lax.broadcasted_iota(jnp.int32, (rows, 128), 0)


def turn(v, by):
    return v if by % 128 == 0 else pltpu.roll(v, by % 128, 1)


def sink(v, by):
    return pltpu.roll(v, by % 8, 0)


def two_sum(a, b):
    s = a + b
    z = s - a
    return s, (a - (s - z)) + (b - z)


def quick_sum(a, b):
    s = a + b
    return s, b - (s - a)


def split(a):
    c = a * 4097.0
    high = c - (c - a)
    return high, a - high


def two_prod(a, b):
    p = a * b
    ah, al = split(a)
    bh, bl = split(b)
    return p, ((ah * bh - p) + ah * bl + al * bh) + al * bl


def dd_add(a, b):
    s, e = two_sum(a[0], b[0])
    return quick_sum(s, e + (a[1] + b[1]))


def dd_mul(a, b):
    p, e = two_prod(a[0], b[0])
    return quick_sum(p, e + (a[0] * b[1] + a[1] * b[0]))


def dd_inverse(a):
    x = 1.0 / a[0]
    p, e = two_prod(a[0], x)
    return quick_sum(x, x * (((1.0 - p) - e) - a[1] * x))


def add_pairs(a, b):
    s, e = two_sum(a[0], b[0])
    return s, e + (a[1] + b[1])


def total_of(pairs):
    pairs = list(pairs)
    while len(pairs) > 1:
        pairs = [
            add_pairs(pairs[i], pairs[i + 1]) if i + 1 < len(pairs) else pairs[i]
            for i in range(0, len(pairs), 2)
        ]
    return pairs[0]


def fold_sublanes(a):
    for by in (4, 2, 1):
        a = add_pairs(a, (sink(a[0], by), sink(a[1], by)))
    return quick_sum(*a)


def merge(a, b, d):
    low = (sublanes() & d) == 0
    return add_pairs(
        tuple(jnp.where(low, x, y) for x, y in zip(a, b)),
        tuple(jnp.where(low, sink(x, -d), sink(y, d)) for x, y in zip(a, b)),
    )


def swap_blocks(v, width):
    v = list(v)
    block = lanes() // width
    d = len(v) // 2
    while d >= 1:
        low = (block & d) == 0
        for k in range(len(v)):
            if k & d == 0:
                a, b = v[k], v[k + d]
                v[k] = jnp.where(low, a, turn(b, width * d))
                v[k + d] = jnp.where(low, turn(a, -width * d), b)
        d //= 2
    return v


def pack_kernel(source, intra, extra, membrane, out):
    refs = [(intra, 0), (intra, 1), (intra, 2), (extra, 0), (extra, 1), (extra, 2), (source, 0), (source, 1)]
    top = sublanes() < 4
    lower, upper = [], []
    for x in range(4):
        for f in range(0, 8, 2):
            a, b = refs[f][0][refs[f][1], x], refs[f + 1][0][refs[f + 1][1], x]
            lower.append(jnp.where(top, a, sink(b, 4)))
            upper.append(jnp.where(top, sink(a, 4), b))
    empty = jnp.zeros((24, 128), f32)
    last = []
    for x in range(4):
        last += [membrane[x], empty]
    lower, upper, last = (jnp.concatenate(part, 0).T for part in (lower, upper, last))
    group = (lanes() % 32) // 8
    for j in range(8):
        a, b = last[16 * j : 16 * j + 8], last[16 * j + 8 : 16 * j + 16]
        m = jnp.where(group == 2, turn(b, 16), turn(sink(b, 4), 24))
        m = jnp.where(group == 1, turn(sink(a, 4), 8), m)
        m = jnp.where(group == 0, a, m)
        for at in (2 * j * ROWS, (2 * j + 1) * ROWS):
            out[pl.ds(at, 16), :] = lower[16 * j : 16 * j + 16]
            out[pl.ds(at + 16, 4), :] = m[:4]
            out[pl.ds(at + 20, 16), :] = upper[16 * j : 16 * j + 16]


def choose_kernel(pair, wide, thin):
    odd = lax.axis_index("gy_1") == 1
    for s in range(8):
        at = 2 * ROWS * s
        rows = pair[pl.ds(at + 16, WIDE), :], pair[pl.ds(at, WIDE), :]
        wide[pl.ds(WIDE * s, WIDE), :] = jnp.where(odd, *rows)
        rows = pair[pl.ds(at + 2 * ROWS - THIN, THIN), :], pair[pl.ds(at, THIN), :]
        thin[pl.ds(THIN * s, THIN), :] = jnp.where(odd, *rows)


def plane_kernel(pair, wide, thin, out, first, final):
    y = lanes() % 32
    odd = lax.axis_index("gy_1")
    is_even = jnp.full((8, 128), odd, jnp.int32) == 0

    def take(ref, row, height):
        return ref[pl.ds(row, 8, stride=height), :]

    def ordered(own, far, last):
        even = far + own + last
        other = last + own + far
        return [a if a is b else jnp.where(is_even, a, b) for a, b in zip(even, other)]

    def plane(z):
        own = [take(pair, at + z, 2 * ROWS) for at in (0, 20, 36, 56)]
        far = [take(wide, at + z, WIDE) for at in (4 - 4 * odd, 20, 40 - 4 * odd)]
        v = swap_blocks(ordered(own, far, [take(thin, 4 * odd + z, THIN)]), 4)
        r, shift = z % 4, 8 * (z // 4)
        own = [take(pair, at + r, 2 * ROWS) for at in (16, 52)]
        far = [take(wide, at + 16 * odd + r, WIDE) for at in (0, 36)]
        parts = ordered(own, far, [take(thin, 16 - 16 * odd + r, THIN)])
        m = turn(parts[4], 28 - shift)
        for n in (3, 2, 1, 0):
            m = jnp.where(y < 8 * n + 4, turn(parts[n], 8 * n - 4 - shift), m)
        return v + [m]

    for z in range(FINE):
        for f, value in enumerate(plane(z)):
            out[f, z] = value
    for ref, at in ((first, lambda d: d - 1), (final, lambda d: FINE - d)):
        for d in range(1, SENT + 1):
            near = (y > d) & (y < 31 - d)
            for f in range(FIELDS):
                value = out[f, at(d)]
                if 2 < d < SENT:
                    value = jnp.where(near, value, turn(out[f, at(14 - d)], 16))
                ref[f, d - 1] = value


def x_up(v):
    v = turn(v, -32)
    return jnp.where(lanes() < 96, v, sink(v, -1))


def x_down(v):
    v = turn(v, 32)
    return jnp.where(lanes() >= 32, v, sink(v, 1))


def y_up(v):
    return turn(v, -1)


def y_down(v):
    return turn(v, 1)


def slot_of(r, s):
    if s < 0:
        return UNIQUE + r if r < KRYLOV - 1 else 64 + UNIQUE
    return r * (r + 1) // 2 + s


def cycle_kernel(main, low, high, sums, back, face, inv, ta, tb, images, halves, acc):
    lane = lanes()
    ix = sublanes() * 4 + lane // 32
    last_x, first_x = ix == 31, ix == 0

    def far(ref, f, d):
        return ref[f, d - 1] if d <= SENT else turn(ref[f, 13 - d], -16)

    def field(f, i):
        if i < DEPTH:
            return far(low, f, DEPTH - i)
        if i < DEPTH + FINE:
            return main[f, i - DEPTH]
        return far(high, f, i - DEPTH - FINE + 1)

    block = (lane % 32) // 8

    def compact(planes):
        value = turn(planes[3], 12)
        for j in (2, 1, 0):
            value = jnp.where(block == j, turn(planes[j], 8 * j - 12), value)
        return value

    def send_back(array, g, planes):
        back[pl.ds(array * 4 + g, 8, stride=BACK), :] = compact(planes)

    blocks_kept = ([], [], [])
    sz = [field(2, 0), field(5, 0)]
    low_z = [None, None]
    for i in range(EXT - 1):
        diagonals = []
        for s in range(2):
            above = field(s * 3 + 2, i + 1)
            up_z = 0.5 * (sz[s] + above)
            face[s * 3 + 2, i] = up_z
            if i > 0:
                sx, sy = field(s * 3, i), field(s * 3 + 1, i)
                up_x = 0.5 * (sx + jnp.where(last_x, 0.0, x_up(sx)))
                low_x = 0.5 * (sx + jnp.where(first_x, 0.0, x_down(sx)))
                up_y = 0.5 * (sy + y_up(sy))
                low_y = 0.5 * (sy + y_down(sy))
                face[s * 3, i] = jnp.where(last_x, 0.0, up_x)
                face[s * 3 + 1, i] = up_y
                diagonals.append(up_x + low_x + up_y + low_y + up_z + low_z[s])
            sz[s], low_z[s] = above, up_z
        if i > 0:
            di, de = diagonals
            m = field(8, i)
            det = m * di + m * de + di * de
            inside = m > 0.0
            scale = jnp.where(inside, 1.0 / jnp.where(inside, det, 1.0), 0.0)
            inv[0, i] = de * scale
            inv[1, i] = m * scale
            inv[2, i] = -di * scale
            inv[3, i] = (m + di) * scale
            if DEPTH <= i < DEPTH + FINE:
                for n, value in enumerate(((di + de) * scale, -di * scale, (m + di) * scale)):
                    blocks_kept[n].append(value)
                if len(blocks_kept[0]) == 4:
                    for n in range(3):
                        send_back(2 * KRYLOV + 2 + n, (i - DEPTH) // 4, blocks_kept[n])
                    blocks_kept = ([], [], [])

    def remember(r, at, value):
        images[r, at] = value
        halves[0, r, at], halves[1, r, at] = split(value)

    for part in range(2):
        for g in range(FINE // 4):
            planes = [main[6 + part, 4 * g + j] for j in range(4)]
            remember(0, part * 4 + g, compact(planes))
            send_back(part, g, planes)

    buffers = (ta, tb)

    def vector(k, part, i):
        return field(6 + part, i) if k == 0 else buffers[k % 2][part, i]

    for k in range(KRYLOV):

        def blocks(i):
            v, p = vector(k, 0, i), vector(k, 1, i)
            return (inv[0, i] * v + inv[1, i] * p, inv[2, i] * v + inv[3, i] * p), (v, p)

        def spread(s, i, u):
            fx, fy = face[s * 3, i], face[s * 3 + 1, i]
            across = fx * x_up(u[1][s]) + x_down(fx * u[1][s])
            along = fy * y_up(u[1][s]) + y_down(fy * u[1][s])
            deep = face[s * 3 + 2, i] * u[2][s] + face[s * 3 + 2, i - 1] * u[0][s]
            return across + along + deep

        start, end = 2 + k, EXT - 2 - k
        (before, _), (here, t_here) = blocks(start - 1), blocks(start)
        kept = ([], [], [], [])
        for i in range(start, end):
            after, t_after = blocks(i + 1)
            shared = spread(0, i, (before, here, after))
            b = (-shared, -(shared + spread(1, i, (before, here, after))))
            if DEPTH <= i < DEPTH + FINE:
                for part in range(2):
                    kept[part].append(t_here[part] + b[part])
            for part in range(2):
                value = b[part]
                if k > 0:
                    value = 2.0 * value - vector(k - 1, part, i)
                if k + 1 < KRYLOV:
                    buffers[(k + 1) % 2][part, i] = value
                if DEPTH <= i < DEPTH + FINE:
                    kept[2 + part].append(value)
            if len(kept[0]) == 4:
                g = (i - DEPTH) // 4
                for part in range(2):
                    remember(k + 1, part * 4 + g, compact(kept[part]))
                    send_back(2 * k + 2 + part, g, kept[2 + part])
                kept = ([], [], [], [])
            before, here, t_here = here, after, t_after

    def product(r, s):
        terms = []
        for at in range(8):
            a, b = images[r, at], images[s, at]
            ah, al, bh, bl = halves[0, r, at], halves[1, r, at], halves[0, s, at], halves[1, s, at]
            p = a * b
            terms.append((p, ((ah * bh - p) + ah * bl + al * bh) + al * bl))
        return total_of(terms)

    pairs = {
        slot_of(r - 1, s - 1): (r, s) for r in range(1, KRYLOV + 1) for s in range(r + 1)
    }
    for group in range(16):
        found = [pairs.get(8 * group + i) for i in range(8)]
        if None not in found:
            values = [product(*pair) for pair in found]
            for d in (4, 2, 1):
                values = [merge(values[i], values[i + d], d) for i in range(d)]
            value = values[0]
        elif any(found):
            (pair,) = (pair for pair in found if pair)
            value = fold_sublanes(product(*pair))
        else:
            value = (jnp.zeros((8, 128), f32),) * 2
        acc[0, pl.ds(group * 8, 8), :] = value[0]
        acc[1, pl.ds(group * 8, 8), :] = value[1]
    turned = acc[0].T, acc[1].T
    value = fold_sublanes(
        total_of((turned[0][8 * i : 8 * i + 8], turned[1][8 * i : 8 * i + 8]) for i in range(16))
    )
    row = jnp.where(is_high(), value[0], turn(value[1], 64))
    for i in range(sums.shape[0] // 8):
        sums[pl.ds(8 * i, 8), :] = row


def is_high():
    return (lanes() < 64) | (lanes() == 64 + UNIQUE)


def low_words(error):
    return turn(jnp.where(lanes() < UNIQUE, error, 0.0), 64)


def sum_kernel(received, _, back):
    zero = jnp.zeros((8, 128), f32)
    groups = range(received.shape[0] // 8)
    high, error = fold_sublanes(total_of((received[pl.ds(8 * i, 8), :], zero) for i in groups))
    row = jnp.where(is_high(), high, high + low_words(error))
    back[pl.ds(SUMS, 8, stride=BACK), :] = row


def solve_kernel(received, solution, residual, rows):
    def take(array, g):
        return received[pl.ds(array * 4 + g, 8, stride=BACK), :]

    zero = jnp.zeros((8, 128), f32)
    high, error = fold_sublanes((received[pl.ds(SUMS, 8, stride=BACK), :], zero))
    error = jnp.where(lanes() < UNIQUE, error + turn(high, 64), error)
    row, lane = sublanes(16), lanes(16)
    matrix = []
    for n, part in enumerate((high, error)):
        part = jnp.concatenate([part, part], 0)
        value = jnp.zeros((16, 128), f32)
        for r in range(KRYLOV):
            value = jnp.where(row == r, turn(part, -slot_of(r, 0)), value)
        value = jnp.where(lane <= row, value, 0.0)
        flipped = jnp.concatenate([value, jnp.zeros((112, 128), f32)], 0).T[:16]
        value = jnp.where(lane <= row, value, flipped)
        right = jnp.zeros((16, 128), f32)
        for r in range(KRYLOV):
            right = jnp.where(row == r, turn(part, KRYLOV - slot_of(r, -1)), right)
        matrix.append(jnp.where(lane == KRYLOV, right, value))
    matrix = quick_sum(*matrix)
    for j in range(KRYLOV):
        pivot_row = tuple(jnp.broadcast_to(part[j : j + 1, :], (8, 128)) for part in matrix)
        pivot = tuple(jnp.broadcast_to(part[j : j + 1, j : j + 1], (8, 128)) for part in matrix)
        scaled = dd_mul(pivot_row, dd_inverse(pivot))
        scaled = tuple(jnp.concatenate([part, part], 0) for part in scaled)
        column = tuple(-jnp.broadcast_to(part[:, j : j + 1], (16, 128)) for part in matrix)
        rest = dd_add(matrix, dd_mul(column, scaled))
        matrix = tuple(jnp.where(row == j, a, b) for a, b in zip(scaled, rest))
    coeffs = [
        jnp.broadcast_to(matrix[0][k : k + 1, KRYLOV : KRYLOV + 1], (8, 128))
        for k in range(KRYLOV)
    ]
    image = [y for y in coeffs] + [jnp.zeros((8, 128), f32)]
    for k in range(KRYLOV):
        image[k + 1] = image[k + 1] + (coeffs[k] if k == 0 else 0.5 * coeffs[k])
        if k > 0:
            image[k - 1] = image[k - 1] + 0.5 * coeffs[k]
    image[0] = image[0] - 1.0
    for g in range(FINE // 4):
        combined, left = [], []
        for part in range(2):
            vectors = [take(2 * m + part, g) for m in range(KRYLOV + 1)]
            combined.append(sum(coeffs[k] * vectors[k] for k in range(KRYLOV)))
            left.append(-sum(image[m] * vectors[m] for m in range(KRYLOV + 1)))
        b = [take(2 * KRYLOV + 2 + n, g) for n in range(3)]
        v = [
            b[0] * combined[0] + b[1] * combined[1],
            b[1] * combined[0] + b[2] * combined[1],
        ]
        for j, value in enumerate(swap_blocks(v + left, 8)):
            rows[pl.ds(4 * g + j, 8, stride=FINE), :] = value
    turned = rows[...].T
    for f in range(4):
        ref = solution if f < 2 else residual
        for x in range(4):
            ref[f % 2, x] = turned[x * 32 + f * 8 : x * 32 + f * 8 + 8]


def shape(*dims):
    return jax.ShapeDtypeStruct(dims, f32)


def held(*dims):
    return pltpu.VMEM(dims, f32)


def near(*values):
    return tuple(pltpu.with_memory_space_constraint(v, pltpu.VMEM) for v in values)


def scratch(*dims):
    return pltpu.VMEM(dims, f32)


def body(source, sigma_intra, sigma_extra, membrane):
    nx, nz = (lax.axis_size(a) for a in ("gx", "gz"))
    ny = lax.axis_size(GY)
    packed = pl.pallas_call(pack_kernel, out_shape=held(16 * ROWS, 128))(
        source, sigma_intra, sigma_extra, membrane
    )
    pair = lax.all_to_all(packed.reshape(16, ROWS, 1, 128), ("gx", "gy_1"), 0, 0, tiled=True)
    (pair,) = near(pair.reshape(-1, 128))
    wide, thin = pl.pallas_call(
        choose_kernel, out_shape=(held(8 * WIDE, 128), held(8 * THIN, 128))
    )(pair)
    across = [(i, i + 1) for i in range(1, ny - 1, 2)]
    wide = lax.ppermute(wide, GY, across + [(b, a) for a, b in across])
    thin = lax.ppermute(
        thin,
        GY,
        [(i, i - 2) for i in range(2, ny, 2)] + [(i, i + 2) for i in range(1, ny - 2, 2)],
    )
    halo = wide, thin
    planes, first, final = pl.pallas_call(
        plane_kernel,
        out_shape=(
            held(FIELDS, FINE, 8, 128),
            held(FIELDS, SENT, 8, 128),
            held(FIELDS, SENT, 8, 128),
        ),
    )(*near(pair, *halo))

    def place(c):
        return (c % nx) * nz + c // nx

    up = [(place(c), place(c + 1)) for c in range(nx * nz - 1)]
    low = lax.ppermute(final, ("gx", "gz"), up)
    high = lax.ppermute(first, ("gx", "gz"), [(b, a) for a, b in up])

    sums, back = pl.pallas_call(
        cycle_kernel,
        out_shape=(held(ny * nz, 128), held(8 * BACK, 128)),
        scratch_shapes=[
            scratch(6, EXT, 8, 128),
            scratch(4, EXT, 8, 128),
            scratch(2, EXT, 8, 128),
            scratch(2, EXT, 8, 128),
            scratch(KRYLOV + 1, 8, 8, 128),
            scratch(2, KRYLOV + 1, 8, 8, 128),
            scratch(2, 128, 128),
        ],
    )(*near(planes, low, high))

    got = lax.all_to_all(sums.reshape(-1, 1, 128), GY + ("gz",), 0, 0, tiled=True)
    back = pl.pallas_call(
        sum_kernel, out_shape=held(8 * BACK, 128), input_output_aliases={1: 0}
    )(*near(got.reshape(-1, 128), back))
    got = lax.all_to_all(back.reshape(8, BACK, 1, 128), "gx", 0, 0, tiled=True)
    return pl.pallas_call(
        solve_kernel,
        out_shape=(shape(2, 4, 8, 128), shape(2, 4, 8, 128)),
        scratch_shapes=[scratch(128, 128)],
    )(*near(got.reshape(-1, 128)))


def solution(mesh):
    nx, ny, nz = (mesh.shape[a] for a in ("gx", "gy", "gz"))
    pairs = Mesh(mesh.devices.reshape(nx, ny // 2, 2, nz), ("gx", *GY, "gz"))
    spread = P(None, "gx", GY, "gz")
    return jax.shard_map(
        body,
        mesh=pairs,
        in_specs=(spread, spread, spread, P("gx", GY, "gz")),
        out_specs=(spread, spread),
        check_vma=False,
    )
```

```python
import jax
import jax.numpy as jnp
from jax import lax
from jax.experimental import pallas as pl
from jax.experimental.pallas import tpu as pltpu
from jax.sharding import Mesh
from jax.sharding import PartitionSpec as P

KRYLOV = 10
DEPTH = KRYLOV + 1
FINE = 16
EXT = FINE + 2 * DEPTH
SENT = 7
FIELDS = 9
ROWS = 36
WIDE, THIN = 56, 20
BACK = 101
SUMS = 4 * (2 * KRYLOV + 5)
UNIQUE = KRYLOV * (KRYLOV + 1) // 2
f32 = jnp.float32
GY = ("gy_0", "gy_1")


def lanes(rows=8):
    return lax.broadcasted_iota(jnp.int32, (rows, 128), 1)


def sublanes(rows=8):
    return lax.broadcasted_iota(jnp.int32, (rows, 128), 0)


def turn(v, by):
    return v if by % 128 == 0 else pltpu.roll(v, by % 128, 1)


def sink(v, by):
    return pltpu.roll(v, by % 8, 0)


def two_sum(a, b):
    s = a + b
    z = s - a
    return s, (a - (s - z)) + (b - z)


def quick_sum(a, b):
    s = a + b
    return s, b - (s - a)


def split(a):
    c = a * 4097.0
    high = c - (c - a)
    return high, a - high


def two_prod(a, b):
    p = a * b
    ah, al = split(a)
    bh, bl = split(b)
    return p, ((ah * bh - p) + ah * bl + al * bh) + al * bl


def dd_add(a, b):
    s, e = two_sum(a[0], b[0])
    return quick_sum(s, e + (a[1] + b[1]))


def dd_mul(a, b):
    p, e = two_prod(a[0], b[0])
    return quick_sum(p, e + (a[0] * b[1] + a[1] * b[0]))


def dd_inverse(a):
    x = 1.0 / a[0]
    p, e = two_prod(a[0], x)
    return quick_sum(x, x * (((1.0 - p) - e) - a[1] * x))


def add_pairs(a, b):
    s, e = two_sum(a[0], b[0])
    return s, e + (a[1] + b[1])


def total_of(pairs):
    pairs = list(pairs)
    while len(pairs) > 1:
        pairs = [
            add_pairs(pairs[i], pairs[i + 1]) if i + 1 < len(pairs) else pairs[i]
            for i in range(0, len(pairs), 2)
        ]
    return pairs[0]


def fold_sublanes(a):
    for by in (4, 2, 1):
        a = add_pairs(a, (sink(a[0], by), sink(a[1], by)))
    return quick_sum(*a)


def merge(a, b, d):
    low = (sublanes() & d) == 0
    return add_pairs(
        tuple(jnp.where(low, x, y) for x, y in zip(a, b)),
        tuple(jnp.where(low, sink(x, -d), sink(y, d)) for x, y in zip(a, b)),
    )


def swap_blocks(v, width):
    v = list(v)
    block = lanes() // width
    d = len(v) // 2
    while d >= 1:
        low = (block & d) == 0
        for k in range(len(v)):
            if k & d == 0:
                a, b = v[k], v[k + d]
                v[k] = jnp.where(low, a, turn(b, width * d))
                v[k + d] = jnp.where(low, turn(a, -width * d), b)
        d //= 2
    return v


def pack_kernel(source, intra, extra, membrane, out):
    refs = [(intra, 0), (intra, 1), (intra, 2), (extra, 0), (extra, 1), (extra, 2), (source, 0), (source, 1)]
    top = sublanes() < 4
    lower, upper = [], []
    for x in range(4):
        for f in range(0, 8, 2):
            a, b = refs[f][0][refs[f][1], x], refs[f + 1][0][refs[f + 1][1], x]
            lower.append(jnp.where(top, a, sink(b, 4)))
            upper.append(jnp.where(top, sink(a, 4), b))
    empty = jnp.zeros((24, 128), f32)
    last = []
    for x in range(4):
        last += [membrane[x], empty]
    lower, upper, last = (jnp.concatenate(part, 0).T for part in (lower, upper, last))
    group = (lanes() % 32) // 8
    for j in range(8):
        a, b = last[16 * j : 16 * j + 8], last[16 * j + 8 : 16 * j + 16]
        m = jnp.where(group == 2, turn(b, 16), turn(sink(b, 4), 24))
        m = jnp.where(group == 1, turn(sink(a, 4), 8), m)
        m = jnp.where(group == 0, a, m)
        for at in (2 * j * ROWS, (2 * j + 1) * ROWS):
            out[pl.ds(at, 16), :] = lower[16 * j : 16 * j + 16]
            out[pl.ds(at + 16, 4), :] = m[:4]
            out[pl.ds(at + 20, 16), :] = upper[16 * j : 16 * j + 16]


def choose_kernel(pair, wide, thin):
    odd = lax.axis_index("gy_1") == 1
    for s in range(8):
        at = 2 * ROWS * s
        rows = pair[pl.ds(at + 16, WIDE), :], pair[pl.ds(at, WIDE), :]
        wide[pl.ds(WIDE * s, WIDE), :] = jnp.where(odd, *rows)
        rows = pair[pl.ds(at + 2 * ROWS - THIN, THIN), :], pair[pl.ds(at, THIN), :]
        thin[pl.ds(THIN * s, THIN), :] = jnp.where(odd, *rows)


def plane_kernel(pair, wide, thin, out, first, final):
    y = lanes() % 32
    odd = lax.axis_index("gy_1")
    is_even = jnp.full((8, 128), odd, jnp.int32) == 0

    def take(ref, row, height):
        return ref[pl.ds(row, 8, stride=height), :]

    def ordered(own, far, last):
        even = far + own + last
        other = last + own + far
        return [a if a is b else jnp.where(is_even, a, b) for a, b in zip(even, other)]

    def plane(r, n):
        z, shift = 4 * n + r, 8 * n
        own = [take(pair, at + z, 2 * ROWS) for at in (0, 20, 36, 56)]
        far = [take(wide, at + z, WIDE) for at in (4 - 4 * odd, 20, 40 - 4 * odd)]
        v = swap_blocks(ordered(own, far, [take(thin, 4 * odd + z, THIN)]), 4)
        own = [take(pair, at + r, 2 * ROWS) for at in (16, 52)]
        far = [take(wide, at + 16 * odd + r, WIDE) for at in (0, 36)]
        parts = ordered(own, far, [take(thin, 16 - 16 * odd + r, THIN)])
        m = turn(parts[4], 28 - shift)
        for n in (3, 2, 1, 0):
            m = jnp.where(y < 8 * n + 4, turn(parts[n], 8 * n - 4 - shift), m)
        return v + [m]

    def four(r, _):
        for n in range(FINE // 4):
            for f, value in enumerate(plane(r, n)):
                out[f, 4 * n + r] = value
        return _

    lax.fori_loop(0, 4, four, 0)

    def edges(f, _):
        for ref, at in ((first, lambda d: d - 1), (final, lambda d: FINE - d)):
            for d in range(1, SENT + 1):
                value = out[f, at(d)]
                if 2 < d < SENT:
                    inner = (y > d) & (y < 31 - d)
                    value = jnp.where(inner, value, turn(out[f, at(14 - d)], 16))
                ref[f, d - 1] = value
        return _

    lax.fori_loop(0, FIELDS, edges, 0)


def x_up(v):
    v = turn(v, -32)
    return jnp.where(lanes() < 96, v, sink(v, -1))


def x_down(v):
    v = turn(v, 32)
    return jnp.where(lanes() >= 32, v, sink(v, 1))


def y_up(v):
    return turn(v, -1)


def y_down(v):
    return turn(v, 1)


def slot_of(r, s):
    if s < 0:
        return UNIQUE + r if r < KRYLOV - 1 else 64 + UNIQUE
    return r * (r + 1) // 2 + s


def cycle_kernel(main, low, high, sums, back, face, inv, ta, tb, images, halves, acc):
    lane = lanes()
    ix = sublanes() * 4 + lane // 32
    last_x, first_x = ix == 31, ix == 0

    def far(ref, f, d):
        return ref[f, d - 1] if d <= SENT else turn(ref[f, 13 - d], -16)

    def field(f, i):
        if i < DEPTH:
            return far(low, f, DEPTH - i)
        if i < DEPTH + FINE:
            return main[f, i - DEPTH]
        return far(high, f, i - DEPTH - FINE + 1)

    block = (lane % 32) // 8

    def compact(planes):
        value = turn(planes[3], 12)
        for j in (2, 1, 0):
            value = jnp.where(block == j, turn(planes[j], 8 * j - 12), value)
        return value

    def send_back(array, g, planes):
        back[pl.ds(array * 4 + g, 8, stride=BACK), :] = compact(planes)

    blocks_kept = ([], [], [])
    sz = [field(2, 0), field(5, 0)]
    low_z = [None, None]
    for i in range(EXT - 1):
        diagonals = []
        for s in range(2):
            above = field(s * 3 + 2, i + 1)
            up_z = 0.5 * (sz[s] + above)
            face[s * 3 + 2, i] = up_z
            if i > 0:
                sx, sy = field(s * 3, i), field(s * 3 + 1, i)
                up_x = 0.5 * (sx + jnp.where(last_x, 0.0, x_up(sx)))
                low_x = 0.5 * (sx + jnp.where(first_x, 0.0, x_down(sx)))
                up_y = 0.5 * (sy + y_up(sy))
                low_y = 0.5 * (sy + y_down(sy))
                face[s * 3, i] = jnp.where(last_x, 0.0, up_x)
                face[s * 3 + 1, i] = up_y
                diagonals.append(up_x + low_x + up_y + low_y + up_z + low_z[s])
            sz[s], low_z[s] = above, up_z
        if i > 0:
            di, de = diagonals
            m = field(8, i)
            det = m * di + m * de + di * de
            inside = m > 0.0
            scale = jnp.where(inside, 1.0 / jnp.where(inside, det, 1.0), 0.0)
            inv[0, i] = de * scale
            inv[1, i] = m * scale
            inv[2, i] = -di * scale
            inv[3, i] = (m + di) * scale
            if DEPTH <= i < DEPTH + FINE:
                for n, value in enumerate(((di + de) * scale, -di * scale, (m + di) * scale)):
                    blocks_kept[n].append(value)
                if len(blocks_kept[0]) == 4:
                    for n in range(3):
                        send_back(2 * KRYLOV + 2 + n, (i - DEPTH) // 4, blocks_kept[n])
                    blocks_kept = ([], [], [])

    def remember(r, at, value):
        images[r, at] = value
        halves[0, r, at], halves[1, r, at] = split(value)

    for part in range(2):
        for g in range(FINE // 4):
            planes = [main[6 + part, 4 * g + j] for j in range(4)]
            remember(0, part * 4 + g, compact(planes))
            send_back(part, g, planes)

    buffers = (ta, tb)

    def vector(k, part, i):
        return field(6 + part, i) if k == 0 else buffers[k % 2][part, i]

    for k in range(KRYLOV):

        def blocks(i):
            v, p = vector(k, 0, i), vector(k, 1, i)
            return (inv[0, i] * v + inv[1, i] * p, inv[2, i] * v + inv[3, i] * p), (v, p)

        def spread(s, i, u):
            fx, fy = face[s * 3, i], face[s * 3 + 1, i]
            across = fx * x_up(u[1][s]) + x_down(fx * u[1][s])
            along = fy * y_up(u[1][s]) + y_down(fy * u[1][s])
            deep = face[s * 3 + 2, i] * u[2][s] + face[s * 3 + 2, i - 1] * u[0][s]
            return across + along + deep

        start, end = 2 + k, EXT - 2 - k
        (before, _), (here, t_here) = blocks(start - 1), blocks(start)
        kept = ([], [], [], [])
        for i in range(start, end):
            after, t_after = blocks(i + 1)
            shared = spread(0, i, (before, here, after))
            b = (-shared, -(shared + spread(1, i, (before, here, after))))
            if DEPTH <= i < DEPTH + FINE:
                for part in range(2):
                    kept[part].append(t_here[part] + b[part])
            for part in range(2):
                value = b[part]
                if k > 0:
                    value = 2.0 * value - vector(k - 1, part, i)
                if k + 1 < KRYLOV:
                    buffers[(k + 1) % 2][part, i] = value
                if DEPTH <= i < DEPTH + FINE:
                    kept[2 + part].append(value)
            if len(kept[0]) == 4:
                g = (i - DEPTH) // 4
                for part in range(2):
                    remember(k + 1, part * 4 + g, compact(kept[part]))
                    send_back(2 * k + 2 + part, g, kept[2 + part])
                kept = ([], [], [], [])
            before, here, t_here = here, after, t_after

    def product(r, s):
        terms = []
        for at in range(8):
            a, b = images[r, at], images[s, at]
            ah, al, bh, bl = halves[0, r, at], halves[1, r, at], halves[0, s, at], halves[1, s, at]
            p = a * b
            terms.append((p, ((ah * bh - p) + ah * bl + al * bh) + al * bl))
        return total_of(terms)

    pairs = {
        slot_of(r - 1, s - 1): (r, s) for r in range(1, KRYLOV + 1) for s in range(r + 1)
    }
    for group in range(16):
        found = [pairs.get(8 * group + i) for i in range(8)]
        if None not in found:
            values = [product(*pair) for pair in found]
            for d in (4, 2, 1):
                values = [merge(values[i], values[i + d], d) for i in range(d)]
            value = values[0]
        elif any(found):
            (pair,) = (pair for pair in found if pair)
            value = fold_sublanes(product(*pair))
        else:
            value = (jnp.zeros((8, 128), f32),) * 2
        acc[0, pl.ds(group * 8, 8), :] = value[0]
        acc[1, pl.ds(group * 8, 8), :] = value[1]
    turned = acc[0].T, acc[1].T
    value = fold_sublanes(
        total_of((turned[0][8 * i : 8 * i + 8], turned[1][8 * i : 8 * i + 8]) for i in range(16))
    )
    row = jnp.where(is_high(), value[0], turn(value[1], 64))
    for i in range(sums.shape[0] // 8):
        sums[pl.ds(8 * i, 8), :] = row


def is_high():
    return (lanes() < 64) | (lanes() == 64 + UNIQUE)


def low_words(error):
    return turn(jnp.where(lanes() < UNIQUE, error, 0.0), 64)


def sum_kernel(received, _, back):
    zero = jnp.zeros((8, 128), f32)
    groups = range(received.shape[0] // 8)
    high, error = fold_sublanes(total_of((received[pl.ds(8 * i, 8), :], zero) for i in groups))
    row = jnp.where(is_high(), high, high + low_words(error))
    back[pl.ds(SUMS, 8, stride=BACK), :] = row


def solve_kernel(received, solution, residual, rows):
    def take(array, g):
        return received[pl.ds(array * 4 + g, 8, stride=BACK), :]

    zero = jnp.zeros((8, 128), f32)
    high, error = fold_sublanes((received[pl.ds(SUMS, 8, stride=BACK), :], zero))
    error = jnp.where(lanes() < UNIQUE, error + turn(high, 64), error)
    row, lane = sublanes(16), lanes(16)
    matrix = []
    for n, part in enumerate((high, error)):
        part = jnp.concatenate([part, part], 0)
        value = jnp.zeros((16, 128), f32)
        for r in range(KRYLOV):
            value = jnp.where(row == r, turn(part, -slot_of(r, 0)), value)
        value = jnp.where(lane <= row, value, 0.0)
        flipped = jnp.concatenate([value, jnp.zeros((112, 128), f32)], 0).T[:16]
        value = jnp.where(lane <= row, value, flipped)
        right = jnp.zeros((16, 128), f32)
        for r in range(KRYLOV):
            right = jnp.where(row == r, turn(part, KRYLOV - slot_of(r, -1)), right)
        matrix.append(jnp.where(lane == KRYLOV, right, value))
    matrix = quick_sum(*matrix)
    for j in range(KRYLOV):
        pivot_row = tuple(jnp.broadcast_to(part[j : j + 1, :], (8, 128)) for part in matrix)
        pivot = tuple(jnp.broadcast_to(part[j : j + 1, j : j + 1], (8, 128)) for part in matrix)
        scaled = dd_mul(pivot_row, dd_inverse(pivot))
        scaled = tuple(jnp.concatenate([part, part], 0) for part in scaled)
        column = tuple(-jnp.broadcast_to(part[:, j : j + 1], (16, 128)) for part in matrix)
        rest = dd_add(matrix, dd_mul(column, scaled))
        matrix = tuple(jnp.where(row == j, a, b) for a, b in zip(scaled, rest))
    coeffs = [
        jnp.broadcast_to(matrix[0][k : k + 1, KRYLOV : KRYLOV + 1], (8, 128))
        for k in range(KRYLOV)
    ]
    image = [y for y in coeffs] + [jnp.zeros((8, 128), f32)]
    for k in range(KRYLOV):
        image[k + 1] = image[k + 1] + (coeffs[k] if k == 0 else 0.5 * coeffs[k])
        if k > 0:
            image[k - 1] = image[k - 1] + 0.5 * coeffs[k]
    image[0] = image[0] - 1.0
    for g in range(FINE // 4):
        combined, left = [], []
        for part in range(2):
            vectors = [take(2 * m + part, g) for m in range(KRYLOV + 1)]
            combined.append(sum(coeffs[k] * vectors[k] for k in range(KRYLOV)))
            left.append(-sum(image[m] * vectors[m] for m in range(KRYLOV + 1)))
        b = [take(2 * KRYLOV + 2 + n, g) for n in range(3)]
        v = [
            b[0] * combined[0] + b[1] * combined[1],
            b[1] * combined[0] + b[2] * combined[1],
        ]
        for j, value in enumerate(swap_blocks(v + left, 8)):
            rows[pl.ds(4 * g + j, 8, stride=FINE), :] = value
    turned = rows[...].T
    for f in range(4):
        ref = solution if f < 2 else residual
        for x in range(4):
            ref[f % 2, x] = turned[x * 32 + f * 8 : x * 32 + f * 8 + 8]


def shape(*dims):
    return jax.ShapeDtypeStruct(dims, f32)


def held(*dims):
    return pltpu.VMEM(dims, f32)


def near(*values):
    return tuple(pltpu.with_memory_space_constraint(v, pltpu.VMEM) for v in values)


def scratch(*dims):
    return pltpu.VMEM(dims, f32)


def body(source, sigma_intra, sigma_extra, membrane):
    nx, nz = (lax.axis_size(a) for a in ("gx", "gz"))
    ny = lax.axis_size(GY)
    packed = pl.pallas_call(pack_kernel, out_shape=held(16 * ROWS, 128))(
        source, sigma_intra, sigma_extra, membrane
    )
    pair = lax.all_to_all(packed.reshape(16, ROWS, 1, 128), ("gx", "gy_1"), 0, 0, tiled=True)
    (pair,) = near(pair.reshape(-1, 128))
    wide, thin = pl.pallas_call(
        choose_kernel, out_shape=(held(8 * WIDE, 128), held(8 * THIN, 128))
    )(pair)
    across = [(i, i + 1) for i in range(1, ny - 1, 2)]
    wide = lax.ppermute(wide, GY, across + [(b, a) for a, b in across])
    thin = lax.ppermute(
        thin,
        GY,
        [(i, i - 2) for i in range(2, ny, 2)] + [(i, i + 2) for i in range(1, ny - 2, 2)],
    )
    halo = wide, thin
    planes, first, final = pl.pallas_call(
        plane_kernel,
        out_shape=(
            held(FIELDS, FINE, 8, 128),
            held(FIELDS, SENT, 8, 128),
            held(FIELDS, SENT, 8, 128),
        ),
    )(*near(pair, *halo))

    def place(c):
        return (c % nx) * nz + c // nx

    up = [(place(c), place(c + 1)) for c in range(nx * nz - 1)]
    low = lax.ppermute(final, ("gx", "gz"), up)
    high = lax.ppermute(first, ("gx", "gz"), [(b, a) for a, b in up])

    sums, back = pl.pallas_call(
        cycle_kernel,
        out_shape=(held(ny * nz, 128), held(8 * BACK, 128)),
        scratch_shapes=[
            scratch(6, EXT, 8, 128),
            scratch(4, EXT, 8, 128),
            scratch(2, EXT, 8, 128),
            scratch(2, EXT, 8, 128),
            scratch(KRYLOV + 1, 8, 8, 128),
            scratch(2, KRYLOV + 1, 8, 8, 128),
            scratch(2, 128, 128),
        ],
    )(*near(planes, low, high))

    got = lax.all_to_all(sums.reshape(-1, 1, 128), GY + ("gz",), 0, 0, tiled=True)
    back = pl.pallas_call(
        sum_kernel, out_shape=held(8 * BACK, 128), input_output_aliases={1: 0}
    )(*near(got.reshape(-1, 128), back))
    got = lax.all_to_all(back.reshape(8, BACK, 1, 128), "gx", 0, 0, tiled=True)
    return pl.pallas_call(
        solve_kernel,
        out_shape=(shape(2, 4, 8, 128), shape(2, 4, 8, 128)),
        scratch_shapes=[scratch(128, 128)],
    )(*near(got.reshape(-1, 128)))


def solution(mesh):
    nx, ny, nz = (mesh.shape[a] for a in ("gx", "gy", "gz"))
    pairs = Mesh(mesh.devices.reshape(nx, ny // 2, 2, nz), ("gx", *GY, "gz"))
    spread = P(None, "gx", GY, "gz")
    return jax.shard_map(
        body,
        mesh=pairs,
        in_specs=(spread, spread, spread, P("gx", GY, "gz")),
        out_specs=(spread, spread),
        check_vma=False,
    )
```

```python
import jax
import jax.numpy as jnp
from jax import lax
from jax.experimental import pallas as pl
from jax.experimental.pallas import tpu as pltpu
from jax.sharding import Mesh
from jax.sharding import PartitionSpec as P

KRYLOV = 10
DEPTH = KRYLOV + 1
FINE = 16
EXT = FINE + 2 * DEPTH
SENT = 7
FIELDS = 9
ROWS = 36
WIDE, THIN = 56, 20
BACK = 101
SUMS = 4 * (2 * KRYLOV + 5)
UNIQUE = KRYLOV * (KRYLOV + 1) // 2
f32 = jnp.float32
GY = ("gy_0", "gy_1")


def lanes(rows=8):
    return lax.broadcasted_iota(jnp.int32, (rows, 128), 1)


def sublanes(rows=8):
    return lax.broadcasted_iota(jnp.int32, (rows, 128), 0)


def turn(v, by):
    return v if by % 128 == 0 else pltpu.roll(v, by % 128, 1)


def sink(v, by):
    return pltpu.roll(v, by % 8, 0)


def is_reversed():
    return lax.axis_index("gz") % 2 == 1


def backwards(v):
    v = sink(v, 4)
    for d in (2, 1):
        v = jnp.where((sublanes() & d) == 0, sink(v, -d), sink(v, d))
    return v


def two_sum(a, b):
    s = a + b
    z = s - a
    return s, (a - (s - z)) + (b - z)


def quick_sum(a, b):
    s = a + b
    return s, b - (s - a)


def split(a):
    c = a * 4097.0
    high = c - (c - a)
    return high, a - high


def two_prod(a, b):
    p = a * b
    ah, al = split(a)
    bh, bl = split(b)
    return p, ((ah * bh - p) + ah * bl + al * bh) + al * bl


def dd_add(a, b):
    s, e = two_sum(a[0], b[0])
    return quick_sum(s, e + (a[1] + b[1]))


def dd_mul(a, b):
    p, e = two_prod(a[0], b[0])
    return quick_sum(p, e + (a[0] * b[1] + a[1] * b[0]))


def dd_inverse(a):
    x = 1.0 / a[0]
    p, e = two_prod(a[0], x)
    return quick_sum(x, x * (((1.0 - p) - e) - a[1] * x))


def add_pairs(a, b):
    s, e = two_sum(a[0], b[0])
    return s, e + (a[1] + b[1])


def total_of(pairs):
    pairs = list(pairs)
    while len(pairs) > 1:
        pairs = [
            add_pairs(pairs[i], pairs[i + 1]) if i + 1 < len(pairs) else pairs[i]
            for i in range(0, len(pairs), 2)
        ]
    return pairs[0]


def fold_sublanes(a):
    for by in (4, 2, 1):
        a = add_pairs(a, (sink(a[0], by), sink(a[1], by)))
    return quick_sum(*a)


def merge(a, b, d):
    low = (sublanes() & d) == 0
    return add_pairs(
        tuple(jnp.where(low, x, y) for x, y in zip(a, b)),
        tuple(jnp.where(low, sink(x, -d), sink(y, d)) for x, y in zip(a, b)),
    )


def swap_blocks(v, width):
    v = list(v)
    block = lanes() // width
    d = len(v) // 2
    while d >= 1:
        low = (block & d) == 0
        for k in range(len(v)):
            if k & d == 0:
                a, b = v[k], v[k + d]
                v[k] = jnp.where(low, a, turn(b, width * d))
                v[k + d] = jnp.where(low, turn(a, -width * d), b)
        d //= 2
    return v


def pack_kernel(source, intra, extra, membrane, out):
    refs = [(intra, 0), (intra, 1), (intra, 2), (extra, 0), (extra, 1), (extra, 2), (source, 0), (source, 1)]
    top = sublanes() < 4
    lower, upper = [], []
    for x in range(4):
        for f in range(0, 8, 2):
            a, b = refs[f][0][refs[f][1], x], refs[f + 1][0][refs[f + 1][1], x]
            lower.append(jnp.where(top, a, sink(b, 4)))
            upper.append(jnp.where(top, sink(a, 4), b))
    empty = jnp.zeros((24, 128), f32)
    last = []
    for x in range(4):
        last += [membrane[x], empty]
    lower, upper, last = (jnp.concatenate(part, 0).T for part in (lower, upper, last))
    group = (lanes() % 32) // 8
    chunks = []
    for j in range(8):
        a, b = last[16 * j : 16 * j + 8], last[16 * j + 8 : 16 * j + 16]
        m = jnp.where(group == 2, turn(b, 16), turn(sink(b, 4), 24))
        m = jnp.where(group == 1, turn(sink(a, 4), 8), m)
        m = jnp.where(group == 0, a, m)
        chunks.append((lower[16 * j : 16 * j + 16], m, upper[16 * j : 16 * j + 16]))
    for j in range(8):
        picked = [jnp.where(is_reversed(), a, b) for a, b in zip(chunks[7 - j], chunks[j])]
        for at in (2 * j * ROWS, (2 * j + 1) * ROWS):
            out[pl.ds(at, 16), :] = picked[0]
            out[pl.ds(at + 16, 4), :] = picked[1][:4]
            out[pl.ds(at + 20, 16), :] = picked[2]


def choose_kernel(pair, wide, thin):
    odd = lax.axis_index("gy_1") == 1
    for s in range(8):
        at = 2 * ROWS * s
        rows = pair[pl.ds(at + 16, WIDE), :], pair[pl.ds(at, WIDE), :]
        wide[pl.ds(WIDE * s, WIDE), :] = jnp.where(odd, *rows)
        rows = pair[pl.ds(at + 2 * ROWS - THIN, THIN), :], pair[pl.ds(at, THIN), :]
        thin[pl.ds(THIN * s, THIN), :] = jnp.where(odd, *rows)


def plane_kernel(pair, wide, thin, out, first, final):
    y = lanes() % 32
    odd = lax.axis_index("gy_1")
    is_even = jnp.full((8, 128), odd, jnp.int32) == 0

    def take(ref, row, height):
        return ref[pl.ds(row, 8, stride=height), :]

    def ordered(own, far, last):
        even = far + own + last
        other = last + own + far
        return [a if a is b else jnp.where(is_even, a, b) for a, b in zip(even, other)]

    def plane(r, n):
        z, shift = 4 * n + r, 8 * n
        own = [take(pair, at + z, 2 * ROWS) for at in (0, 20, 36, 56)]
        far = [take(wide, at + z, WIDE) for at in (4 - 4 * odd, 20, 40 - 4 * odd)]
        v = swap_blocks(ordered(own, far, [take(thin, 4 * odd + z, THIN)]), 4)
        own = [take(pair, at + r, 2 * ROWS) for at in (16, 52)]
        far = [take(wide, at + 16 * odd + r, WIDE) for at in (0, 36)]
        parts = ordered(own, far, [take(thin, 16 - 16 * odd + r, THIN)])
        m = turn(parts[4], 28 - shift)
        for n in (3, 2, 1, 0):
            m = jnp.where(y < 8 * n + 4, turn(parts[n], 8 * n - 4 - shift), m)
        return v + [m]

    def four(r, _):
        for n in range(FINE // 4):
            for f, value in enumerate(plane(r, n)):
                out[f, 4 * n + r] = value
        return _

    lax.fori_loop(0, 4, four, 0)

    def edges(f, _):
        for ref, at in ((first, lambda d: d - 1), (final, lambda d: FINE - d)):
            for d in range(1, SENT + 1):
                value = out[f, at(d)]
                if 2 < d < SENT:
                    inner = (y > d) & (y < 31 - d)
                    value = jnp.where(inner, value, turn(out[f, at(14 - d)], 16))
                ref[f, d - 1] = value
        return _

    lax.fori_loop(0, FIELDS, edges, 0)


def x_up(v):
    v = turn(v, -32)
    return jnp.where(lanes() < 96, v, sink(v, -1))


def x_down(v):
    v = turn(v, 32)
    return jnp.where(lanes() >= 32, v, sink(v, 1))


def y_up(v):
    return turn(v, -1)


def y_down(v):
    return turn(v, 1)


def slot_of(r, s):
    if s < 0:
        return UNIQUE + r if r < KRYLOV - 1 else 64 + UNIQUE
    return r * (r + 1) // 2 + s


def cycle_kernel(main, low, high, sums, back, face, inv, ta, tb, images, halves, acc):
    lane = lanes()
    ix = sublanes() * 4 + lane // 32
    last_x, first_x = ix == 31, ix == 0

    def far(ref, f, d):
        return ref[f, d - 1] if d <= SENT else turn(ref[f, 13 - d], -16)

    def field(f, i):
        if i < DEPTH:
            return far(low, f, DEPTH - i)
        if i < DEPTH + FINE:
            return main[f, i - DEPTH]
        return far(high, f, i - DEPTH - FINE + 1)

    block = (lane % 32) // 8

    def compact(planes):
        value = turn(planes[3], 12)
        for j in (2, 1, 0):
            value = jnp.where(block == j, turn(planes[j], 8 * j - 12), value)
        return value

    def send_back(array, g, planes):
        back[pl.ds(array * 4 + g, 8, stride=BACK), :] = compact(planes)

    blocks_kept = ([], [], [])
    sz = [field(2, 0), field(5, 0)]
    low_z = [None, None]
    for i in range(EXT - 1):
        diagonals = []
        for s in range(2):
            above = field(s * 3 + 2, i + 1)
            up_z = 0.5 * (sz[s] + above)
            face[s * 3 + 2, i] = up_z
            if i > 0:
                sx, sy = field(s * 3, i), field(s * 3 + 1, i)
                up_x = 0.5 * (sx + jnp.where(last_x, 0.0, x_up(sx)))
                low_x = 0.5 * (sx + jnp.where(first_x, 0.0, x_down(sx)))
                up_y = 0.5 * (sy + y_up(sy))
                low_y = 0.5 * (sy + y_down(sy))
                face[s * 3, i] = jnp.where(last_x, 0.0, up_x)
                face[s * 3 + 1, i] = up_y
                diagonals.append(up_x + low_x + up_y + low_y + up_z + low_z[s])
            sz[s], low_z[s] = above, up_z
        if i > 0:
            di, de = diagonals
            m = field(8, i)
            det = m * di + m * de + di * de
            inside = m > 0.0
            scale = jnp.where(inside, 1.0 / jnp.where(inside, det, 1.0), 0.0)
            inv[0, i] = de * scale
            inv[1, i] = m * scale
            inv[2, i] = -di * scale
            inv[3, i] = (m + di) * scale
            if DEPTH <= i < DEPTH + FINE:
                for n, value in enumerate(((di + de) * scale, -di * scale, (m + di) * scale)):
                    blocks_kept[n].append(value)
                if len(blocks_kept[0]) == 4:
                    for n in range(3):
                        send_back(2 * KRYLOV + 2 + n, (i - DEPTH) // 4, blocks_kept[n])
                    blocks_kept = ([], [], [])

    def remember(r, at, value):
        images[r, at] = value
        halves[0, r, at], halves[1, r, at] = split(value)

    for part in range(2):
        for g in range(FINE // 4):
            planes = [main[6 + part, 4 * g + j] for j in range(4)]
            remember(0, part * 4 + g, compact(planes))
            send_back(part, g, planes)

    buffers = (ta, tb)

    def vector(k, part, i):
        return field(6 + part, i) if k == 0 else buffers[k % 2][part, i]

    for k in range(KRYLOV):

        def blocks(i):
            v, p = vector(k, 0, i), vector(k, 1, i)
            return (inv[0, i] * v + inv[1, i] * p, inv[2, i] * v + inv[3, i] * p), (v, p)

        def spread(s, i, u):
            fx, fy = face[s * 3, i], face[s * 3 + 1, i]
            across = fx * x_up(u[1][s]) + x_down(fx * u[1][s])
            along = fy * y_up(u[1][s]) + y_down(fy * u[1][s])
            deep = face[s * 3 + 2, i] * u[2][s] + face[s * 3 + 2, i - 1] * u[0][s]
            return across + along + deep

        start, end = 2 + k, EXT - 2 - k
        (before, _), (here, t_here) = blocks(start - 1), blocks(start)
        kept = ([], [], [], [])
        for i in range(start, end):
            after, t_after = blocks(i + 1)
            shared = spread(0, i, (before, here, after))
            b = (-shared, -(shared + spread(1, i, (before, here, after))))
            if DEPTH <= i < DEPTH + FINE:
                for part in range(2):
                    kept[part].append(t_here[part] + b[part])
            for part in range(2):
                value = b[part]
                if k > 0:
                    value = 2.0 * value - vector(k - 1, part, i)
                if k + 1 < KRYLOV:
                    buffers[(k + 1) % 2][part, i] = value
                if DEPTH <= i < DEPTH + FINE:
                    kept[2 + part].append(value)
            if len(kept[0]) == 4:
                g = (i - DEPTH) // 4
                for part in range(2):
                    remember(k + 1, part * 4 + g, compact(kept[part]))
                    send_back(2 * k + 2 + part, g, kept[2 + part])
                kept = ([], [], [], [])
            before, here, t_here = here, after, t_after

    def product(r, s):
        terms = []
        for at in range(8):
            a, b = images[r, at], images[s, at]
            ah, al, bh, bl = halves[0, r, at], halves[1, r, at], halves[0, s, at], halves[1, s, at]
            p = a * b
            terms.append((p, ((ah * bh - p) + ah * bl + al * bh) + al * bl))
        return total_of(terms)

    pairs = {
        slot_of(r - 1, s - 1): (r, s) for r in range(1, KRYLOV + 1) for s in range(r + 1)
    }
    for group in range(16):
        found = [pairs.get(8 * group + i) for i in range(8)]
        if None not in found:
            values = [product(*pair) for pair in found]
            for d in (4, 2, 1):
                values = [merge(values[i], values[i + d], d) for i in range(d)]
            value = values[0]
        elif any(found):
            (pair,) = (pair for pair in found if pair)
            value = fold_sublanes(product(*pair))
        else:
            value = (jnp.zeros((8, 128), f32),) * 2
        acc[0, pl.ds(group * 8, 8), :] = value[0]
        acc[1, pl.ds(group * 8, 8), :] = value[1]
    turned = acc[0].T, acc[1].T
    value = fold_sublanes(
        total_of((turned[0][8 * i : 8 * i + 8], turned[1][8 * i : 8 * i + 8]) for i in range(16))
    )
    row = jnp.where(is_high(), value[0], turn(value[1], 64))
    for i in range(sums.shape[0] // 8):
        sums[pl.ds(8 * i, 8), :] = row


def is_high():
    return (lanes() < 64) | (lanes() == 64 + UNIQUE)


def low_words(error):
    return turn(jnp.where(lanes() < UNIQUE, error, 0.0), 64)


def sum_kernel(received, _, back):
    zero = jnp.zeros((8, 128), f32)
    groups = range(received.shape[0] // 8)
    high, error = fold_sublanes(total_of((received[pl.ds(8 * i, 8), :], zero) for i in groups))
    row = jnp.where(is_high(), high, high + low_words(error))
    back[pl.ds(SUMS, 8, stride=BACK), :] = row


def solve_kernel(received, solution, residual, rows):
    def take(array, g):
        return received[pl.ds(array * 4 + g, 8, stride=BACK), :]

    zero = jnp.zeros((8, 128), f32)
    high, error = fold_sublanes((received[pl.ds(SUMS, 8, stride=BACK), :], zero))
    error = jnp.where(lanes() < UNIQUE, error + turn(high, 64), error)
    row, lane = sublanes(16), lanes(16)
    matrix = []
    for n, part in enumerate((high, error)):
        part = jnp.concatenate([part, part], 0)
        value = jnp.zeros((16, 128), f32)
        for r in range(KRYLOV):
            value = jnp.where(row == r, turn(part, -slot_of(r, 0)), value)
        value = jnp.where(lane <= row, value, 0.0)
        flipped = jnp.concatenate([value, jnp.zeros((112, 128), f32)], 0).T[:16]
        value = jnp.where(lane <= row, value, flipped)
        right = jnp.zeros((16, 128), f32)
        for r in range(KRYLOV):
            right = jnp.where(row == r, turn(part, KRYLOV - slot_of(r, -1)), right)
        matrix.append(jnp.where(lane == KRYLOV, right, value))
    matrix = quick_sum(*matrix)
    for j in range(KRYLOV):
        pivot_row = tuple(jnp.broadcast_to(part[j : j + 1, :], (8, 128)) for part in matrix)
        pivot = tuple(jnp.broadcast_to(part[j : j + 1, j : j + 1], (8, 128)) for part in matrix)
        scaled = dd_mul(pivot_row, dd_inverse(pivot))
        scaled = tuple(jnp.concatenate([part, part], 0) for part in scaled)
        column = tuple(-jnp.broadcast_to(part[:, j : j + 1], (16, 128)) for part in matrix)
        rest = dd_add(matrix, dd_mul(column, scaled))
        matrix = tuple(jnp.where(row == j, a, b) for a, b in zip(scaled, rest))
    coeffs = [
        jnp.broadcast_to(matrix[0][k : k + 1, KRYLOV : KRYLOV + 1], (8, 128))
        for k in range(KRYLOV)
    ]
    image = [y for y in coeffs] + [jnp.zeros((8, 128), f32)]
    for k in range(KRYLOV):
        image[k + 1] = image[k + 1] + (coeffs[k] if k == 0 else 0.5 * coeffs[k])
        if k > 0:
            image[k - 1] = image[k - 1] + 0.5 * coeffs[k]
    image[0] = image[0] - 1.0
    for g in range(FINE // 4):
        combined, left = [], []
        for part in range(2):
            vectors = [take(2 * m + part, g) for m in range(KRYLOV + 1)]
            combined.append(sum(coeffs[k] * vectors[k] for k in range(KRYLOV)))
            left.append(-sum(image[m] * vectors[m] for m in range(KRYLOV + 1)))
        b = [take(2 * KRYLOV + 2 + n, g) for n in range(3)]
        v = [
            b[0] * combined[0] + b[1] * combined[1],
            b[1] * combined[0] + b[2] * combined[1],
        ]
        for j, value in enumerate(swap_blocks(v + left, 8)):
            value = jnp.where(is_reversed(), backwards(value), value)
            rows[pl.ds(4 * g + j, 8, stride=FINE), :] = value
    turned = rows[...].T
    for f in range(4):
        ref = solution if f < 2 else residual
        for x in range(4):
            ref[f % 2, x] = turned[x * 32 + f * 8 : x * 32 + f * 8 + 8]


def shape(*dims):
    return jax.ShapeDtypeStruct(dims, f32)


def held(*dims):
    return pltpu.VMEM(dims, f32)


def near(*values):
    return tuple(pltpu.with_memory_space_constraint(v, pltpu.VMEM) for v in values)


def scratch(*dims):
    return pltpu.VMEM(dims, f32)


def body(source, sigma_intra, sigma_extra, membrane):
    nx, nz = (lax.axis_size(a) for a in ("gx", "gz"))
    ny = lax.axis_size(GY)
    packed = pl.pallas_call(pack_kernel, out_shape=held(16 * ROWS, 128))(
        source, sigma_intra, sigma_extra, membrane
    )
    pair = lax.all_to_all(packed.reshape(16, ROWS, 1, 128), ("gx", "gy_1"), 0, 0, tiled=True)
    (pair,) = near(pair.reshape(-1, 128))
    wide, thin = pl.pallas_call(
        choose_kernel, out_shape=(held(8 * WIDE, 128), held(8 * THIN, 128))
    )(pair)
    across = [(i, i + 1) for i in range(1, ny - 1, 2)]
    wide = lax.ppermute(wide, GY, across + [(b, a) for a, b in across])
    thin = lax.ppermute(
        thin,
        GY,
        [(i, i - 2) for i in range(2, ny, 2)] + [(i, i + 2) for i in range(1, ny - 2, 2)],
    )
    halo = wide, thin
    planes, first, final = pl.pallas_call(
        plane_kernel,
        out_shape=(
            held(FIELDS, FINE, 8, 128),
            held(FIELDS, SENT, 8, 128),
            held(FIELDS, SENT, 8, 128),
        ),
    )(*near(pair, *halo))

    def place(c):
        block, j = c // nx, c % nx
        return (j if block % 2 == 0 else nx - 1 - j) * nz + block

    up = [(place(c), place(c + 1)) for c in range(nx * nz - 1)]
    low = lax.ppermute(final, ("gx", "gz"), up)
    high = lax.ppermute(first, ("gx", "gz"), [(b, a) for a, b in up])

    sums, back = pl.pallas_call(
        cycle_kernel,
        out_shape=(held(ny * nz, 128), held(8 * BACK, 128)),
        scratch_shapes=[
            scratch(6, EXT, 8, 128),
            scratch(4, EXT, 8, 128),
            scratch(2, EXT, 8, 128),
            scratch(2, EXT, 8, 128),
            scratch(KRYLOV + 1, 8, 8, 128),
            scratch(2, KRYLOV + 1, 8, 8, 128),
            scratch(2, 128, 128),
        ],
    )(*near(planes, low, high))

    got = lax.all_to_all(sums.reshape(-1, 1, 128), GY + ("gz",), 0, 0, tiled=True)
    back = pl.pallas_call(
        sum_kernel, out_shape=held(8 * BACK, 128), input_output_aliases={1: 0}
    )(*near(got.reshape(-1, 128), back))
    got = lax.all_to_all(back.reshape(8, BACK, 1, 128), "gx", 0, 0, tiled=True)
    return pl.pallas_call(
        solve_kernel,
        out_shape=(shape(2, 4, 8, 128), shape(2, 4, 8, 128)),
        scratch_shapes=[scratch(128, 128)],
    )(*near(got.reshape(-1, 128)))


def solution(mesh):
    nx, ny, nz = (mesh.shape[a] for a in ("gx", "gy", "gz"))
    pairs = Mesh(mesh.devices.reshape(nx, ny // 2, 2, nz), ("gx", *GY, "gz"))
    spread = P(None, "gx", GY, "gz")
    return jax.shard_map(
        body,
        mesh=pairs,
        in_specs=(spread, spread, spread, P("gx", GY, "gz")),
        out_specs=(spread, spread),
        check_vma=False,
    )
```

```python
import jax
import jax.numpy as jnp
from jax import lax
from jax.experimental import pallas as pl
from jax.experimental.pallas import tpu as pltpu
from jax.sharding import Mesh
from jax.sharding import PartitionSpec as P

KRYLOV = 10
DEPTH = KRYLOV + 1
FINE = 16
EXT = FINE + 2 * DEPTH
SENT = 7
FIELDS = 9
ROWS = 36
WIDE, THIN = 56, 20
BACK = 101
SUMS = 4 * (2 * KRYLOV + 5)
UNIQUE = KRYLOV * (KRYLOV + 1) // 2
f32 = jnp.float32
GY = ("gy_0", "gy_1")


def lanes(rows=8):
    return lax.broadcasted_iota(jnp.int32, (rows, 128), 1)


def sublanes(rows=8):
    return lax.broadcasted_iota(jnp.int32, (rows, 128), 0)


def turn(v, by):
    return v if by % 128 == 0 else pltpu.roll(v, by % 128, 1)


def sink(v, by):
    return pltpu.roll(v, by % 8, 0)


def is_reversed():
    return lax.axis_index("gz") % 2 == 1


def backwards(v):
    v = sink(v, 4)
    for d in (2, 1):
        v = jnp.where((sublanes() & d) == 0, sink(v, -d), sink(v, d))
    return v


def two_sum(a, b):
    s = a + b
    z = s - a
    return s, (a - (s - z)) + (b - z)


def quick_sum(a, b):
    s = a + b
    return s, b - (s - a)


def split(a):
    c = a * 4097.0
    high = c - (c - a)
    return high, a - high


def two_prod(a, b):
    p = a * b
    ah, al = split(a)
    bh, bl = split(b)
    return p, ((ah * bh - p) + ah * bl + al * bh) + al * bl


def dd_add(a, b):
    s, e = two_sum(a[0], b[0])
    return quick_sum(s, e + (a[1] + b[1]))


def dd_mul(a, b):
    p, e = two_prod(a[0], b[0])
    return quick_sum(p, e + (a[0] * b[1] + a[1] * b[0]))


def dd_inverse(a):
    x = 1.0 / a[0]
    p, e = two_prod(a[0], x)
    return quick_sum(x, x * (((1.0 - p) - e) - a[1] * x))


def add_pairs(a, b):
    s, e = two_sum(a[0], b[0])
    return s, e + (a[1] + b[1])


def total_of(pairs):
    pairs = list(pairs)
    while len(pairs) > 1:
        pairs = [
            add_pairs(pairs[i], pairs[i + 1]) if i + 1 < len(pairs) else pairs[i]
            for i in range(0, len(pairs), 2)
        ]
    return pairs[0]


def fold_sublanes(a):
    for by in (4, 2, 1):
        a = add_pairs(a, (sink(a[0], by), sink(a[1], by)))
    return quick_sum(*a)


def merge(a, b, d):
    low = (sublanes() & d) == 0
    return add_pairs(
        tuple(jnp.where(low, x, y) for x, y in zip(a, b)),
        tuple(jnp.where(low, sink(x, -d), sink(y, d)) for x, y in zip(a, b)),
    )


def swap_blocks(v, width):
    v = list(v)
    block = lanes() // width
    d = len(v) // 2
    while d >= 1:
        low = (block & d) == 0
        for k in range(len(v)):
            if k & d == 0:
                a, b = v[k], v[k + d]
                v[k] = jnp.where(low, a, turn(b, width * d))
                v[k + d] = jnp.where(low, turn(a, -width * d), b)
        d //= 2
    return v


def pack_kernel(source, intra, extra, membrane, out):
    refs = [(intra, 0), (intra, 1), (intra, 2), (extra, 0), (extra, 1), (extra, 2), (source, 0), (source, 1)]
    top = sublanes() < 4
    lower, upper = [], []
    for x in range(4):
        for f in range(0, 8, 2):
            a, b = refs[f][0][refs[f][1], x], refs[f + 1][0][refs[f + 1][1], x]
            lower.append(jnp.where(top, a, sink(b, 4)))
            upper.append(jnp.where(top, sink(a, 4), b))
    empty = jnp.zeros((24, 128), f32)
    last = []
    for x in range(4):
        last += [membrane[x], empty]
    lower, upper, last = (jnp.concatenate(part, 0).T for part in (lower, upper, last))
    group = (lanes() % 32) // 8
    chunks = []
    for j in range(8):
        a, b = last[16 * j : 16 * j + 8], last[16 * j + 8 : 16 * j + 16]
        m = jnp.where(group == 2, turn(b, 16), turn(sink(b, 4), 24))
        m = jnp.where(group == 1, turn(sink(a, 4), 8), m)
        m = jnp.where(group == 0, a, m)
        chunks.append((lower[16 * j : 16 * j + 16], m, upper[16 * j : 16 * j + 16]))
    for j in range(8):
        picked = [jnp.where(is_reversed(), a, b) for a, b in zip(chunks[7 - j], chunks[j])]
        for at in (2 * j * ROWS, (2 * j + 1) * ROWS):
            out[pl.ds(at, 16), :] = picked[0]
            out[pl.ds(at + 16, 4), :] = picked[1][:4]
            out[pl.ds(at + 20, 16), :] = picked[2]


def choose_kernel(pair, wide, thin):
    odd = lax.axis_index("gy_1") == 1
    for s in range(8):
        at = 2 * ROWS * s
        rows = pair[pl.ds(at + 16, WIDE), :], pair[pl.ds(at, WIDE), :]
        wide[pl.ds(WIDE * s, WIDE), :] = jnp.where(odd, *rows)
        rows = pair[pl.ds(at + 2 * ROWS - THIN, THIN), :], pair[pl.ds(at, THIN), :]
        thin[pl.ds(THIN * s, THIN), :] = jnp.where(odd, *rows)


def plane_kernel(pair, wide, thin, out, first, final):
    y = lanes() % 32
    odd = lax.axis_index("gy_1")
    is_even = jnp.full((8, 128), odd, jnp.int32) == 0

    def take(ref, row, height):
        return ref[pl.ds(row, 8, stride=height), :]

    def ordered(own, far, last):
        even = far + own + last
        other = last + own + far
        return [a if a is b else jnp.where(is_even, a, b) for a, b in zip(even, other)]

    def plane(r, n):
        z, shift = 4 * n + r, 8 * n
        own = [take(pair, at + z, 2 * ROWS) for at in (0, 20, 36, 56)]
        far = [take(wide, at + z, WIDE) for at in (4 - 4 * odd, 20, 40 - 4 * odd)]
        v = swap_blocks(ordered(own, far, [take(thin, 4 * odd + z, THIN)]), 4)
        own = [take(pair, at + r, 2 * ROWS) for at in (16, 52)]
        far = [take(wide, at + 16 * odd + r, WIDE) for at in (0, 36)]
        parts = ordered(own, far, [take(thin, 16 - 16 * odd + r, THIN)])
        m = turn(parts[4], 28 - shift)
        for n in (3, 2, 1, 0):
            m = jnp.where(y < 8 * n + 4, turn(parts[n], 8 * n - 4 - shift), m)
        return v + [m]

    def four(r, _):
        for n in range(FINE // 4):
            for f, value in enumerate(plane(r, n)):
                out[f, 4 * n + r] = value
        return _

    lax.fori_loop(0, 4, four, 0)

    def edges(f, _):
        for ref, at in ((first, lambda d: d - 1), (final, lambda d: FINE - d)):
            for d in range(1, SENT + 1):
                value = out[f, at(d)]
                if 2 < d < SENT:
                    inner = (y > d) & (y < 31 - d)
                    value = jnp.where(inner, value, turn(out[f, at(14 - d)], 16))
                ref[f, d - 1] = value
        return _

    lax.fori_loop(0, FIELDS, edges, 0)


def x_up(v):
    v = turn(v, -32)
    return jnp.where(lanes() < 96, v, sink(v, -1))


def x_down(v):
    v = turn(v, 32)
    return jnp.where(lanes() >= 32, v, sink(v, 1))


def y_up(v):
    return turn(v, -1)


def y_down(v):
    return turn(v, 1)


def slot_of(r, s):
    if s < 0:
        return UNIQUE + r if r < KRYLOV - 1 else 64 + UNIQUE
    return r * (r + 1) // 2 + s


def cycle_kernel(main, low, high, sums, back, face, inv, ta, tb, images, halves, acc):
    lane = lanes()
    ix = sublanes() * 4 + lane // 32
    last_x, first_x = ix == 31, ix == 0

    def far(ref, f, d):
        return ref[f, d - 1] if d <= SENT else turn(ref[f, 13 - d], -16)

    def field(f, i):
        if i < DEPTH:
            return far(low, f, DEPTH - i)
        if i < DEPTH + FINE:
            return main[f, i - DEPTH]
        return far(high, f, i - DEPTH - FINE + 1)

    block = (lane % 32) // 8

    def compact(planes):
        value = turn(planes[3], 12)
        for j in (2, 1, 0):
            value = jnp.where(block == j, turn(planes[j], 8 * j - 12), value)
        return value

    def send_back(array, g, planes):
        back[pl.ds(array * 4 + g, 8, stride=BACK), :] = compact(planes)

    blocks_kept = ([], [], [])
    sz = [field(2, 0), field(5, 0)]
    low_z = [None, None]
    for i in range(EXT - 1):
        diagonals = []
        for s in range(2):
            above = field(s * 3 + 2, i + 1)
            up_z = sz[s] + above
            face[s * 3 + 2, i] = up_z
            if i > 0:
                sx, sy = field(s * 3, i), field(s * 3 + 1, i)
                up_x = sx + jnp.where(last_x, 0.0, x_up(sx))
                low_x = sx + jnp.where(first_x, 0.0, x_down(sx))
                up_y = sy + y_up(sy)
                low_y = sy + y_down(sy)
                face[s * 3, i] = jnp.where(last_x, 0.0, up_x)
                face[s * 3 + 1, i] = up_y
                diagonals.append(0.5 * (up_x + low_x + up_y + low_y + up_z + low_z[s]))
            sz[s], low_z[s] = above, up_z
        if i > 0:
            di, de = diagonals
            m = field(8, i)
            det = m * di + m * de + di * de
            inside = m > 0.0
            scale = jnp.where(inside, 1.0 / jnp.where(inside, det, 1.0), 0.0)
            values = (-de * scale, -m * scale, di * scale, -(m + di) * scale)
            for n in range(4):
                inv[n, i] = values[n]
            if DEPTH <= i < DEPTH + FINE:
                for n, value in enumerate(((di + de) * scale, values[2], values[3])):
                    blocks_kept[n].append(value)
                if len(blocks_kept[0]) == 4:
                    for n in range(3):
                        send_back(2 * KRYLOV + 2 + n, (i - DEPTH) // 4, blocks_kept[n])
                    blocks_kept = ([], [], [])

    def remember(r, value):
        size = None
        for v in value:
            size = jnp.abs(v) if size is None else jnp.maximum(size, jnp.abs(v))
        grid = size * 12288.0
        for at, v in enumerate(value):
            high_part = (v + grid) - grid
            images[r, at], halves[0, r, at], halves[1, r, at] = v, high_part, v - high_part

    image = []
    for part in range(2):
        for g in range(FINE // 4):
            planes = [main[6 + part, 4 * g + j] for j in range(4)]
            image.append(compact(planes))
            send_back(part, g, planes)
    remember(0, image)

    buffers = (ta, tb)

    def vector(k, part, i):
        return field(6 + part, i) if k == 0 else buffers[k % 2][part, i]

    for k in range(KRYLOV):

        def blocks(i):
            v, p = vector(k, 0, i), vector(k, 1, i)
            return (inv[0, i] * v + inv[1, i] * p, inv[2, i] * v + inv[3, i] * p), (v, p)

        def spread(s, i, u):
            fx, fy = face[s * 3, i], face[s * 3 + 1, i]
            across = fx * x_up(u[1][s]) + x_down(fx * u[1][s])
            along = fy * y_up(u[1][s]) + y_down(fy * u[1][s])
            deep = face[s * 3 + 2, i] * u[2][s] + face[s * 3 + 2, i - 1] * u[0][s]
            return across + along + deep

        start, end = 2 + k, EXT - 2 - k
        (before, _), (here, t_here) = blocks(start - 1), blocks(start)
        kept = ([], [], [], [])
        image = ([], [])
        for i in range(start, end):
            after, t_after = blocks(i + 1)
            shared = spread(0, i, (before, here, after))
            twice = (shared, shared + spread(1, i, (before, here, after)))
            for part in range(2):
                value = 0.5 * twice[part] if k == 0 else twice[part] - vector(k - 1, part, i)
                if k + 1 < KRYLOV:
                    buffers[(k + 1) % 2][part, i] = value
                if DEPTH <= i < DEPTH + FINE:
                    kept[part].append(t_here[part] + 0.5 * twice[part])
                    kept[2 + part].append(value)
            if len(kept[0]) == 4:
                g = (i - DEPTH) // 4
                for part in range(2):
                    image[part].append(compact(kept[part]))
                    send_back(2 * k + 2 + part, g, kept[2 + part])
                kept = ([], [], [], [])
            before, here, t_here = here, after, t_after
        remember(k + 1, image[0] + image[1])

    def product(r, s):
        exact, rest = [], []
        for at in range(8):
            high_a, low_a, high_b, low_b = (
                halves[n, image, at] for image in (r, s) for n in range(2)
            )
            exact.append(high_a * high_b)
            rest.append(high_a * low_b + low_a * images[s, at])
        while len(exact) > 1:
            exact = [a + b for a, b in zip(exact[::2], exact[1::2])]
            rest = [a + b for a, b in zip(rest[::2], rest[1::2])]
        return exact[0], rest[0]

    pairs = {
        slot_of(r - 1, s - 1): (r, s) for r in range(1, KRYLOV + 1) for s in range(r + 1)
    }
    for group in range(16):
        found = [pairs.get(8 * group + i) for i in range(8)]
        if None not in found:
            values = [product(*pair) for pair in found]
            for d in (4, 2, 1):
                values = [merge(values[i], values[i + d], d) for i in range(d)]
            value = values[0]
        elif any(found):
            (pair,) = (pair for pair in found if pair)
            value = fold_sublanes(product(*pair))
        else:
            value = (jnp.zeros((8, 128), f32),) * 2
        acc[0, pl.ds(group * 8, 8), :] = value[0]
        acc[1, pl.ds(group * 8, 8), :] = value[1]
    turned = acc[0].T, acc[1].T
    value = fold_sublanes(
        total_of((turned[0][8 * i : 8 * i + 8], turned[1][8 * i : 8 * i + 8]) for i in range(16))
    )
    row = jnp.where(is_high(), value[0], turn(value[1], 64))
    for i in range(sums.shape[0] // 8):
        sums[pl.ds(8 * i, 8), :] = row


def is_high():
    return (lanes() < 64) | (lanes() == 64 + UNIQUE)


def low_words(error):
    return turn(jnp.where(lanes() < UNIQUE, error, 0.0), 64)


def sum_kernel(received, _, back):
    zero = jnp.zeros((8, 128), f32)
    groups = range(received.shape[0] // 8)
    high, error = fold_sublanes(total_of((received[pl.ds(8 * i, 8), :], zero) for i in groups))
    row = jnp.where(is_high(), high, high + low_words(error))
    back[pl.ds(SUMS, 8, stride=BACK), :] = row


def solve_kernel(received, solution, residual, rows):
    def take(array, g):
        return received[pl.ds(array * 4 + g, 8, stride=BACK), :]

    zero = jnp.zeros((8, 128), f32)
    high, error = fold_sublanes((received[pl.ds(SUMS, 8, stride=BACK), :], zero))
    error = jnp.where(lanes() < UNIQUE, error + turn(high, 64), error)
    row, lane = sublanes(16), lanes(16)
    matrix = []
    for n, part in enumerate((high, error)):
        part = jnp.concatenate([part, part], 0)
        value = jnp.zeros((16, 128), f32)
        for r in range(KRYLOV):
            value = jnp.where(row == r, turn(part, -slot_of(r, 0)), value)
        value = jnp.where(lane <= row, value, 0.0)
        flipped = jnp.concatenate([value, jnp.zeros((112, 128), f32)], 0).T[:16]
        value = jnp.where(lane <= row, value, flipped)
        right = jnp.zeros((16, 128), f32)
        for r in range(KRYLOV):
            right = jnp.where(row == r, turn(part, KRYLOV - slot_of(r, -1)), right)
        matrix.append(jnp.where(lane == KRYLOV, right, value))
    matrix = quick_sum(*matrix)
    for j in range(KRYLOV):
        pivot_row = tuple(jnp.broadcast_to(part[j : j + 1, :], (8, 128)) for part in matrix)
        pivot = tuple(jnp.broadcast_to(part[j : j + 1, j : j + 1], (8, 128)) for part in matrix)
        scaled = dd_mul(pivot_row, dd_inverse(pivot))
        scaled = tuple(jnp.concatenate([part, part], 0) for part in scaled)
        column = tuple(-jnp.broadcast_to(part[:, j : j + 1], (16, 128)) for part in matrix)
        rest = dd_add(matrix, dd_mul(column, scaled))
        matrix = tuple(jnp.where(row == j, a, b) for a, b in zip(scaled, rest))
    coeffs = [
        jnp.broadcast_to(matrix[0][k : k + 1, KRYLOV : KRYLOV + 1], (8, 128))
        for k in range(KRYLOV)
    ]
    image = [y for y in coeffs] + [jnp.zeros((8, 128), f32)]
    for k in range(KRYLOV):
        image[k + 1] = image[k + 1] + (coeffs[k] if k == 0 else 0.5 * coeffs[k])
        if k > 0:
            image[k - 1] = image[k - 1] + 0.5 * coeffs[k]
    image[0] = image[0] - 1.0
    for g in range(FINE // 4):
        combined, left = [], []
        for part in range(2):
            vectors = [take(2 * m + part, g) for m in range(KRYLOV + 1)]
            combined.append(sum(coeffs[k] * vectors[k] for k in range(KRYLOV)))
            left.append(-sum(image[m] * vectors[m] for m in range(KRYLOV + 1)))
        b = [take(2 * KRYLOV + 2 + n, g) for n in range(3)]
        v = [
            b[0] * combined[0] - b[1] * combined[1],
            -(b[1] * combined[0] + b[2] * combined[1]),
        ]
        for j, value in enumerate(swap_blocks(v + left, 8)):
            value = jnp.where(is_reversed(), backwards(value), value)
            rows[pl.ds(4 * g + j, 8, stride=FINE), :] = value
    turned = rows[...].T
    for f in range(4):
        ref = solution if f < 2 else residual
        for x in range(4):
            ref[f % 2, x] = turned[x * 32 + f * 8 : x * 32 + f * 8 + 8]


def shape(*dims):
    return jax.ShapeDtypeStruct(dims, f32)


def held(*dims):
    return pltpu.VMEM(dims, f32)


def near(*values):
    return tuple(pltpu.with_memory_space_constraint(v, pltpu.VMEM) for v in values)


def scratch(*dims):
    return pltpu.VMEM(dims, f32)


def body(source, sigma_intra, sigma_extra, membrane):
    nx, nz = (lax.axis_size(a) for a in ("gx", "gz"))
    ny = lax.axis_size(GY)
    packed = pl.pallas_call(pack_kernel, out_shape=held(16 * ROWS, 128))(
        source, sigma_intra, sigma_extra, membrane
    )
    pair = lax.all_to_all(packed.reshape(16, ROWS, 1, 128), ("gx", "gy_1"), 0, 0, tiled=True)
    (pair,) = near(pair.reshape(-1, 128))
    wide, thin = pl.pallas_call(
        choose_kernel, out_shape=(held(8 * WIDE, 128), held(8 * THIN, 128))
    )(pair)
    across = [(i, i + 1) for i in range(1, ny - 1, 2)]
    wide = lax.ppermute(wide, GY, across + [(b, a) for a, b in across])
    thin = lax.ppermute(
        thin,
        GY,
        [(i, i - 2) for i in range(2, ny, 2)] + [(i, i + 2) for i in range(1, ny - 2, 2)],
    )
    halo = wide, thin
    planes, first, final = pl.pallas_call(
        plane_kernel,
        out_shape=(
            held(FIELDS, FINE, 8, 128),
            held(FIELDS, SENT, 8, 128),
            held(FIELDS, SENT, 8, 128),
        ),
    )(*near(pair, *halo))

    def place(c):
        block, j = c // nx, c % nx
        return (j if block % 2 == 0 else nx - 1 - j) * nz + block

    up = [(place(c), place(c + 1)) for c in range(nx * nz - 1)]
    low = lax.ppermute(final, ("gx", "gz"), up)
    high = lax.ppermute(first, ("gx", "gz"), [(b, a) for a, b in up])

    sums, back = pl.pallas_call(
        cycle_kernel,
        out_shape=(held(ny * nz, 128), held(8 * BACK, 128)),
        scratch_shapes=[
            scratch(6, EXT, 8, 128),
            scratch(4, EXT, 8, 128),
            scratch(2, EXT, 8, 128),
            scratch(2, EXT, 8, 128),
            scratch(KRYLOV + 1, 8, 8, 128),
            scratch(2, KRYLOV + 1, 8, 8, 128),
            scratch(2, 128, 128),
        ],
    )(*near(planes, low, high))

    got = lax.all_to_all(sums.reshape(-1, 1, 128), GY + ("gz",), 0, 0, tiled=True)
    back = pl.pallas_call(
        sum_kernel, out_shape=held(8 * BACK, 128), input_output_aliases={1: 0}
    )(*near(got.reshape(-1, 128), back))
    got = lax.all_to_all(back.reshape(8, BACK, 1, 128), "gx", 0, 0, tiled=True)
    return pl.pallas_call(
        solve_kernel,
        out_shape=(shape(2, 4, 8, 128), shape(2, 4, 8, 128)),
        scratch_shapes=[scratch(128, 128)],
    )(*near(got.reshape(-1, 128)))


def solution(mesh):
    nx, ny, nz = (mesh.shape[a] for a in ("gx", "gy", "gz"))
    pairs = Mesh(mesh.devices.reshape(nx, ny // 2, 2, nz), ("gx", *GY, "gz"))
    spread = P(None, "gx", GY, "gz")
    return jax.shard_map(
        body,
        mesh=pairs,
        in_specs=(spread, spread, spread, P("gx", GY, "gz")),
        out_specs=(spread, spread),
        check_vma=False,
    )
```

```python
import jax
import jax.numpy as jnp
from jax import lax
from jax.experimental import pallas as pl
from jax.experimental.pallas import tpu as pltpu
from jax.sharding import Mesh
from jax.sharding import PartitionSpec as P

KRYLOV = 10
DEPTH = KRYLOV + 1
FINE = 16
EXT = FINE + 2 * DEPTH
SENT = 7
FIELDS = 9
ROWS = 36
WIDE, THIN = 56, 20
BACK = 102
SUMS = 4 * (2 * KRYLOV + 5)
UNIQUE = KRYLOV * (KRYLOV + 1) // 2
f32 = jnp.float32
GY = ("gy_0", "gy_1")


def lanes(rows=8):
    return lax.broadcasted_iota(jnp.int32, (rows, 128), 1)


def sublanes(rows=8):
    return lax.broadcasted_iota(jnp.int32, (rows, 128), 0)


def turn(v, by):
    return v if by % 128 == 0 else pltpu.roll(v, by % 128, 1)


def sink(v, by):
    return pltpu.roll(v, by % 8, 0)


def is_reversed():
    return lax.axis_index("gz") % 2 == 1


def backwards(v):
    v = sink(v, 4)
    for d in (2, 1):
        v = jnp.where((sublanes() & d) == 0, sink(v, -d), sink(v, d))
    return v


def two_sum(a, b):
    s = a + b
    z = s - a
    return s, (a - (s - z)) + (b - z)


def quick_sum(a, b):
    s = a + b
    return s, b - (s - a)


def split(a):
    c = a * 4097.0
    high = c - (c - a)
    return high, a - high


def two_prod(a, b):
    p = a * b
    ah, al = split(a)
    bh, bl = split(b)
    return p, ((ah * bh - p) + ah * bl + al * bh) + al * bl


def dd_add(a, b):
    s, e = two_sum(a[0], b[0])
    return quick_sum(s, e + (a[1] + b[1]))


def dd_mul(a, b):
    p, e = two_prod(a[0], b[0])
    return quick_sum(p, e + (a[0] * b[1] + a[1] * b[0]))


def dd_inverse(a):
    x = 1.0 / a[0]
    p, e = two_prod(a[0], x)
    return quick_sum(x, x * (((1.0 - p) - e) - a[1] * x))


def add_pairs(a, b):
    s, e = two_sum(a[0], b[0])
    return s, e + (a[1] + b[1])


def total_of(pairs):
    pairs = list(pairs)
    while len(pairs) > 1:
        pairs = [
            add_pairs(pairs[i], pairs[i + 1]) if i + 1 < len(pairs) else pairs[i]
            for i in range(0, len(pairs), 2)
        ]
    return pairs[0]


def fold_sublanes(a):
    for by in (4, 2, 1):
        a = add_pairs(a, (sink(a[0], by), sink(a[1], by)))
    return quick_sum(*a)


def merge(a, b, d):
    low = (sublanes() & d) == 0
    return add_pairs(
        tuple(jnp.where(low, x, y) for x, y in zip(a, b)),
        tuple(jnp.where(low, sink(x, -d), sink(y, d)) for x, y in zip(a, b)),
    )


def swap_blocks(v, width):
    v = list(v)
    block = lanes() // width
    d = len(v) // 2
    while d >= 1:
        low = (block & d) == 0
        for k in range(len(v)):
            if k & d == 0:
                a, b = v[k], v[k + d]
                v[k] = jnp.where(low, a, turn(b, width * d))
                v[k + d] = jnp.where(low, turn(a, -width * d), b)
        d //= 2
    return v


def pack_kernel(source, intra, extra, membrane, out):
    refs = [(intra, 0), (intra, 1), (intra, 2), (extra, 0), (extra, 1), (extra, 2), (source, 0), (source, 1)]
    top = sublanes() < 4
    lower, upper = [], []
    for x in range(4):
        for f in range(0, 8, 2):
            a, b = refs[f][0][refs[f][1], x], refs[f + 1][0][refs[f + 1][1], x]
            lower.append(jnp.where(top, a, sink(b, 4)))
            upper.append(jnp.where(top, sink(a, 4), b))
    empty = jnp.zeros((24, 128), f32)
    last = []
    for x in range(4):
        last += [membrane[x], empty]
    lower, upper, last = (jnp.concatenate(part, 0).T for part in (lower, upper, last))
    group = (lanes() % 32) // 8
    chunks = []
    for j in range(8):
        a, b = last[16 * j : 16 * j + 8], last[16 * j + 8 : 16 * j + 16]
        m = jnp.where(group == 2, turn(b, 16), turn(sink(b, 4), 24))
        m = jnp.where(group == 1, turn(sink(a, 4), 8), m)
        m = jnp.where(group == 0, a, m)
        chunks.append((lower[16 * j : 16 * j + 16], m, upper[16 * j : 16 * j + 16]))
    for j in range(8):
        picked = [jnp.where(is_reversed(), a, b) for a, b in zip(chunks[7 - j], chunks[j])]
        for at in (2 * j * ROWS, (2 * j + 1) * ROWS):
            out[pl.ds(at, 16), :] = picked[0]
            out[pl.ds(at + 16, 4), :] = picked[1][:4]
            out[pl.ds(at + 20, 16), :] = picked[2]


def choose_kernel(pair, wide, thin):
    odd = lax.axis_index("gy_1") == 1
    for s in range(8):
        at = 2 * ROWS * s
        rows = pair[pl.ds(at + 16, WIDE), :], pair[pl.ds(at, WIDE), :]
        wide[pl.ds(WIDE * s, WIDE), :] = jnp.where(odd, *rows)
        rows = pair[pl.ds(at + 2 * ROWS - THIN, THIN), :], pair[pl.ds(at, THIN), :]
        thin[pl.ds(THIN * s, THIN), :] = jnp.where(odd, *rows)


def plane_kernel(pair, wide, thin, out, first, final):
    y = lanes() % 32
    odd = lax.axis_index("gy_1")
    is_even = jnp.full((8, 128), odd, jnp.int32) == 0

    def take(ref, row, height):
        return ref[pl.ds(row, 8, stride=height), :]

    def ordered(own, far, last):
        even = far + own + last
        other = last + own + far
        return [a if a is b else jnp.where(is_even, a, b) for a, b in zip(even, other)]

    def plane(r, n):
        z, shift = 4 * n + r, 8 * n
        own = [take(pair, at + z, 2 * ROWS) for at in (0, 20, 36, 56)]
        far = [take(wide, at + z, WIDE) for at in (4 - 4 * odd, 20, 40 - 4 * odd)]
        v = swap_blocks(ordered(own, far, [take(thin, 4 * odd + z, THIN)]), 4)
        own = [take(pair, at + r, 2 * ROWS) for at in (16, 52)]
        far = [take(wide, at + 16 * odd + r, WIDE) for at in (0, 36)]
        parts = ordered(own, far, [take(thin, 16 - 16 * odd + r, THIN)])
        m = turn(parts[4], 28 - shift)
        for n in (3, 2, 1, 0):
            m = jnp.where(y < 8 * n + 4, turn(parts[n], 8 * n - 4 - shift), m)
        return v + [m]

    def four(r, _):
        for n in range(FINE // 4):
            for f, value in enumerate(plane(r, n)):
                out[f, 4 * n + r] = value
        return _

    lax.fori_loop(0, 4, four, 0)

    def edges(f, _):
        for ref, at in ((first, lambda d: d - 1), (final, lambda d: FINE - d)):
            for d in range(1, SENT + 1):
                value = out[f, at(d)]
                if 2 < d < SENT:
                    inner = (y > d) & (y < 31 - d)
                    value = jnp.where(inner, value, turn(out[f, at(14 - d)], 16))
                ref[f, d - 1] = value
        return _

    lax.fori_loop(0, FIELDS, edges, 0)


def x_up(v):
    v = turn(v, -32)
    return jnp.where(lanes() < 96, v, sink(v, -1))


def x_down(v):
    v = turn(v, 32)
    return jnp.where(lanes() >= 32, v, sink(v, 1))


def y_up(v):
    return turn(v, -1)


def y_down(v):
    return turn(v, 1)


def slot_of(r, s):
    if s < 0:
        return UNIQUE + r
    return r * (r + 1) // 2 + s


def cycle_kernel(main, low, high, sums, back, face, inv, ta, tb, images, halves, acc):
    lane = lanes()
    ix = sublanes() * 4 + lane // 32
    last_x, first_x = ix == 31, ix == 0

    def far(ref, f, d):
        return ref[f, d - 1] if d <= SENT else turn(ref[f, 13 - d], -16)

    def field(f, i):
        if i < DEPTH:
            return far(low, f, DEPTH - i)
        if i < DEPTH + FINE:
            return main[f, i - DEPTH]
        return far(high, f, i - DEPTH - FINE + 1)

    block = (lane % 32) // 8

    def compact(planes):
        value = turn(planes[3], 12)
        for j in (2, 1, 0):
            value = jnp.where(block == j, turn(planes[j], 8 * j - 12), value)
        return value

    def send_back(array, g, planes):
        back[pl.ds(array * 4 + g, 8, stride=BACK), :] = compact(planes)

    blocks_kept = ([], [], [])
    sz = [field(2, 0), field(5, 0)]
    low_z = [None, None]
    for i in range(EXT - 1):
        diagonals = []
        for s in range(2):
            above = field(s * 3 + 2, i + 1)
            up_z = sz[s] + above
            face[s * 3 + 2, i] = up_z
            if i > 0:
                sx, sy = field(s * 3, i), field(s * 3 + 1, i)
                up_x = sx + jnp.where(last_x, 0.0, x_up(sx))
                low_x = sx + jnp.where(first_x, 0.0, x_down(sx))
                up_y = sy + y_up(sy)
                low_y = sy + y_down(sy)
                face[s * 3, i] = jnp.where(last_x, 0.0, up_x)
                face[s * 3 + 1, i] = up_y
                diagonals.append(0.5 * (up_x + low_x + up_y + low_y + up_z + low_z[s]))
            sz[s], low_z[s] = above, up_z
        if i > 0:
            di, de = diagonals
            m = field(8, i)
            det = m * di + m * de + di * de
            inside = m > 0.0
            scale = jnp.where(inside, 1.0 / jnp.where(inside, det, 1.0), 0.0)
            values = (-de * scale, -m * scale, di * scale, -(m + di) * scale)
            for n in range(4):
                inv[n, i] = values[n]
            if DEPTH <= i < DEPTH + FINE:
                for n, value in enumerate(((di + de) * scale, values[2], values[3])):
                    blocks_kept[n].append(value)
                if len(blocks_kept[0]) == 4:
                    for n in range(3):
                        send_back(2 * KRYLOV + 2 + n, (i - DEPTH) // 4, blocks_kept[n])
                    blocks_kept = ([], [], [])

    def remember(r, value):
        size = None
        for v in value:
            size = jnp.abs(v) if size is None else jnp.maximum(size, jnp.abs(v))
        grid = size * 12288.0
        for at, v in enumerate(value):
            high_part = (v + grid) - grid
            images[r, at], halves[0, r, at], halves[1, r, at] = v, high_part, v - high_part

    image = []
    for part in range(2):
        for g in range(FINE // 4):
            planes = [main[6 + part, 4 * g + j] for j in range(4)]
            image.append(compact(planes))
            send_back(part, g, planes)
    remember(0, image)

    buffers = (ta, tb)

    def vector(k, part, i):
        return field(6 + part, i) if k == 0 else buffers[k % 2][part, i]

    for k in range(KRYLOV):

        def blocks(i):
            v, p = vector(k, 0, i), vector(k, 1, i)
            return (inv[0, i] * v + inv[1, i] * p, inv[2, i] * v + inv[3, i] * p), (v, p)

        def spread(s, i, u):
            fx, fy = face[s * 3, i], face[s * 3 + 1, i]
            across = fx * x_up(u[1][s]) + x_down(fx * u[1][s])
            along = fy * y_up(u[1][s]) + y_down(fy * u[1][s])
            deep = face[s * 3 + 2, i] * u[2][s] + face[s * 3 + 2, i - 1] * u[0][s]
            return across + along + deep

        start, end = 2 + k, EXT - 2 - k
        (before, _), (here, t_here) = blocks(start - 1), blocks(start)
        kept = ([], [], [], [])
        image = ([], [])
        for i in range(start, end):
            after, t_after = blocks(i + 1)
            shared = spread(0, i, (before, here, after))
            twice = (shared, shared + spread(1, i, (before, here, after)))
            for part in range(2):
                value = 0.5 * twice[part] if k == 0 else twice[part] - vector(k - 1, part, i)
                if k + 1 < KRYLOV:
                    buffers[(k + 1) % 2][part, i] = value
                if DEPTH <= i < DEPTH + FINE:
                    kept[part].append(t_here[part] + 0.5 * twice[part])
                    kept[2 + part].append(value)
            if len(kept[0]) == 4:
                g = (i - DEPTH) // 4
                for part in range(2):
                    image[part].append(compact(kept[part]))
                    send_back(2 * k + 2 + part, g, kept[2 + part])
                kept = ([], [], [], [])
            before, here, t_here = here, after, t_after
        remember(k + 1, image[0] + image[1])

    def product(r, s):
        exact, rest = [], []
        for at in range(8):
            high_a, low_a, high_b, low_b = (
                halves[n, image, at] for image in (r, s) for n in range(2)
            )
            exact.append(high_a * high_b)
            rest.append(high_a * low_b + low_a * images[s, at])
        while len(exact) > 1:
            exact = [a + b for a, b in zip(exact[::2], exact[1::2])]
            rest = [a + b for a, b in zip(rest[::2], rest[1::2])]
        return exact[0], rest[0]

    pairs = {
        slot_of(r - 1, s - 1): (r, s) for r in range(1, KRYLOV + 1) for s in range(r + 1)
    }
    for group in range(16):
        found = [pairs.get(8 * group + i) for i in range(8)]
        if None not in found:
            values = [product(*pair) for pair in found]
            for d in (4, 2, 1):
                values = [merge(values[i], values[i + d], d) for i in range(d)]
            value = values[0]
        elif any(found):
            (pair,) = (pair for pair in found if pair)
            value = fold_sublanes(product(*pair))
        else:
            value = (jnp.zeros((8, 128), f32),) * 2
        acc[0, pl.ds(group * 8, 8), :] = value[0]
        acc[1, pl.ds(group * 8, 8), :] = value[1]
    turned = acc[0].T, acc[1].T
    value = fold_sublanes(
        total_of((turned[0][8 * i : 8 * i + 8], turned[1][8 * i : 8 * i + 8]) for i in range(16))
    )
    rows = jnp.where(sublanes() % 2 == 0, *value)
    for i in range(sums.shape[0] // 8):
        sums[pl.ds(8 * i, 8), :] = rows


def sum_kernel(received, _, back):
    zero = jnp.zeros((8, 128), f32)
    groups = range(received.shape[0] // 8)
    value = total_of((received[pl.ds(8 * i, 8), :], zero) for i in groups)
    for by in (4, 2):
        value = add_pairs(value, (sink(value[0], by), sink(value[1], by)))
    high, error = value
    value = quick_sum(high, error + sink(high, -1))
    even = sublanes() % 2 == 0
    for n in range(2):
        back[pl.ds(SUMS + n, 8, stride=BACK), :] = jnp.where(even, value[n], sink(value[n], 1))


def solve_kernel(received, solution, residual, rows):
    def take(array, g):
        return received[pl.ds(array * 4 + g, 8, stride=BACK), :]

    high, error = fold_sublanes(
        tuple(received[pl.ds(SUMS + n, 8, stride=BACK), :] for n in range(2))
    )
    row, lane = sublanes(16), lanes(16)
    matrix = []
    for n, part in enumerate((high, error)):
        part = jnp.concatenate([part, part], 0)
        value = jnp.zeros((16, 128), f32)
        for r in range(KRYLOV):
            value = jnp.where(row == r, turn(part, -slot_of(r, 0)), value)
        value = jnp.where(lane <= row, value, 0.0)
        flipped = jnp.concatenate([value, jnp.zeros((112, 128), f32)], 0).T[:16]
        value = jnp.where(lane <= row, value, flipped)
        right = jnp.zeros((16, 128), f32)
        for r in range(KRYLOV):
            right = jnp.where(row == r, turn(part, KRYLOV - slot_of(r, -1)), right)
        matrix.append(jnp.where(lane == KRYLOV, right, value))
    matrix = quick_sum(*matrix)
    for j in range(KRYLOV):
        pivot_row = tuple(jnp.broadcast_to(part[j : j + 1, :], (8, 128)) for part in matrix)
        pivot = tuple(jnp.broadcast_to(part[j : j + 1, j : j + 1], (8, 128)) for part in matrix)
        scaled = dd_mul(pivot_row, dd_inverse(pivot))
        scaled = tuple(jnp.concatenate([part, part], 0) for part in scaled)
        column = tuple(-jnp.broadcast_to(part[:, j : j + 1], (16, 128)) for part in matrix)
        rest = dd_add(matrix, dd_mul(column, scaled))
        matrix = tuple(jnp.where(row == j, a, b) for a, b in zip(scaled, rest))
    coeffs = [
        jnp.broadcast_to(matrix[0][k : k + 1, KRYLOV : KRYLOV + 1], (8, 128))
        for k in range(KRYLOV)
    ]
    image = [y for y in coeffs] + [jnp.zeros((8, 128), f32)]
    for k in range(KRYLOV):
        image[k + 1] = image[k + 1] + (coeffs[k] if k == 0 else 0.5 * coeffs[k])
        if k > 0:
            image[k - 1] = image[k - 1] + 0.5 * coeffs[k]
    image[0] = image[0] - 1.0
    for g in range(FINE // 4):
        combined, left = [], []
        for part in range(2):
            vectors = [take(2 * m + part, g) for m in range(KRYLOV + 1)]
            combined.append(sum(coeffs[k] * vectors[k] for k in range(KRYLOV)))
            left.append(-sum(image[m] * vectors[m] for m in range(KRYLOV + 1)))
        b = [take(2 * KRYLOV + 2 + n, g) for n in range(3)]
        v = [
            b[0] * combined[0] - b[1] * combined[1],
            -(b[1] * combined[0] + b[2] * combined[1]),
        ]
        for j, value in enumerate(swap_blocks(v + left, 8)):
            value = jnp.where(is_reversed(), backwards(value), value)
            rows[pl.ds(4 * g + j, 8, stride=FINE), :] = value
    turned = rows[...].T
    for f in range(4):
        ref = solution if f < 2 else residual
        for x in range(4):
            ref[f % 2, x] = turned[x * 32 + f * 8 : x * 32 + f * 8 + 8]


def shape(*dims):
    return jax.ShapeDtypeStruct(dims, f32)


def held(*dims):
    return pltpu.VMEM(dims, f32)


def near(*values):
    return tuple(pltpu.with_memory_space_constraint(v, pltpu.VMEM) for v in values)


def scratch(*dims):
    return pltpu.VMEM(dims, f32)


def body(source, sigma_intra, sigma_extra, membrane):
    nx, nz = (lax.axis_size(a) for a in ("gx", "gz"))
    ny = lax.axis_size(GY)
    packed = pl.pallas_call(pack_kernel, out_shape=held(16 * ROWS, 128))(
        source, sigma_intra, sigma_extra, membrane
    )
    pair = lax.all_to_all(packed.reshape(16, ROWS, 1, 128), ("gx", "gy_1"), 0, 0, tiled=True)
    (pair,) = near(pair.reshape(-1, 128))
    wide, thin = pl.pallas_call(
        choose_kernel, out_shape=(held(8 * WIDE, 128), held(8 * THIN, 128))
    )(pair)
    across = [(i, i + 1) for i in range(1, ny - 1, 2)]
    wide = lax.ppermute(wide, GY, across + [(b, a) for a, b in across])
    thin = lax.ppermute(
        thin,
        GY,
        [(i, i - 2) for i in range(2, ny, 2)] + [(i, i + 2) for i in range(1, ny - 2, 2)],
    )
    halo = wide, thin
    planes, first, final = pl.pallas_call(
        plane_kernel,
        out_shape=(
            held(FIELDS, FINE, 8, 128),
            held(FIELDS, SENT, 8, 128),
            held(FIELDS, SENT, 8, 128),
        ),
    )(*near(pair, *halo))

    def place(c):
        block, j = c // nx, c % nx
        return (j if block % 2 == 0 else nx - 1 - j) * nz + block

    up = [(place(c), place(c + 1)) for c in range(nx * nz - 1)]
    low = lax.ppermute(final, ("gx", "gz"), up)
    high = lax.ppermute(first, ("gx", "gz"), [(b, a) for a, b in up])

    sums, back = pl.pallas_call(
        cycle_kernel,
        out_shape=(held(2 * ny * nz, 128), held(8 * BACK, 128)),
        scratch_shapes=[
            scratch(6, EXT, 8, 128),
            scratch(4, EXT, 8, 128),
            scratch(2, EXT, 8, 128),
            scratch(2, EXT, 8, 128),
            scratch(KRYLOV + 1, 8, 8, 128),
            scratch(2, KRYLOV + 1, 8, 8, 128),
            scratch(2, 128, 128),
        ],
    )(*near(planes, low, high))

    got = lax.all_to_all(sums.reshape(-1, 2, 128), GY + ("gz",), 0, 0, tiled=True)
    back = pl.pallas_call(
        sum_kernel, out_shape=held(8 * BACK, 128), input_output_aliases={1: 0}
    )(*near(got.reshape(-1, 128), back))
    got = lax.all_to_all(back.reshape(8, BACK, 1, 128), "gx", 0, 0, tiled=True)
    return pl.pallas_call(
        solve_kernel,
        out_shape=(shape(2, 4, 8, 128), shape(2, 4, 8, 128)),
        scratch_shapes=[scratch(128, 128)],
    )(*near(got.reshape(-1, 128)))


def solution(mesh):
    nx, ny, nz = (mesh.shape[a] for a in ("gx", "gy", "gz"))
    pairs = Mesh(mesh.devices.reshape(nx, ny // 2, 2, nz), ("gx", *GY, "gz"))
    spread = P(None, "gx", GY, "gz")
    return jax.shard_map(
        body,
        mesh=pairs,
        in_specs=(spread, spread, spread, P("gx", GY, "gz")),
        out_specs=(spread, spread),
        check_vma=False,
    )
```
